256 devices in a mesh: dp: 32 (over x, z), tensor: 8 (over y, core).
Axes of the slice: x: 4, y: 4, z: 8, core: 2. Of those that a mesh axis runs over, the one named last changes fastest.
Arguments:
- vis_rows: bfloat16 [8, 256, 2, 3200], P(None, 'dp', None, 'tensor'), may hold values from -6 to 6
- ln_gain: float32 [2, 3200], replicated, may hold values from 0.25 to 1.75
- ln_bias: float32 [2, 3200], replicated, may hold values from -3 to 3
- proj_weight: bfloat16 [3200, 2, 8192], P('dp', None, 'tensor'), may hold values from -0.078125 to 0.078125
- text_rows: bfloat16 [32, 384, 8192], P('dp', None, 'tensor'), may hold values from -8 to 8
- attn_gain: float32 [8192], replicated, may hold values from 0.25 to 1.75
- w_query: bfloat16 [8192, 4096], P('dp', 'tensor'), may hold values from -0.088388348 to 0.088388348
- key_value_weight: bfloat16 [8192, 2, 1024], P('dp', None, 'tensor'), may hold values from -0.088388348 to 0.088388348
- tile_counts: int32 [32], replicated, may hold values from 1 to 16, 256 in all
- image_offsets: int32 [32], P('dp'), may hold values from 0 to 256
Outputs:
- attn_context: bfloat16 [32, 384, 4096], P('dp', None, 'tensor')
The draws below stay inside these ranges and needn't reach their ends.
Inputs may be any that keep to these rules, and one draw needn't show every extreme that they name: tile_counts counts all 256 tiles, and its largest entry is exactly 16.
All inputs are finite; a program needn't handle non-finite values.
Results may differ from the reference program's by a relative error of at most 0.0074.
Values may be sent and summed in bfloat16 or wider, within the bound.
A program may use at most 128 MiB of HBM per device.

```python
import math
import jax
import jax.numpy as jnp
import numpy as np
from jax import lax

DV = 3200
MERGE = 2
PW = 6400
MODEL_WIDTH = 8192
QUERY_HEADS = 32
KEY_VALUE_HEADS = 8
HEAD_WIDTH = 128
TILE_DEV = 8
TILE_TOK = 8
SEQUENCE_LENGTH = 384
SAMPLES = 32
TILES = 256
ROW_TOK = 256
MAXT_TILES = 16
N_DP = 32


def draw_w_query(key, part):
    bound_value = 8.0 * MODEL_WIDTH ** (-0.5)
    sampled_values = jnp.clip(jax.random.normal(jax.random.fold_in(key, 1), (MODEL_WIDTH, QUERY_HEADS * HEAD_WIDTH), jnp.float32), -4.0, 4.0) * MODEL_WIDTH ** (-0.5)
    return jnp.clip(sampled_values, -bound_value, bound_value).astype(jnp.bfloat16)


def draw_key_value_weight(key, part):
    bound_value = 8.0 * MODEL_WIDTH ** (-0.5)
    sampled_values = jnp.clip(jax.random.normal(jax.random.fold_in(key, 2), (MODEL_WIDTH, 2, KEY_VALUE_HEADS * HEAD_WIDTH), jnp.float32), -4.0, 4.0) * MODEL_WIDTH ** (-0.5)
    return jnp.clip(sampled_values, -bound_value, bound_value).astype(jnp.bfloat16)


def draw_text_rows(key, part):
    sampled_values = jnp.clip(jax.random.normal(jax.random.fold_in(key, 3), (SAMPLES, SEQUENCE_LENGTH, MODEL_WIDTH), jnp.float32), -5.0, 5.0)
    return jnp.clip(sampled_values, -8.0, 8.0).astype(jnp.bfloat16)


def with_ends(entries, own_key, smallest, top_value):
    index_at = [jax.random.randint(jax.random.fold_in(own_key, axis), (), 0, length) for axis, length in enumerate(entries.shape)]
    widest = entries.shape.index(max(entries.shape))
    beside = index_at[:widest] + [(index_at[widest] + 1) % entries.shape[widest]] + index_at[widest + 1:]
    return entries.at[tuple(index_at)].set(smallest).at[tuple(beside)].set(top_value)


def shard_levels(key, dims, pieces, smallest, largest):
    def one(axis_at, shards_of):
        draws = jax.random.uniform(jax.random.fold_in(jax.random.fold_in(key, 6), axis_at), (shards_of,), jnp.float32, smallest / len(pieces), largest / len(pieces))
        return jnp.repeat(jnp.exp(draws), dims[axis_at] // shards_of).reshape((-1,) + (1,) * (len(dims) - axis_at - 1))

    level = one(*pieces[0])
    for cut in pieces[1:]:
        level = level * one(*cut)
    return level


def profile(number_of, total, most, lean):
    loads = [(1 << 20) // math.isqrt(rank ** lean) + 1 for rank in range(2, number_of + 1)]
    spare, given = total - most - (number_of - 1), [1] * (number_of - 1)
    while spare > 0:
        movable = [i for i in range(number_of - 1) if given[i] < most]
        pool, left = sum([loads[i] for i in movable]), spare
        for i in movable:
            extra = min(most - given[i], max(1, left * loads[i] // pool), spare)
            given[i] = given[i] + extra
            spare = spare - extra
    return np.array([most] + given)


def uneven_parts(stream_key, number_of, total, most, slope):
    if number_of == 2:
        one = jax.random.randint(stream_key, (), max(1, total - most), min(most, total - 1) + 1)
        return jnp.stack([one, total - one])
    lengths = jnp.asarray(profile(number_of, total, most, slope), jnp.int32)
    couples = (number_of - 1) // 2
    source_of, receiver = lengths[1:1 + 2 * couples:2], lengths[2:2 + 2 * couples:2]
    room = jnp.minimum(source_of - 1, most - receiver)
    moved = jax.random.randint(jax.random.fold_in(stream_key, 1), (couples,), 0, 1 << 20) % (room + 1)
    lengths = lengths.at[1:1 + 2 * couples:2].set(source_of - moved).at[2:2 + 2 * couples:2].set(receiver + moved)
    return lengths[jax.random.permutation(jax.random.fold_in(stream_key, 2), number_of)]


def normal_values(own_key, dims, scale, bound, split=(), kind=jnp.bfloat16):
    level = shard_levels(own_key, dims, split, -0.22, 0.18) if split else 1.0
    entries = jax.random.normal(own_key, dims, jnp.float32) * scale * level
    return jnp.minimum(jnp.maximum(entries, -bound), bound).astype(kind)


def setup_inputs(seed: int = 0) -> dict:
    key_of = jax.random.split(jax.random.key(seed), 11)
    return {
        "vis_rows": normal_values(key_of[0], (TILE_DEV, ROW_TOK, MERGE, DV), 1.0, 6.0, ((1, 32), (3, 8))),
        "ln_gain": jnp.clip(1.0 + 0.15 * jax.random.normal(key_of[1], (MERGE, DV), jnp.float32), 0.25, 1.75),
        "ln_bias": normal_values(key_of[2], (MERGE, DV), 0.5, 3.0, (), jnp.float32),
        "proj_weight": normal_values(key_of[3], (DV, MERGE, MODEL_WIDTH), PW ** -0.5, 0.078125, ((0, 32), (2, 8))),
        "text_rows": draw_text_rows(jax.random.fold_in(key_of[10], 71), 0),
        "attn_gain": jnp.clip(1.0 + 0.15 * jax.random.normal(key_of[5], (MODEL_WIDTH,), jnp.float32), 0.25, 1.75),
        "w_query": draw_w_query(jax.random.fold_in(key_of[10], 71), 0),
        "key_value_weight": draw_key_value_weight(jax.random.fold_in(key_of[10], 71), 0),
        "tile_counts": uneven_parts(key_of[8], SAMPLES, TILES, MAXT_TILES, 2).astype(jnp.int32),
        "image_offsets": with_ends(jax.random.randint(key_of[9], (SAMPLES,), 0, SEQUENCE_LENGTH - MAXT_TILES * TILE_TOK + 1), jax.random.fold_in(key_of[9], 1), 0, SEQUENCE_LENGTH - MAXT_TILES * TILE_TOK).astype(jnp.int32),
    }


vision_epsilon = 1e-06
decoder_epsilon = 1e-05
rope_base = 500000.0

def apply_rotary(value_rows, position_indices):
    half_width = value_rows.shape[-1] // 2
    exponents = jnp.arange(half_width, dtype=jnp.float32) * (2.0 / value_rows.shape[-1])
    frequency = rope_base ** (-exponents)
    angles = position_indices.astype(jnp.float32)[:, None] * frequency[None, :]
    cosine = jnp.cos(angles)[:, None, :]
    sine = jnp.sin(angles)[:, None, :]
    first_half = value_rows[..., :half_width]
    second_half = value_rows[..., half_width:]
    return jnp.concatenate([first_half * cosine - second_half * sine, second_half * cosine + first_half * sine], axis=-1)

def layer_norm(value_rows, gain, bias_values):
    average = lax.optimization_barrier(jnp.mean(value_rows, axis=(-2, -1), keepdims=True))
    centered = value_rows - average
    variance = lax.optimization_barrier(jnp.mean(centered * centered, axis=(-2, -1), keepdims=True))
    return centered * lax.rsqrt(variance + vision_epsilon) * gain + bias_values

def decoder_sample(sequence, w_query, key_value_weight, attn_gain):
    seq_float = sequence.astype(jnp.float32)
    mean_square = lax.optimization_barrier(jnp.mean(seq_float * seq_float, axis=-1, keepdims=True))
    normalized_sequence = (seq_float * lax.rsqrt(mean_square + decoder_epsilon) * attn_gain).astype(jnp.bfloat16)
    query_full = jnp.dot(normalized_sequence, w_query, preferred_element_type=jnp.float32)
    key_value_complete = jnp.dot(normalized_sequence, key_value_weight.reshape(MODEL_WIDTH, 2 * KEY_VALUE_HEADS * HEAD_WIDTH), preferred_element_type=jnp.float32)
    key_value_complete = key_value_complete.reshape(SEQUENCE_LENGTH, 2, KEY_VALUE_HEADS * HEAD_WIDTH)
    position_indices = jnp.arange(SEQUENCE_LENGTH, dtype=jnp.int32)
    query_group_count = QUERY_HEADS // KEY_VALUE_HEADS
    query_rows = apply_rotary(query_full.reshape(SEQUENCE_LENGTH, QUERY_HEADS, HEAD_WIDTH), position_indices).astype(jnp.bfloat16)
    query_rows = query_rows.reshape(SEQUENCE_LENGTH, KEY_VALUE_HEADS, query_group_count, HEAD_WIDTH)
    key_rows = apply_rotary(key_value_complete[:, 0].reshape(SEQUENCE_LENGTH, KEY_VALUE_HEADS, HEAD_WIDTH), position_indices).astype(jnp.bfloat16)
    value_rows = key_value_complete[:, 1].reshape(SEQUENCE_LENGTH, KEY_VALUE_HEADS, HEAD_WIDTH).astype(jnp.bfloat16)
    scores = jnp.einsum('pgjd,kgd->gjpk', query_rows.astype(jnp.float32), key_rows.astype(jnp.float32)) * HEAD_WIDTH ** (-0.5)
    causal = position_indices[:, None] >= position_indices[None, :]
    scores = jnp.where(causal[None, None], scores, -1e+30)
    row_max = lax.optimization_barrier(jnp.max(scores, axis=-1, keepdims=True))
    exponentials = jnp.exp(scores - row_max)
    weights = (exponentials / lax.optimization_barrier(jnp.sum(exponentials, axis=-1, keepdims=True))).astype(jnp.bfloat16)
    context = jnp.einsum('gjpk,kgd->pgjd', weights.astype(jnp.float32), value_rows.astype(jnp.float32))
    return context.astype(jnp.bfloat16).reshape(SEQUENCE_LENGTH, QUERY_HEADS * HEAD_WIDTH)

def reference(vis_rows, ln_gain, ln_bias, proj_weight, text_rows, attn_gain, w_query, key_value_weight, tile_counts, image_offsets):
    merged = vis_rows.reshape(TILE_DEV * ROW_TOK, MERGE, DV).astype(jnp.float32)
    normed_vis = layer_norm(merged, ln_gain, ln_bias).astype(jnp.bfloat16)
    flat_weight = jnp.transpose(proj_weight, (1, 0, 2)).reshape(MERGE * DV, MODEL_WIDTH)
    image_cols = jnp.dot(normed_vis.reshape(TILE_DEV * ROW_TOK, MERGE * DV), flat_weight, preferred_element_type=jnp.float32).astype(jnp.bfloat16)
    image_tiles = image_cols.reshape(TILE_DEV, N_DP, TILE_TOK, MODEL_WIDTH).reshape(TILES, TILE_TOK, MODEL_WIDTH)
    tile_ends = jnp.cumsum(tile_counts).astype(jnp.int32)
    tile_first = (tile_ends - tile_counts).astype(jnp.int32)
    tile_order = jnp.arange(MAXT_TILES, dtype=jnp.int32)
    image_span = MAXT_TILES * TILE_TOK

    def per_sample(inputs):
        sequence, first_tile, count, offset = inputs
        picked = jnp.clip(first_tile + tile_order, 0, TILES - 1).astype(jnp.int32)
        arrived = image_tiles[picked].reshape(image_span, MODEL_WIDTH)
        start_row = offset.astype(jnp.int32)
        current = lax.dynamic_slice_in_dim(sequence, start_row, image_span, 0)
        is_image = jnp.repeat(tile_order < count, TILE_TOK)[:, None]
        merged_rows = jnp.where(is_image, arrived, current)
        sequence = lax.dynamic_update_slice_in_dim(sequence, merged_rows, start_row, 0)
        return decoder_sample(sequence, w_query, key_value_weight, attn_gain)
    return lax.map(per_sample, (text_rows, tile_first, tile_counts, image_offsets))
```

```python
import functools

import jax
import jax.numpy as jnp
import numpy as np
from jax import lax
from jax.experimental import pallas as pl
from jax.experimental.pallas import tpu as pltpu
from jax.sharding import PartitionSpec as P

MESH = pl.DeviceIdType.MESH
BF = jnp.bfloat16
F32 = jnp.float32

HEAD_WIDTH = 128
SEQ = 384
TOK = 64
NX, NY, NZ = 4, 4, 8
LANES = 256
ROWS = 208
PART = 200
vision_epsilon = 1e-06
decoder_epsilon = 1e-05
rope_base = 500000.0

STARTS = (0, 0, 3, 5, 7)
SLOTS = max(STARTS) + 5


def dot(a, b):
    return jnp.dot(a, b, preferred_element_type=F32)


def lane_of(shape):
    return lax.broadcasted_iota(jnp.int32, shape, len(shape) - 1)


def row_of(shape):
    return lax.broadcasted_iota(jnp.int32, shape, len(shape) - 2)


def kernel(
    cnt_ref, off_ref, vis_ref, gain_ref, bias_ref, proj_ref, qkv_ref, text_ref, cos_ref, sin_ref,
    out_ref,
    wp, wq, vis_all, vis_own, stats, acts, vs, vr, im, ia, ot, rt, oi, ri, stt, rstt, sti, rsti,
    a2s, a2r,
    l_sem, z_s, z_r, st_s, st_r, b_s, b_r, d_s, d_r, vs_s, vs_r, t_s, t_r, i_s, i_r, n_s, n_r,
    a_s, a_r,
):
    dp = lax.axis_index("dp")
    tn = lax.axis_index("tensor")
    x, z = dp // NZ, dp % NZ
    y, c = tn // 2, tn % 2
    pending = []

    def remote(src, dst, ssem, rsem, to):
        return pltpu.make_async_remote_copy(
            src_ref=src, dst_ref=dst, send_sem=ssem, recv_sem=rsem, device_id=to,
            device_id_type=MESH,
        )

    def send(src, dst, ssem, rsem, to):
        copy = remote(src, dst, ssem, rsem, to)
        copy.start()
        pending.append(copy)

    here = (dp, tn)

    def arrived(ref, ssem, rsem):
        remote(ref, ref, ssem, rsem, here).wait_recv()

    def own(u):
        return proj_ref.at[u] if u < 2 else qkv_ref.at[u - 2]

    def slot_ref(u, source):
        if u < 2:
            return wp.at[u, source, pl.ds(0, ROWS)]
        return wq.at[u - 2, source]

    def goes(u, e, k):
        return k < 4 or (u % 2 == e)

    def ring(slot):
        for u, start in enumerate(STARTS):
            k = slot - start
            if k < 0 or k > 4:
                continue
            for e in range(2):
                sign = 1 if e == 0 else -1
                source = (z - sign * k + 2 * NZ) % NZ
                if k >= 1 and goes(u, e, k):
                    arrived(slot_ref(u, source), z_s.at[u, e, k - 1], z_r.at[u, e, k - 1])
                if k <= 3 and goes(u, e, k + 1):
                    to = (x * NZ + (z + sign + NZ) % NZ, tn)
                    src = own(u) if k == 0 else slot_ref(u, source)
                    send(src, slot_ref(u, source), z_s.at[u, e, k], z_r.at[u, e, k], to)

    def spread(kind, src, dst):
        for o in range(NY):
            to = (y * NZ + z, ((y + o) % NY) * 2 + c)
            copy = remote(src, dst, b_s.at[kind, o], b_r.at[kind, x], to)
            if o:
                copy.start()
                pending.append(copy)
            else:
                local = pltpu.make_async_copy(src, dst, b_r.at[kind, x])

                @pl.when(x != y)
                def _():
                    copy.start()

                @pl.when(x == y)
                def _():
                    local.start()

    def spread_done(kind, src, dst):
        copy = remote(src, dst, b_s.at[kind, 0], b_r.at[kind, x], (y * NZ + z, y * 2 + c))

        @pl.when(x != y)
        def _():
            copy.wait_send()

    def to_sibling(kind, place):
        for s in range(NX):
            arrived(place(c, s), b_s.at[kind, 0], b_r.at[kind, s])
            send(place(c, s), place(c, s), d_s.at[kind, s], d_r.at[kind, s], (dp, tn + 1 - 2 * c))

    def from_sibling(kind, place):
        for s in range(NX):
            arrived(place(1 - c, s), d_s.at[kind, s], d_r.at[kind, s])

    def vis_place(core, s):
        return vis_all.at[pl.ds(4 * core, 4), s]

    def text_place(core, s):
        return acts.at[core, s]

    def image_place(core, s):
        return ia.at[core, s]

    def along_x(o):
        return (((x + o) % NX) * NZ + z, tn)

    ring(0)
    locals_ = []
    for u in range(5):
        local = pltpu.make_async_copy(own(u), slot_ref(u, z), l_sem.at[u])
        local.start()
        locals_.append(local)

    xv = vis_ref[...].astype(F32)
    mean = jnp.sum(jnp.sum(xv, axis=0), axis=-1, keepdims=True) / (4 * PART)
    centred = jnp.where(lane_of(xv.shape) < PART, xv - mean[None], 0.0)
    m2 = jnp.sum(jnp.sum(centred * centred, axis=0), axis=-1, keepdims=True)
    stats[tn] = jnp.where(lane_of((TOK, 128)) == 0, mean, m2)
    for o in range(1, 8):
        send(stats.at[tn], stats.at[tn], st_s.at[o - 1], st_r.at[o - 1], (dp, (tn + o) % 8))
    for u in range(2):
        for s in range(NZ):
            wp[u, s, ROWS:LANES, :] = jnp.zeros((LANES - ROWS, 512), BF)
    for o in range(1, 8):
        arrived(stats.at[(tn - o + 8) % 8], st_s.at[o - 1], st_r.at[o - 1])
    means = [stats[t][:, 0:1] for t in range(8)]
    mean = sum(means[1:], means[0]) / 8.0
    total = jnp.zeros((TOK, 1), F32)
    for t in range(8):
        apart = means[t] - mean
        total = total + stats[t][:, 1:2] + (4.0 * PART) * apart * apart
    scale = lax.rsqrt(total / (32.0 * PART) + vision_epsilon)
    for i in range(4):
        piece = vis_ref[i].astype(F32)
        vis_own[i] = ((piece - mean) * scale * gain_ref[i] + bias_ref[i]).astype(BF)
    spread(0, vis_own, vis_place(c, x))
    spread(1, text_ref, text_place(c, x))

    def vision():
        from_sibling(0, vis_place)
        for h in range(2):
            acc = None
            for s in range(NZ):
                term = dot(vis_all[s].reshape(NX * TOK, LANES), wp[h, s])
                acc = term if acc is None else acc + term
            cols = pl.ds(512 * h, 512)
            vs[:, :, cols] = acc.reshape(NX, TOK, 512).astype(BF)
        for o in range(1, NX):
            send(vs.at[(x + o) % NX], vr.at[o - 1], vs_s.at[o - 1], vs_r.at[o - 1], along_x(o))

    def image():
        acc = vs[x].astype(F32)
        for o in range(1, NX):
            arrived(vr.at[o - 1], vs_s.at[o - 1], vs_r.at[o - 1])
            acc = acc + vr[o - 1].astype(F32)
        im[...] = acc.astype(BF)
        spread(2, im, image_place(c, x))

    def squares(source, o, rows):
        s = (x + o) % NX
        acc = jnp.zeros((rows, 1), F32)
        for core in range(2):
            v = source[core, s].astype(F32)
            acc = acc + jnp.sum(v * v, axis=-1, keepdims=True)
        high = acc.astype(BF).astype(F32)
        mid = (acc - high).astype(BF).astype(F32)
        low = acc - high - mid
        lane = lane_of((rows, 128))
        return jnp.where(lane == 0, high, jnp.where(lane == 1, mid, low)).astype(BF)

    def text_squares():
        for o in range(NX):
            if o == 0:
                rstt[0] = squares(acts, 0, SEQ)
            else:
                stt[o - 1] = squares(acts, o, SEQ)
        for o in range(1, NX):
            send(stt.at[o - 1], rstt.at[o], n_s.at[0, o - 1], n_r.at[0, o - 1], along_x(o))

    def image_squares():
        for o in range(NX):
            if o == 0:
                rsti[0] = squares(ia, 0, TOK)
            else:
                sti[o - 1] = squares(ia, o, TOK)
        for o in range(1, NX):
            send(sti.at[o - 1], rsti.at[o], n_s.at[1, o - 1], n_r.at[1, o - 1], along_x(o))

    def project(source, u, o):
        s = (x + o) % NX
        first = dot(source[0, s], wq[u, 0:4].reshape(1024, 256))
        return first + dot(source[1, s], wq[u, 4:8].reshape(1024, 256))

    def text_unit(u):
        for o in (2, 1, 3, 0):
            value = project(acts, u, o).astype(BF)
            if o == 0:
                rt[u, 0] = value
            else:
                ot[u, o - 1] = value
                send(ot.at[u, o - 1], rt.at[u, o], t_s.at[u, o - 1], t_r.at[u, o - 1], along_x(o))

    def image_unit(u):
        for o in (2, 1, 3, 0):
            value = project(ia, u, o).astype(BF)
            if o == 0:
                ri[u, 0] = value
            else:
                oi[u, o - 1] = value
                send(oi.at[u, o - 1], ri.at[u, o], i_s.at[u, o - 1], i_r.at[u, o - 1], along_x(o))

    def locals_done(us):
        for u in us:
            locals_[u].wait()

    for slot in range(1, SLOTS):
        ring(slot)
        if slot == 1:
            to_sibling(0, vis_place)
        if slot == 4:
            locals_done((0, 1))
            vision()
        if slot == 5:
            to_sibling(1, text_place)
        if slot == 6:
            image()
            from_sibling(1, text_place)
            text_squares()
        if slot == 7:
            locals_done((2, 3, 4))
            text_unit(0)
        if slot == 8:
            to_sibling(2, image_place)
        if slot == 9:
            from_sibling(2, image_place)
            text_unit(1)
            image_squares()
            image_unit(0)
            image_unit(1)
        if slot == 11:
            image_unit(2)

    first = jnp.int32(0)
    my_first = jnp.int32(0)
    my_count = jnp.int32(0)
    owners = [jnp.int32(0)] * 8
    for s in range(NX * NZ):
        count = cnt_ref[s]
        my_first = my_first + jnp.where(s < dp, count, 0)
        my_count = my_count + jnp.where(s == dp, count, 0)
        first = first + count
        owners = [a + jnp.where(first <= r * 32 + dp, 1, 0) for r, a in enumerate(owners)]
    shape = (512, 128)
    row, col = row_of(shape), lane_of(shape)
    owner = jnp.zeros(shape, jnp.int32)
    for r in range(8):
        owner = jnp.where(((col >> 3) & 7) == r, owners[r], owner)
    same = ((row >> 4) == owner) & (((row >> 3) & 1) == (col >> 6)) & ((row & 7) == (col & 7))
    pick = jnp.where(same, 1.0, 0.0).astype(BF)

    def gathered(buffer, rows, sems, receives):
        acc = buffer[0].astype(F32)
        for o in range(1, NX):
            arrived(buffer.at[o], sems.at[o - 1], receives.at[o - 1])
            acc = acc + buffer[o].astype(F32)
        return acc

    def row_scale(buffer, rows, which):
        acc = gathered(buffer, rows, n_s.at[which], n_r.at[which])
        total = jnp.sum(jnp.where(lane_of(acc.shape) < 3, acc, 0.0), axis=-1, keepdims=True)
        return lax.rsqrt(total / 8192.0 + decoder_epsilon)

    image_scale = row_scale(rsti, TOK, 1)
    pieces = [(gathered(ri.at[u], TOK, i_s.at[u], i_r.at[u]) * image_scale).astype(BF)
              for u in range(3)]
    low = jnp.concatenate([pieces[0], pieces[1][:, 0:128]], axis=1)
    high = jnp.concatenate([pieces[1][:, 128:256], pieces[2]], axis=1)
    both = jnp.concatenate([low, high], axis=0)
    a2s[...] = dot(pick, both).astype(BF).reshape(32, 16, 384)
    a2r[dp] = a2s[dp]

    def route(o, carry):
        to = (dp + o) % 32
        remote(a2s.at[to], a2r.at[dp], a_s.at[o - 1], a_r.at[o - 1], (to, tn)).start()
        return carry

    lax.fori_loop(1, 32, route, 0)
    text_unit(2)

    shape = (SEQ, 512)
    row, col = row_of(shape), lane_of(shape)
    place = row - off_ref[0]
    inside = (place >= 0) & (place < 8 * my_count)
    source = (my_first + (place >> 3)) & 31
    match = inside & ((col >> 4) == source) & ((col & 7) == (place & 7))
    sel_low = jnp.where(match & (((col >> 3) & 1) == 0), 1.0, 0.0).astype(BF)
    sel_high = jnp.where(match & (((col >> 3) & 1) == 1), 1.0, 0.0).astype(BF)
    place = row_of((SEQ, 128)) - off_ref[0]
    is_image = (place >= 0) & (place < 8 * my_count)
    causal = row_of((SEQ, SEQ)) >= lane_of((SEQ, SEQ))
    text_scale = row_scale(rstt, SEQ, 0)

    def route_done(o, carry):
        source = (dp - o + 32) % 32
        remote(a2s.at[source], a2r.at[source], a_s.at[o - 1], a_r.at[o - 1], here).wait_recv()
        return carry

    lax.fori_loop(1, 32, route_done, 0)
    routed = a2r[...].reshape(512, 384)
    image_low = dot(sel_low, routed)
    image_high = dot(sel_high, routed)

    texts = [gathered(rt.at[u], SEQ, t_s.at[u], t_r.at[u]) * text_scale for u in range(3)]
    cos, sin = cos_ref[...], sin_ref[...]

    def column(i):
        text = texts[i // 2][:, 128 * (i % 2) : 128 * (i % 2) + 128]
        picture = image_low if i < 3 else image_high
        picture = picture[:, 128 * (i % 3) : 128 * (i % 3) + 128]
        return jnp.where(is_image, picture, text)

    def turned(value):
        return (value * cos + pltpu.roll(value, 64, 1) * sin).astype(BF)

    key = turned(column(4))
    value = column(5).astype(BF)
    for h in range(4):
        query = turned(column(h))
        scores = lax.dot_general(query, key, (((1,), (1,)), ((), ())), preferred_element_type=F32)
        scores = jnp.where(causal, scores * HEAD_WIDTH ** (-0.5), -1e30)
        powers = jnp.exp(scores - jnp.max(scores, axis=-1, keepdims=True))
        weights = (powers / jnp.sum(powers, axis=-1, keepdims=True)).astype(BF)
        out_ref[:, 128 * h : 128 * h + 128] = dot(weights, value).astype(BF)

    for copy in pending:
        copy.wait_send()
    spread_done(0, vis_own, vis_place(c, x))
    spread_done(1, text_ref, text_place(c, x))
    spread_done(2, im, image_place(c, x))

    def sent(o, carry):
        to = (dp + o) % 32
        remote(a2s.at[to], a2r.at[dp], a_s.at[o - 1], a_r.at[o - 1], here).wait_send()
        return carry

    lax.fori_loop(1, 32, sent, 0)


def rotation_tables():
    exponents = np.arange(64, dtype=np.float32) * np.float32(2.0 / 128)
    frequency = np.float32(rope_base) ** (-exponents)
    angles = np.arange(SEQ, dtype=np.float32)[:, None] * frequency[None, :]
    cos, sin = np.cos(angles), np.sin(angles)
    return (
        np.concatenate([cos, cos], axis=1).astype(np.float32),
        np.concatenate([-sin, sin], axis=1).astype(np.float32),
    )


def per_device(vis_rows, ln_gain, ln_bias, proj_weight, text_rows, attn_gain, w_query,
               key_value_weight, tile_counts, image_offsets):
    dp = lax.axis_index("dp")
    tn = lax.axis_index("tensor")

    def lanes(a):
        return jnp.pad(a, [(0, 0)] * (a.ndim - 1) + [(0, LANES - PART)])

    vis = vis_rows.reshape(TOK, 2, 4, 100).transpose(2, 0, 3, 1).reshape(4, TOK, PART)
    vis = lanes(vis)

    def features(a):
        a = lax.dynamic_slice_in_dim(a, tn * 400, 400, 1)
        return lanes(a.reshape(2, 4, 100).transpose(1, 2, 0).reshape(4, 1, PART))

    proj = jnp.pad(proj_weight.reshape(PART, 1024), ((0, ROWS - PART), (0, 0)))
    proj = proj.reshape(ROWS, 2, 512).transpose(1, 0, 2)
    rows = lax.dynamic_slice_in_dim(attn_gain, dp * 256, 256, 0)[:, None]
    qkv = jnp.concatenate([w_query, key_value_weight.reshape(256, 256)], axis=1)
    qkv = (qkv.astype(F32) * rows).astype(BF).reshape(256, 3, 256).transpose(1, 0, 2)
    cos, sin = rotation_tables()
    vmem = pl.BlockSpec(memory_space=pltpu.VMEM)
    smem = pl.BlockSpec(memory_space=pltpu.SMEM)
    dma = pltpu.SemaphoreType.DMA
    out = pl.pallas_call(
        kernel,
        out_shape=jax.ShapeDtypeStruct((SEQ, 512), BF),
        in_specs=[smem, smem] + [vmem] * 8,
        out_specs=vmem,
        scratch_shapes=[
            pltpu.VMEM((2, NZ, LANES, 512), BF),
            pltpu.VMEM((3, NZ, 256, 256), BF),
            pltpu.VMEM((NZ, NX, TOK, LANES), BF),
            pltpu.VMEM((4, TOK, LANES), BF),
            pltpu.VMEM((8, TOK, 128), F32),
            pltpu.VMEM((2, NX, SEQ, 1024), BF),
            pltpu.VMEM((NX, TOK, 1024), BF),
            pltpu.VMEM((NX - 1, TOK, 1024), BF),
            pltpu.VMEM((TOK, 1024), BF),
            pltpu.VMEM((2, NX, TOK, 1024), BF),
            pltpu.VMEM((3, NX - 1, SEQ, 256), BF),
            pltpu.VMEM((3, NX, SEQ, 256), BF),
            pltpu.VMEM((3, NX - 1, TOK, 256), BF),
            pltpu.VMEM((3, NX, TOK, 256), BF),
            pltpu.VMEM((NX - 1, SEQ, 128), BF),
            pltpu.VMEM((NX, SEQ, 128), BF),
            pltpu.VMEM((NX - 1, TOK, 128), BF),
            pltpu.VMEM((NX, TOK, 128), BF),
            pltpu.VMEM((32, 16, 384), BF),
            pltpu.VMEM((32, 16, 384), BF),
            dma((5,)),
            dma((5, 2, 4)),
            dma((5, 2, 4)),
            dma((7,)),
            dma((7,)),
            dma((3, NY)),
            dma((3, NX)),
            dma((3, NX)),
            dma((3, NX)),
            dma((3,)),
            dma((3,)),
            dma((3, 3)),
            dma((3, 3)),
            dma((3, 3)),
            dma((3, 3)),
            dma((2, 3)),
            dma((2, 3)),
            dma((31,)),
            dma((31,)),
        ],
        compiler_params=pltpu.CompilerParams(has_side_effects=True, vmem_limit_bytes=60 << 20),
        name="step",
    )(tile_counts, image_offsets, vis, features(ln_gain), features(ln_bias), proj, qkv,
      text_rows[0], jnp.asarray(cos), jnp.asarray(sin))
    return out[None]


def solution(mesh):
    in_specs = (
        P(None, "dp", None, "tensor"),
        P(),
        P(),
        P("dp", None, "tensor"),
        P("dp", None, "tensor"),
        P(),
        P("dp", "tensor"),
        P("dp", None, "tensor"),
        P(),
        P("dp"),
    )
    return jax.shard_map(per_device, mesh=mesh, in_specs=in_specs,
                         out_specs=P("dp", None, "tensor"), check_vma=False)
```

```python
import functools

import jax
import jax.numpy as jnp
import numpy as np
from jax import lax
from jax.experimental import pallas as pl
from jax.experimental.pallas import tpu as pltpu
from jax.sharding import PartitionSpec as P

MESH = pl.DeviceIdType.MESH
BF = jnp.bfloat16
F32 = jnp.float32

HEAD_WIDTH = 128
SEQ = 384
TOK = 64
NX, NY, NZ = 4, 4, 8
LANES = 256
ROWS = 208
PART = 200
vision_epsilon = 1e-06
decoder_epsilon = 1e-05
rope_base = 500000.0

STARTS = (0, 0, 3, 5, 7)
SLOTS = max(STARTS) + 5


def dot(a, b):
    return jnp.dot(a, b, preferred_element_type=F32)


def lane_of(shape):
    return lax.broadcasted_iota(jnp.int32, shape, len(shape) - 1)


def row_of(shape):
    return lax.broadcasted_iota(jnp.int32, shape, len(shape) - 2)


def kernel(
    cnt_ref, off_ref, vis_ref, gain_ref, bias_ref, proj_ref, qkv_ref, text_ref, cos_ref, sin_ref,
    out_ref,
    wp, wq, vis_all, vis_own, stats, acts, vs, vr, im, ia, ot, rt, oi, ri, stt, rstt, sti, rsti,
    a2s, a2r, vis_col, text_col, im_col,
    l_sem, z_s, z_r, st_s, st_r, ys_s, ys_r, xs_s, xs_r, d_s, d_r, vs_s, vs_r, t_s, t_r, i_s, i_r, n_s, n_r,
    a_s, a_r,
):
    dp = lax.axis_index("dp")
    tn = lax.axis_index("tensor")
    x, z = dp // NZ, dp % NZ
    y, c = tn // 2, tn % 2
    pending = []

    def remote(src, dst, ssem, rsem, to):
        return pltpu.make_async_remote_copy(
            src_ref=src, dst_ref=dst, send_sem=ssem, recv_sem=rsem, device_id=to,
            device_id_type=MESH,
        )

    def send(src, dst, ssem, rsem, to):
        copy = remote(src, dst, ssem, rsem, to)
        copy.start()
        pending.append(copy)

    here = (dp, tn)

    def arrived(ref, ssem, rsem):
        remote(ref, ref, ssem, rsem, here).wait_recv()

    def own(u):
        return proj_ref.at[u] if u < 2 else qkv_ref.at[u - 2]

    def slot_ref(u, source):
        if u < 2:
            return wp.at[u, source, pl.ds(0, ROWS)]
        return wq.at[u - 2, source]

    def goes(u, e, k):
        return k < 4 or (u % 2 == e)

    def ring(slot):
        for u, start in enumerate(STARTS):
            k = slot - start
            if k < 0 or k > 4:
                continue
            for e in range(2):
                sign = 1 if e == 0 else -1
                source = (z - sign * k + 2 * NZ) % NZ
                if k >= 1 and goes(u, e, k):
                    arrived(slot_ref(u, source), z_s.at[u, e, k - 1], z_r.at[u, e, k - 1])
                if k <= 3 and goes(u, e, k + 1):
                    to = (x * NZ + (z + sign + NZ) % NZ, tn)
                    src = own(u) if k == 0 else slot_ref(u, source)
                    send(src, slot_ref(u, source), z_s.at[u, e, k], z_r.at[u, e, k], to)

    class Spread:
        def __init__(self, kind, own, column, place):
            self.kind, self.own, self.column, self.place = kind, own, column, place

        def on_y(self, src, slot, h, step):
            k = self.kind
            send(src, self.column(slot, h), ys_s.at[k, slot, h], ys_r.at[k, slot, h],
                 (dp, ((y + step + NY) % NY) * 2 + c))

        def on_x(self, src, j, h, kappa):
            k = self.kind
            copy = remote(src, self.place(c, x, h), xs_s.at[k, j, h], xs_r.at[k, x, h],
                          (kappa * NZ + z, tn))
            local = pltpu.make_async_copy(src, self.place(c, x, h), xs_r.at[k, x, h])

            @pl.when(kappa != x)
            def _():
                copy.start()

            @pl.when(kappa == x)
            def _():
                local.start()

            later.append((copy, kappa))

        def begin(self):
            for h in range(2):
                self.on_y(self.own(h), 0, h, 1)
                self.on_y(self.own(h), 1, h, -1)
            for h in range(2):
                self.on_x(self.own(h), 3, h, y)

        def near(self, h):
            k = self.kind
            for slot, step in ((0, 1), (1, -1)):
                arrived(self.column(slot, h), ys_s.at[k, slot, h], ys_r.at[k, slot, h])
                if slot == h:
                    src = self.column(slot, h)
                    send(src, self.column(2, h), ys_s.at[k, 2, h], ys_r.at[k, 2, h],
                         (dp, ((y + step + NY) % NY) * 2 + c))
            for slot, step in ((0, 1), (1, -1)):
                self.on_x(self.column(slot, h), slot, h, (y - step + NY) % NY)

        def far(self, h):
            k = self.kind
            arrived(self.column(2, h), ys_s.at[k, 2, h], ys_r.at[k, 2, h])
            self.on_x(self.column(2, h), 2, h, (y + 2) % NY)

        def to_sibling(self):
            k = self.kind
            for s in range(NX):
                for h in range(2):
                    ref = self.place(c, s, h)
                    arrived(ref, xs_s.at[k, 0, h], xs_r.at[k, s, h])
                    send(ref, ref, d_s.at[k, s, h], d_r.at[k, s, h], (dp, tn + 1 - 2 * c))

        def from_sibling(self):
            k = self.kind
            for s in range(NX):
                for h in range(2):
                    arrived(self.place(1 - c, s, h), d_s.at[k, s, h], d_r.at[k, s, h])

    later = []
    vis_spread = Spread(
        0,
        lambda h: vis_own.at[pl.ds(2 * h, 2)],
        lambda j, h: vis_col.at[j, pl.ds(2 * h, 2)],
        lambda core, s, h: vis_all.at[pl.ds(4 * core + 2 * h, 2), s],
    )
    text_spread = Spread(
        1,
        lambda h: text_ref.at[pl.ds(192 * h, 192)],
        lambda j, h: text_col.at[j, pl.ds(192 * h, 192)],
        lambda core, s, h: acts.at[core, s, pl.ds(192 * h, 192)],
    )
    image_spread = Spread(
        2,
        lambda h: im.at[pl.ds(32 * h, 32)],
        lambda j, h: im_col.at[j, pl.ds(32 * h, 32)],
        lambda core, s, h: ia.at[core, s, pl.ds(32 * h, 32)],
    )

    def along_x(o):
        return (((x + o) % NX) * NZ + z, tn)

    ring(0)
    locals_ = []
    for u in range(5):
        local = pltpu.make_async_copy(own(u), slot_ref(u, z), l_sem.at[u])
        local.start()
        locals_.append(local)

    xv = vis_ref[...].astype(F32)
    mean = jnp.sum(jnp.sum(xv, axis=0), axis=-1, keepdims=True) / (4 * PART)
    centred = jnp.where(lane_of(xv.shape) < PART, xv - mean[None], 0.0)
    m2 = jnp.sum(jnp.sum(centred * centred, axis=0), axis=-1, keepdims=True)
    stats[tn] = jnp.where(lane_of((TOK, 128)) == 0, mean, m2)
    for o in range(1, 8):
        send(stats.at[tn], stats.at[tn], st_s.at[o - 1], st_r.at[o - 1], (dp, (tn + o) % 8))
    for u in range(2):
        for s in range(NZ):
            wp[u, s, ROWS:LANES, :] = jnp.zeros((LANES - ROWS, 512), BF)
    for o in range(1, 8):
        arrived(stats.at[(tn - o + 8) % 8], st_s.at[o - 1], st_r.at[o - 1])
    means = [stats[t][:, 0:1] for t in range(8)]
    mean = sum(means[1:], means[0]) / 8.0
    total = jnp.zeros((TOK, 1), F32)
    for t in range(8):
        apart = means[t] - mean
        total = total + stats[t][:, 1:2] + (4.0 * PART) * apart * apart
    scale = lax.rsqrt(total / (32.0 * PART) + vision_epsilon)
    for i in range(4):
        piece = vis_ref[i].astype(F32)
        vis_own[i] = ((piece - mean) * scale * gain_ref[i] + bias_ref[i]).astype(BF)
    vis_spread.begin()
    text_spread.begin()

    def vision():
        vis_spread.from_sibling()
        for h in range(2):
            acc = None
            for s in range(NZ):
                term = dot(vis_all[s].reshape(NX * TOK, LANES), wp[h, s])
                acc = term if acc is None else acc + term
            cols = pl.ds(512 * h, 512)
            vs[:, :, cols] = acc.reshape(NX, TOK, 512).astype(BF)
        for o in range(1, NX):
            send(vs.at[(x + o) % NX], vr.at[o - 1], vs_s.at[o - 1], vs_r.at[o - 1], along_x(o))

    def image():
        acc = vs[x].astype(F32)
        for o in range(1, NX):
            arrived(vr.at[o - 1], vs_s.at[o - 1], vs_r.at[o - 1])
            acc = acc + vr[o - 1].astype(F32)
        im[...] = acc.astype(BF)
        image_spread.begin()

    def squares(source, o, rows):
        s = (x + o) % NX
        acc = jnp.zeros((rows, 1), F32)
        for core in range(2):
            v = source[core, s].astype(F32)
            acc = acc + jnp.sum(v * v, axis=-1, keepdims=True)
        high = acc.astype(BF).astype(F32)
        mid = (acc - high).astype(BF).astype(F32)
        low = acc - high - mid
        lane = lane_of((rows, 128))
        return jnp.where(lane == 0, high, jnp.where(lane == 1, mid, low)).astype(BF)

    def text_squares():
        for o in range(NX):
            if o == 0:
                rstt[0] = squares(acts, 0, SEQ)
            else:
                stt[o - 1] = squares(acts, o, SEQ)
        for o in range(1, NX):
            send(stt.at[o - 1], rstt.at[o], n_s.at[0, o - 1], n_r.at[0, o - 1], along_x(o))

    def image_squares():
        for o in range(NX):
            if o == 0:
                rsti[0] = squares(ia, 0, TOK)
            else:
                sti[o - 1] = squares(ia, o, TOK)
        for o in range(1, NX):
            send(sti.at[o - 1], rsti.at[o], n_s.at[1, o - 1], n_r.at[1, o - 1], along_x(o))

    def project(source, u, o):
        s = (x + o) % NX
        first = dot(source[0, s], wq[u, 0:4].reshape(1024, 256))
        return first + dot(source[1, s], wq[u, 4:8].reshape(1024, 256))

    def text_unit(u):
        for o in (2, 1, 3, 0):
            value = project(acts, u, o).astype(BF)
            if o == 0:
                rt[u, 0] = value
            else:
                ot[u, o - 1] = value
                send(ot.at[u, o - 1], rt.at[u, o], t_s.at[u, o - 1], t_r.at[u, o - 1], along_x(o))

    def image_unit(u):
        for o in (2, 1, 3, 0):
            value = project(ia, u, o).astype(BF)
            if o == 0:
                ri[u, 0] = value
            else:
                oi[u, o - 1] = value
                send(oi.at[u, o - 1], ri.at[u, o], i_s.at[u, o - 1], i_r.at[u, o - 1], along_x(o))

    def locals_done(us):
        for u in us:
            locals_[u].wait()

    for slot in range(1, SLOTS):
        ring(slot)
        if slot == 1:
            vis_spread.near(0)
            vis_spread.near(1)
            text_spread.near(0)
            vis_spread.far(0)
            vis_spread.far(1)
        if slot == 2:
            vis_spread.to_sibling()
            text_spread.near(1)
        if slot == 3:
            text_spread.far(0)
            text_spread.far(1)
        if slot == 4:
            locals_done((0, 1))
            vision()
        if slot == 5:
            text_spread.to_sibling()
        if slot == 6:
            image()
            text_spread.from_sibling()
            image_spread.near(0)
            image_spread.near(1)
            text_squares()
            image_spread.far(0)
            image_spread.far(1)
        if slot == 7:
            locals_done((2, 3, 4))
            text_unit(0)
            image_spread.to_sibling()
        if slot == 9:
            image_spread.from_sibling()
            text_unit(1)
            image_squares()
            image_unit(0)
            image_unit(1)
        if slot == 11:
            image_unit(2)

    first = jnp.int32(0)
    my_first = jnp.int32(0)
    my_count = jnp.int32(0)
    owners = [jnp.int32(0)] * 8
    for s in range(NX * NZ):
        count = cnt_ref[s]
        my_first = my_first + jnp.where(s < dp, count, 0)
        my_count = my_count + jnp.where(s == dp, count, 0)
        first = first + count
        owners = [a + jnp.where(first <= r * 32 + dp, 1, 0) for r, a in enumerate(owners)]
    shape = (512, 128)
    row, col = row_of(shape), lane_of(shape)
    owner = jnp.zeros(shape, jnp.int32)
    for r in range(8):
        owner = jnp.where(((col >> 3) & 7) == r, owners[r], owner)
    same = ((row >> 4) == owner) & (((row >> 3) & 1) == (col >> 6)) & ((row & 7) == (col & 7))
    pick = jnp.where(same, 1.0, 0.0).astype(BF)

    def gathered(buffer, rows, sems, receives):
        acc = buffer[0].astype(F32)
        for o in range(1, NX):
            arrived(buffer.at[o], sems.at[o - 1], receives.at[o - 1])
            acc = acc + buffer[o].astype(F32)
        return acc

    def row_scale(buffer, rows, which):
        acc = gathered(buffer, rows, n_s.at[which], n_r.at[which])
        total = jnp.sum(jnp.where(lane_of(acc.shape) < 3, acc, 0.0), axis=-1, keepdims=True)
        return lax.rsqrt(total / 8192.0 + decoder_epsilon)

    image_scale = row_scale(rsti, TOK, 1)
    pieces = [(gathered(ri.at[u], TOK, i_s.at[u], i_r.at[u]) * image_scale).astype(BF)
              for u in range(3)]
    low = jnp.concatenate([pieces[0], pieces[1][:, 0:128]], axis=1)
    high = jnp.concatenate([pieces[1][:, 128:256], pieces[2]], axis=1)
    both = jnp.concatenate([low, high], axis=0)
    a2s[...] = dot(pick, both).astype(BF).reshape(32, 16, 384)
    a2r[dp] = a2s[dp]

    def route(o, carry):
        to = (dp + o) % 32
        remote(a2s.at[to], a2r.at[dp], a_s.at[o - 1], a_r.at[o - 1], (to, tn)).start()
        return carry

    lax.fori_loop(1, 32, route, 0)
    text_unit(2)

    shape = (SEQ, 512)
    row, col = row_of(shape), lane_of(shape)
    place = row - off_ref[0]
    inside = (place >= 0) & (place < 8 * my_count)
    source = (my_first + (place >> 3)) & 31
    match = inside & ((col >> 4) == source) & ((col & 7) == (place & 7))
    sel_low = jnp.where(match & (((col >> 3) & 1) == 0), 1.0, 0.0).astype(BF)
    sel_high = jnp.where(match & (((col >> 3) & 1) == 1), 1.0, 0.0).astype(BF)
    place = row_of((SEQ, 128)) - off_ref[0]
    is_image = (place >= 0) & (place < 8 * my_count)
    causal = row_of((SEQ, SEQ)) >= lane_of((SEQ, SEQ))
    text_scale = row_scale(rstt, SEQ, 0)

    def route_done(o, carry):
        source = (dp - o + 32) % 32
        remote(a2s.at[source], a2r.at[source], a_s.at[o - 1], a_r.at[o - 1], here).wait_recv()
        return carry

    lax.fori_loop(1, 32, route_done, 0)
    routed = a2r[...].reshape(512, 384)
    image_low = dot(sel_low, routed)
    image_high = dot(sel_high, routed)

    texts = [gathered(rt.at[u], SEQ, t_s.at[u], t_r.at[u]) * text_scale for u in range(3)]
    cos, sin = cos_ref[...], sin_ref[...]

    def column(i):
        text = texts[i // 2][:, 128 * (i % 2) : 128 * (i % 2) + 128]
        picture = image_low if i < 3 else image_high
        picture = picture[:, 128 * (i % 3) : 128 * (i % 3) + 128]
        return jnp.where(is_image, picture, text)

    def turned(value):
        return (value * cos + pltpu.roll(value, 64, 1) * sin).astype(BF)

    key = turned(column(4))
    value = column(5).astype(BF)
    for h in range(4):
        query = turned(column(h))
        scores = lax.dot_general(query, key, (((1,), (1,)), ((), ())), preferred_element_type=F32)
        scores = jnp.where(causal, scores * HEAD_WIDTH ** (-0.5), -1e30)
        powers = jnp.exp(scores - jnp.max(scores, axis=-1, keepdims=True))
        weights = (powers / jnp.sum(powers, axis=-1, keepdims=True)).astype(BF)
        out_ref[:, 128 * h : 128 * h + 128] = dot(weights, value).astype(BF)

    for copy in pending:
        copy.wait_send()
    for copy, kappa in later:

        @pl.when(kappa != x)
        def _(copy=copy):
            copy.wait_send()


    def sent(o, carry):
        to = (dp + o) % 32
        remote(a2s.at[to], a2r.at[dp], a_s.at[o - 1], a_r.at[o - 1], here).wait_send()
        return carry

    lax.fori_loop(1, 32, sent, 0)


def rotation_tables():
    exponents = np.arange(64, dtype=np.float32) * np.float32(2.0 / 128)
    frequency = np.float32(rope_base) ** (-exponents)
    angles = np.arange(SEQ, dtype=np.float32)[:, None] * frequency[None, :]
    cos, sin = np.cos(angles), np.sin(angles)
    return (
        np.concatenate([cos, cos], axis=1).astype(np.float32),
        np.concatenate([-sin, sin], axis=1).astype(np.float32),
    )


def per_device(vis_rows, ln_gain, ln_bias, proj_weight, text_rows, attn_gain, w_query,
               key_value_weight, tile_counts, image_offsets):
    dp = lax.axis_index("dp")
    tn = lax.axis_index("tensor")

    def lanes(a):
        return jnp.pad(a, [(0, 0)] * (a.ndim - 1) + [(0, LANES - PART)])

    vis = vis_rows.reshape(TOK, 2, 4, 100).transpose(2, 0, 3, 1).reshape(4, TOK, PART)
    vis = lanes(vis)

    def features(a):
        a = lax.dynamic_slice_in_dim(a, tn * 400, 400, 1)
        return lanes(a.reshape(2, 4, 100).transpose(1, 2, 0).reshape(4, 1, PART))

    proj = jnp.pad(proj_weight.reshape(PART, 1024), ((0, ROWS - PART), (0, 0)))
    proj = proj.reshape(ROWS, 2, 512).transpose(1, 0, 2)
    rows = lax.dynamic_slice_in_dim(attn_gain, dp * 256, 256, 0)[:, None]
    qkv = jnp.concatenate([w_query, key_value_weight.reshape(256, 256)], axis=1)
    qkv = (qkv.astype(F32) * rows).astype(BF).reshape(256, 3, 256).transpose(1, 0, 2)
    cos, sin = rotation_tables()
    vmem = pl.BlockSpec(memory_space=pltpu.VMEM)
    smem = pl.BlockSpec(memory_space=pltpu.SMEM)
    dma = pltpu.SemaphoreType.DMA
    out = pl.pallas_call(
        kernel,
        out_shape=jax.ShapeDtypeStruct((SEQ, 512), BF),
        in_specs=[smem, smem] + [vmem] * 8,
        out_specs=vmem,
        scratch_shapes=[
            pltpu.VMEM((2, NZ, LANES, 512), BF),
            pltpu.VMEM((3, NZ, 256, 256), BF),
            pltpu.VMEM((NZ, NX, TOK, LANES), BF),
            pltpu.VMEM((4, TOK, LANES), BF),
            pltpu.VMEM((8, TOK, 128), F32),
            pltpu.VMEM((2, NX, SEQ, 1024), BF),
            pltpu.VMEM((NX, TOK, 1024), BF),
            pltpu.VMEM((NX - 1, TOK, 1024), BF),
            pltpu.VMEM((TOK, 1024), BF),
            pltpu.VMEM((2, NX, TOK, 1024), BF),
            pltpu.VMEM((3, NX - 1, SEQ, 256), BF),
            pltpu.VMEM((3, NX, SEQ, 256), BF),
            pltpu.VMEM((3, NX - 1, TOK, 256), BF),
            pltpu.VMEM((3, NX, TOK, 256), BF),
            pltpu.VMEM((NX - 1, SEQ, 128), BF),
            pltpu.VMEM((NX, SEQ, 128), BF),
            pltpu.VMEM((NX - 1, TOK, 128), BF),
            pltpu.VMEM((NX, TOK, 128), BF),
            pltpu.VMEM((32, 16, 384), BF),
            pltpu.VMEM((32, 16, 384), BF),
            pltpu.VMEM((3, 4, TOK, LANES), BF),
            pltpu.VMEM((3, SEQ, 1024), BF),
            pltpu.VMEM((3, TOK, 1024), BF),
            dma((5,)),
            dma((5, 2, 4)),
            dma((5, 2, 4)),
            dma((7,)),
            dma((7,)),
            dma((3, 3, 2)),
            dma((3, 3, 2)),
            dma((3, 4, 2)),
            dma((3, NX, 2)),
            dma((3, NX, 2)),
            dma((3, NX, 2)),
            dma((3,)),
            dma((3,)),
            dma((3, 3)),
            dma((3, 3)),
            dma((3, 3)),
            dma((3, 3)),
            dma((2, 3)),
            dma((2, 3)),
            dma((31,)),
            dma((31,)),
        ],
        compiler_params=pltpu.CompilerParams(has_side_effects=True, vmem_limit_bytes=60 << 20),
        name="step",
    )(tile_counts, image_offsets, vis, features(ln_gain), features(ln_bias), proj, qkv,
      text_rows[0], jnp.asarray(cos), jnp.asarray(sin))
    return out[None]


def solution(mesh):
    in_specs = (
        P(None, "dp", None, "tensor"),
        P(),
        P(),
        P("dp", None, "tensor"),
        P("dp", None, "tensor"),
        P(),
        P("dp", "tensor"),
        P("dp", None, "tensor"),
        P(),
        P("dp"),
    )
    return jax.shard_map(per_device, mesh=mesh, in_specs=in_specs,
                         out_specs=P("dp", None, "tensor"), check_vma=False)
```

```python
import functools

import jax
import jax.numpy as jnp
import numpy as np
from jax import lax
from jax.experimental import pallas as pl
from jax.experimental.pallas import tpu as pltpu
from jax.sharding import PartitionSpec as P

MESH = pl.DeviceIdType.MESH
BF = jnp.bfloat16
F32 = jnp.float32

HEAD_WIDTH = 128
SEQ = 384
TOK = 64
NX, NY, NZ = 4, 4, 8
LANES = 256
ROWS = 208
PART = 200
vision_epsilon = 1e-06
decoder_epsilon = 1e-05
rope_base = 500000.0

STARTS = (0, 0, 3, 4, 5)
SLOTS = max(STARTS) + 5


def dot(a, b):
    return jnp.dot(a, b, preferred_element_type=F32)


def lane_of(shape):
    return lax.broadcasted_iota(jnp.int32, shape, len(shape) - 1)


def row_of(shape):
    return lax.broadcasted_iota(jnp.int32, shape, len(shape) - 2)


def kernel(
    cnt_ref, off_ref, vis_ref, gain_ref, bias_ref, proj_ref, qkv_ref, text_ref, cos_ref, sin_ref,
    out_ref,
    wp, wq, vis_all, vis_own, stats, acts, vs, im, ia, n_out, n_in,
    v_fo, v_fi, v_no, v_ni, v_own, i_fo, i_fi, i_no, i_ni, i_own, t_fo, t_fi, t_no, t_ni, t_own,
    a2s, a2r, vis_col, text_col, im_col, text_relay,
    l_sem, z_s, z_r, st_s, st_r, ys_s, ys_r, xs_s, xs_r, rl_s, rl_r, d_s, d_r, f_s, f_r, g_s, g_r, n_s, n_r,
    a_s, a_r,
):
    dp = lax.axis_index("dp")
    tn = lax.axis_index("tensor")
    x, z = dp // NZ, dp % NZ
    y, c = tn // 2, tn % 2
    pending = []

    def remote(src, dst, ssem, rsem, to):
        return pltpu.make_async_remote_copy(
            src_ref=src, dst_ref=dst, send_sem=ssem, recv_sem=rsem, device_id=to,
            device_id_type=MESH,
        )

    def send(src, dst, ssem, rsem, to):
        copy = remote(src, dst, ssem, rsem, to)
        copy.start()
        pending.append(copy)

    here = (dp, tn)

    def arrived(ref, ssem, rsem):
        remote(ref, ref, ssem, rsem, here).wait_recv()

    def own(u):
        return proj_ref.at[u] if u < 2 else qkv_ref.at[u - 2]

    def slot_ref(u, source):
        if u < 2:
            return wp.at[u, source, pl.ds(0, ROWS)]
        return wq.at[u - 2, source]

    def goes(u, e, k):
        return k < 4 or (u % 2 == e)

    def ring(slot):
        for u, start in enumerate(STARTS):
            k = slot - start
            if k < 0 or k > 4:
                continue
            for e in range(2):
                sign = 1 if e == 0 else -1
                source = (z - sign * k + 2 * NZ) % NZ
                if k >= 1 and goes(u, e, k):
                    arrived(slot_ref(u, source), z_s.at[u, e, k - 1], z_r.at[u, e, k - 1])
                if k <= 3 and goes(u, e, k + 1):
                    to = (x * NZ + (z + sign + NZ) % NZ, tn)
                    src = own(u) if k == 0 else slot_ref(u, source)
                    send(src, slot_ref(u, source), z_s.at[u, e, k], z_r.at[u, e, k], to)

    class Spread:
        def __init__(self, kind, own, column, place, relayed=None):
            self.kind, self.own, self.column, self.place = kind, own, column, place
            self.relayed = relayed

        def on_y(self, src, slot, h, step):
            k = self.kind
            send(src, self.column(slot, h), ys_s.at[k, slot, h], ys_r.at[k, slot, h],
                 (dp, ((y + step + NY) % NY) * 2 + c))

        def on_x(self, src, j, h, kappa):
            k = self.kind
            copy = remote(src, self.place(c, x, h), xs_s.at[k, j, h], xs_r.at[k, x, h],
                          (kappa * NZ + z, tn))
            local = pltpu.make_async_copy(src, self.place(c, x, h), xs_r.at[k, x, h])
            opposite = kappa == (x + 2) % NX
            direct = kappa != x
            if self.relayed is not None:
                direct = direct & jnp.logical_not(opposite)
                beside = ((x + (1 if h == 0 else NX - 1)) % NX) * NZ + z
                via = remote(src, self.relayed.at[h], xs_s.at[k, j, h], rl_r.at[h], (beside, tn))

                @pl.when(opposite)
                def _():
                    via.start()

            @pl.when(direct)
            def _():
                copy.start()

            @pl.when(kappa == x)
            def _():
                local.start()

            later.append((copy, kappa))

        def relay(self, h):
            step = 1 if h == 0 else NX - 1
            source = (x + NX - step) % NX
            arrived(self.relayed.at[h], rl_s.at[h], rl_r.at[h])
            send(self.relayed.at[h], self.place(c, source, h), rl_s.at[h],
                 xs_r.at[self.kind, source, h], (((x + step) % NX) * NZ + z, tn))

        def begin(self):
            for h in range(2):
                self.on_y(self.own(h), 0, h, 1)
                self.on_y(self.own(h), 1, h, -1)
            for h in range(2):
                self.on_x(self.own(h), 3, h, y)

        def near(self, h):
            k = self.kind
            for slot, step in ((0, 1), (1, -1)):
                arrived(self.column(slot, h), ys_s.at[k, slot, h], ys_r.at[k, slot, h])
                if slot == h:
                    src = self.column(slot, h)
                    send(src, self.column(2, h), ys_s.at[k, 2, h], ys_r.at[k, 2, h],
                         (dp, ((y + step + NY) % NY) * 2 + c))
            for slot, step in ((0, 1), (1, -1)):
                self.on_x(self.column(slot, h), slot, h, (y - step + NY) % NY)

        def far(self, h):
            k = self.kind
            arrived(self.column(2, h), ys_s.at[k, 2, h], ys_r.at[k, 2, h])
            self.on_x(self.column(2, h), 2, h, (y + 2) % NY)

        def to_sibling(self):
            k = self.kind
            for s in range(NX):
                for h in range(2):
                    ref = self.place(c, s, h)
                    arrived(ref, xs_s.at[k, 0, h], xs_r.at[k, s, h])
                    send(ref, ref, d_s.at[k, s, h], d_r.at[k, s, h], (dp, tn + 1 - 2 * c))

        def from_sibling(self):
            k = self.kind
            for s in range(NX):
                for h in range(2):
                    arrived(self.place(1 - c, s, h), d_s.at[k, s, h], d_r.at[k, s, h])

    later = []
    vis_spread = Spread(
        0,
        lambda h: vis_own.at[pl.ds(2 * h, 2)],
        lambda j, h: vis_col.at[j, pl.ds(2 * h, 2)],
        lambda core, s, h: vis_all.at[pl.ds(4 * core + 2 * h, 2), s],
    )
    text_spread = Spread(
        1,
        lambda h: text_ref.at[pl.ds(192 * h, 192)],
        lambda j, h: text_col.at[j, pl.ds(192 * h, 192)],
        lambda core, s, h: acts.at[core, s, pl.ds(192 * h, 192)],
        text_relay,
    )
    image_spread = Spread(
        2,
        lambda h: im.at[pl.ds(32 * h, 32)],
        lambda j, h: im_col.at[j, pl.ds(32 * h, 32)],
        lambda core, s, h: ia.at[core, s, pl.ds(32 * h, 32)],
    )

    def along_x(o):
        return (((x + o) % NX) * NZ + z, tn)

    barrier = pltpu.get_barrier_semaphore()

    def greet_dp(o, carry):
        pl.semaphore_signal(barrier, inc=1, device_id=((dp + o) % 32, tn), device_id_type=MESH)
        return carry

    def greet_tensor(o, carry):
        pl.semaphore_signal(barrier, inc=1, device_id=(dp, (tn + o) % 8), device_id_type=MESH)
        return carry

    lax.fori_loop(1, 32, greet_dp, 0)
    lax.fori_loop(1, 8, greet_tensor, 0)
    pl.semaphore_wait(barrier, 38)
    ring(0)
    locals_ = []
    for u in range(5):
        local = pltpu.make_async_copy(own(u), slot_ref(u, z), l_sem.at[u])
        local.start()
        locals_.append(local)

    xv = vis_ref[...].astype(F32)
    mean = jnp.sum(jnp.sum(xv, axis=0), axis=-1, keepdims=True) / (4 * PART)
    centred = jnp.where(lane_of(xv.shape) < PART, xv - mean[None], 0.0)
    m2 = jnp.sum(jnp.sum(centred * centred, axis=0), axis=-1, keepdims=True)
    stats[tn] = jnp.where(lane_of((TOK, 128)) == 0, mean, m2)
    for o in range(1, 8):
        send(stats.at[tn], stats.at[tn], st_s.at[o - 1], st_r.at[o - 1], (dp, (tn + o) % 8))
    for u in range(2):
        for s in range(NZ):
            wp[u, s, ROWS:LANES, :] = jnp.zeros((LANES - ROWS, 512), BF)
    for o in range(1, 8):
        arrived(stats.at[(tn - o + 8) % 8], st_s.at[o - 1], st_r.at[o - 1])
    means = [stats[t][:, 0:1] for t in range(8)]
    mean = sum(means[1:], means[0]) / 8.0
    total = jnp.zeros((TOK, 1), F32)
    for t in range(8):
        apart = means[t] - mean
        total = total + stats[t][:, 1:2] + (4.0 * PART) * apart * apart
    scale = lax.rsqrt(total / (32.0 * PART) + vision_epsilon)
    for i in range(4):
        piece = vis_ref[i].astype(F32)
        vis_own[i] = ((piece - mean) * scale * gain_ref[i] + bias_ref[i]).astype(BF)
    vis_spread.begin()

    class Reduce:
        def __init__(self, index, far_out, far_in, near_out, near_in, own, value):
            self.i, self.value, self.own = index, value, own
            self.far_out, self.far_in = far_out, far_in
            self.near_out, self.near_in = near_out, near_in
            self.half = far_out.shape[0] // 2

        def opposite(self):
            i, half = self.i, self.half
            self.far_out[...] = self.value(2).astype(BF)
            for h in range(2):
                part = pl.ds(half * h, half)
                send(self.far_out.at[part], self.far_in.at[part], f_s.at[i, h], f_r.at[i, h],
                     along_x(1 if h == 0 else 3))
            self.own[...] = self.value(0)

        def neighbours(self):
            i, half = self.i, self.half
            for h in range(2):
                part = pl.ds(half * h, half)
                rest = pl.ds(half * (1 - h), half)
                o = 1 if h == 0 else 3
                value = self.value(o)
                arrived(self.far_in.at[part], f_s.at[i, h], f_r.at[i, h])
                mine = value[half * h : half * h + half] + self.far_in[part, :].astype(F32)
                self.near_out[h, part, :] = mine.astype(BF)
                self.near_out[h, rest, :] = value[half * (1 - h) : half * (1 - h) + half].astype(BF)
                send(self.near_out.at[h], self.near_in.at[h], g_s.at[i, h], g_r.at[i, h], along_x(o))

        def total(self):
            i = self.i
            acc = self.own[...]
            for h in range(2):
                arrived(self.near_in.at[h], g_s.at[i, h], g_r.at[i, h])
                acc = acc + self.near_in[h].astype(F32)
            return acc

    def project(source, u, o):
        s = (x + o) % NX
        first = dot(source[0, s], wq[u, 0:4].reshape(1024, 256))
        return first + dot(source[1, s], wq[u, 4:8].reshape(1024, 256))

    vis_reduce = Reduce(0, v_fo, v_fi, v_no, v_ni, v_own, lambda o: vs[(x + o) % NX])
    image_reduce = Reduce(
        1, i_fo, i_fi, i_no, i_ni, i_own,
        lambda o: jnp.concatenate([project(ia, u, o) for u in range(3)], axis=1),
    )
    text_reduce = [
        Reduce(2 + u, t_fo.at[u], t_fi.at[u], t_no.at[u], t_ni.at[u], t_own.at[u],
               lambda o, u=u: project(acts, u, o))
        for u in range(3)
    ]

    def vision():
        vis_spread.from_sibling()
        for h in range(2):
            acc = None
            for s in range(NZ):
                term = dot(vis_all[s].reshape(NX * TOK, LANES), wp[h, s])
                acc = term if acc is None else acc + term
            vs[:, :, 512 * h : 512 * h + 512] = acc.reshape(NX, TOK, 512)

    def image():
        im[...] = vis_reduce.total().astype(BF)
        image_spread.begin()

    def squares(which, source, rows):
        for o in range(NX):
            s = (x + o) % NX
            acc = jnp.zeros((rows, 1), F32)
            for core in range(2):
                v = source[core, s].astype(F32)
                acc = acc + jnp.sum(v * v, axis=-1, keepdims=True)
            acc = jnp.broadcast_to(acc, (rows, 128))
            if rows % 128:
                acc = jnp.concatenate([acc, jnp.zeros((128 - rows % 128, 128), F32)], axis=0)
            for b in range(acc.shape[0] // 128):
                line = acc[128 * b : 128 * b + 128].T[0:1]
                if o == 0:
                    n_in[which, 0, b : b + 1, :] = line
                else:
                    n_out[which, o - 1, b : b + 1, :] = line
            if o:
                send(n_out.at[which, o - 1], n_in.at[which, o], n_s.at[which, o - 1],
                     n_r.at[which, o - 1], along_x(o))

    def row_scale(which, rows):
        acc = n_in[which, 0]
        for o in range(1, NX):
            arrived(n_in.at[which, o], n_s.at[which, o - 1], n_r.at[which, o - 1])
            acc = acc + n_in[which, o]
        scale = lax.rsqrt(acc / 8192.0 + decoder_epsilon)
        lines = [jnp.broadcast_to(scale[b : b + 1], (128, 128)).T for b in range((rows + 127) // 128)]
        return jnp.concatenate(lines, axis=0)[0:rows, 0:1]

    def locals_done(us):
        for u in us:
            locals_[u].wait()

    for slot in range(1, SLOTS):
        ring(slot)
        if slot == 1:
            vis_spread.near(0)
            vis_spread.near(1)
            text_spread.begin()
            vis_spread.far(0)
            vis_spread.far(1)
        if slot == 2:
            text_spread.near(0)
            vis_spread.to_sibling()
        if slot == 3:
            text_spread.near(1)
        if slot == 4:
            locals_done((0, 1))
            vision()
            vis_reduce.opposite()
            text_spread.far(0)
            text_spread.far(1)
        if slot == 5:
            vis_reduce.neighbours()
            text_spread.relay(0)
            text_spread.relay(1)
        if slot == 6:
            image()
        if slot == 7:
            image_spread.near(0)
            image_spread.near(1)
            image_spread.far(0)
            image_spread.far(1)
            text_spread.to_sibling()
            text_spread.from_sibling()
            locals_done((2, 3, 4))
            text_reduce[0].opposite()
        if slot == 8:
            image_spread.to_sibling()
            text_reduce[0].neighbours()
            text_reduce[1].opposite()
            squares(0, acts, SEQ)
        if slot == 9:
            text_reduce[1].neighbours()
            image_spread.from_sibling()
            squares(1, ia, TOK)
            image_reduce.opposite()
            text_reduce[2].opposite()
            image_reduce.neighbours()

    first = jnp.int32(0)
    my_first = jnp.int32(0)
    my_count = jnp.int32(0)
    owners = [jnp.int32(0)] * 8
    for s in range(NX * NZ):
        count = cnt_ref[s]
        my_first = my_first + jnp.where(s < dp, count, 0)
        my_count = my_count + jnp.where(s == dp, count, 0)
        first = first + count
        owners = [a + jnp.where(first <= r * 32 + dp, 1, 0) for r, a in enumerate(owners)]
    shape = (512, 128)
    row, col = row_of(shape), lane_of(shape)
    owner = jnp.zeros(shape, jnp.int32)
    for r in range(8):
        owner = jnp.where(((col >> 3) & 7) == r, owners[r], owner)
    same = ((row >> 4) == owner) & (((row >> 3) & 1) == (col >> 6)) & ((row & 7) == (col & 7))
    pick = jnp.where(same, 1.0, 0.0).astype(BF)

    image_scale = row_scale(1, TOK)
    image_rows = (image_reduce.total() * image_scale).astype(BF)
    low, high = image_rows[:, 0:384], image_rows[:, 384:768]
    both = jnp.concatenate([low, high], axis=0)
    a2s[...] = dot(pick, both).astype(BF).reshape(32, 16, 384)
    a2r[dp] = a2s[dp]

    def route(o, carry):
        to = (dp + o) % 32
        remote(a2s.at[to], a2r.at[dp], a_s.at[o - 1], a_r.at[o - 1], (to, tn)).start()
        return carry

    lax.fori_loop(1, 32, route, 0)
    text_reduce[2].neighbours()

    shape = (SEQ, 512)
    row, col = row_of(shape), lane_of(shape)
    place = row - off_ref[0]
    inside = (place >= 0) & (place < 8 * my_count)
    source = (my_first + (place >> 3)) & 31
    match = inside & ((col >> 4) == source) & ((col & 7) == (place & 7))
    sel_low = jnp.where(match & (((col >> 3) & 1) == 0), 1.0, 0.0).astype(BF)
    sel_high = jnp.where(match & (((col >> 3) & 1) == 1), 1.0, 0.0).astype(BF)
    place = row_of((SEQ, 128)) - off_ref[0]
    is_image = (place >= 0) & (place < 8 * my_count)
    causal = row_of((SEQ, SEQ)) >= lane_of((SEQ, SEQ))
    text_scale = row_scale(0, SEQ)

    def route_done(o, carry):
        source = (dp - o + 32) % 32
        remote(a2s.at[source], a2r.at[source], a_s.at[o - 1], a_r.at[o - 1], here).wait_recv()
        return carry

    lax.fori_loop(1, 32, route_done, 0)
    routed = a2r[...].reshape(512, 384)
    image_low = dot(sel_low, routed)
    image_high = dot(sel_high, routed)

    texts = [text_reduce[u].total() * text_scale for u in range(3)]
    cos, sin = cos_ref[...], sin_ref[...]

    def column(i):
        text = texts[i // 2][:, 128 * (i % 2) : 128 * (i % 2) + 128]
        picture = image_low if i < 3 else image_high
        picture = picture[:, 128 * (i % 3) : 128 * (i % 3) + 128]
        return jnp.where(is_image, picture, text)

    def turned(value):
        return (value * cos + pltpu.roll(value, 64, 1) * sin).astype(BF)

    key = turned(column(4))
    value = column(5).astype(BF)
    for h in range(4):
        query = turned(column(h))
        scores = lax.dot_general(query, key, (((1,), (1,)), ((), ())), preferred_element_type=F32)
        scores = jnp.where(causal, scores * HEAD_WIDTH ** (-0.5), -1e30)
        powers = jnp.exp(scores - jnp.max(scores, axis=-1, keepdims=True))
        weights = (powers / jnp.sum(powers, axis=-1, keepdims=True)).astype(BF)
        out_ref[:, 128 * h : 128 * h + 128] = dot(weights, value).astype(BF)

    for copy in pending:
        copy.wait_send()
    for copy, kappa in later:

        @pl.when(kappa != x)
        def _(copy=copy):
            copy.wait_send()


    def sent(o, carry):
        to = (dp + o) % 32
        remote(a2s.at[to], a2r.at[dp], a_s.at[o - 1], a_r.at[o - 1], here).wait_send()
        return carry

    lax.fori_loop(1, 32, sent, 0)


def rotation_tables():
    exponents = np.arange(64, dtype=np.float32) * np.float32(2.0 / 128)
    frequency = np.float32(rope_base) ** (-exponents)
    angles = np.arange(SEQ, dtype=np.float32)[:, None] * frequency[None, :]
    cos, sin = np.cos(angles), np.sin(angles)
    return (
        np.concatenate([cos, cos], axis=1).astype(np.float32),
        np.concatenate([-sin, sin], axis=1).astype(np.float32),
    )


def per_device(vis_rows, ln_gain, ln_bias, proj_weight, text_rows, attn_gain, w_query,
               key_value_weight, tile_counts, image_offsets):
    dp = lax.axis_index("dp")
    tn = lax.axis_index("tensor")

    def lanes(a):
        return jnp.pad(a, [(0, 0)] * (a.ndim - 1) + [(0, LANES - PART)])

    vis = vis_rows.reshape(TOK, 2, 4, 100).transpose(2, 0, 3, 1).reshape(4, TOK, PART)
    vis = lanes(vis)

    def features(a):
        a = lax.dynamic_slice_in_dim(a, tn * 400, 400, 1)
        return lanes(a.reshape(2, 4, 100).transpose(1, 2, 0).reshape(4, 1, PART))

    proj = jnp.pad(proj_weight.reshape(PART, 1024), ((0, ROWS - PART), (0, 0)))
    proj = proj.reshape(ROWS, 2, 512).transpose(1, 0, 2)
    rows = lax.dynamic_slice_in_dim(attn_gain, dp * 256, 256, 0)[:, None]
    qkv = jnp.concatenate([w_query, key_value_weight.reshape(256, 256)], axis=1)
    qkv = (qkv.astype(F32) * rows).astype(BF).reshape(256, 3, 256).transpose(1, 0, 2)
    cos, sin = rotation_tables()
    vmem = pl.BlockSpec(memory_space=pltpu.VMEM)
    smem = pl.BlockSpec(memory_space=pltpu.SMEM)
    dma = pltpu.SemaphoreType.DMA
    out = pl.pallas_call(
        kernel,
        out_shape=jax.ShapeDtypeStruct((SEQ, 512), BF),
        in_specs=[smem, smem] + [vmem] * 8,
        out_specs=vmem,
        scratch_shapes=[
            pltpu.VMEM((2, NZ, LANES, 512), BF),
            pltpu.VMEM((3, NZ, 256, 256), BF),
            pltpu.VMEM((NZ, NX, TOK, LANES), BF),
            pltpu.VMEM((4, TOK, LANES), BF),
            pltpu.VMEM((8, TOK, 128), F32),
            pltpu.VMEM((2, NX, SEQ, 1024), BF),
            pltpu.VMEM((NX, TOK, 1024), F32),
            pltpu.VMEM((TOK, 1024), BF),
            pltpu.VMEM((2, NX, TOK, 1024), BF),
            pltpu.VMEM((2, NX - 1, 8, 128), F32),
            pltpu.VMEM((2, NX, 8, 128), F32),
            pltpu.VMEM((TOK, 1024), BF),
            pltpu.VMEM((TOK, 1024), BF),
            pltpu.VMEM((2, TOK, 1024), BF),
            pltpu.VMEM((2, TOK, 1024), BF),
            pltpu.VMEM((TOK, 1024), F32),
            pltpu.VMEM((TOK, 768), BF),
            pltpu.VMEM((TOK, 768), BF),
            pltpu.VMEM((2, TOK, 768), BF),
            pltpu.VMEM((2, TOK, 768), BF),
            pltpu.VMEM((TOK, 768), F32),
            pltpu.VMEM((3, SEQ, 256), BF),
            pltpu.VMEM((3, SEQ, 256), BF),
            pltpu.VMEM((3, 2, SEQ, 256), BF),
            pltpu.VMEM((3, 2, SEQ, 256), BF),
            pltpu.VMEM((3, SEQ, 256), F32),
            pltpu.VMEM((32, 16, 384), BF),
            pltpu.VMEM((32, 16, 384), BF),
            pltpu.VMEM((3, 4, TOK, LANES), BF),
            pltpu.VMEM((3, SEQ, 1024), BF),
            pltpu.VMEM((3, TOK, 1024), BF),
            pltpu.VMEM((2, 192, 1024), BF),
            dma((5,)),
            dma((5, 2, 4)),
            dma((5, 2, 4)),
            dma((7,)),
            dma((7,)),
            dma((3, 3, 2)),
            dma((3, 3, 2)),
            dma((3, 4, 2)),
            dma((3, NX, 2)),
            dma((2,)),
            dma((2,)),
            dma((3, NX, 2)),
            dma((3, NX, 2)),
            dma((5, 2)),
            dma((5, 2)),
            dma((5, 2)),
            dma((5, 2)),
            dma((2, 3)),
            dma((2, 3)),
            dma((31,)),
            dma((31,)),
        ],
        compiler_params=pltpu.CompilerParams(collective_id=0, has_side_effects=True, vmem_limit_bytes=60 << 20),
        name="step",
    )(tile_counts, image_offsets, vis, features(ln_gain), features(ln_bias), proj, qkv,
      text_rows[0], jnp.asarray(cos), jnp.asarray(sin))
    return out[None]


def solution(mesh):
    in_specs = (
        P(None, "dp", None, "tensor"),
        P(),
        P(),
        P("dp", None, "tensor"),
        P("dp", None, "tensor"),
        P(),
        P("dp", "tensor"),
        P("dp", None, "tensor"),
        P(),
        P("dp"),
    )
    return jax.shard_map(per_device, mesh=mesh, in_specs=in_specs,
                         out_specs=P("dp", None, "tensor"), check_vma=False)
```

```python
import functools

import jax
import jax.numpy as jnp
import numpy as np
from jax import lax
from jax.experimental import pallas as pl
from jax.experimental.pallas import tpu as pltpu
from jax.sharding import PartitionSpec as P

MESH = pl.DeviceIdType.MESH
BF = jnp.bfloat16
F32 = jnp.float32

HEAD_WIDTH = 128
SEQ = 384
TOK = 64
CHUNKS = 4
NX, NY, NZ = 4, 4, 8
LANES = 256
ROWS = 208
PART = 200
vision_epsilon = 1e-06
decoder_epsilon = 1e-05
rope_base = 500000.0

STARTS = (0, 0, 2, 3, 4)
SLOTS = max(STARTS) + 5


def dot(a, b):
    return jnp.dot(a, b, preferred_element_type=F32)


def lane_of(shape):
    return lax.broadcasted_iota(jnp.int32, shape, len(shape) - 1)


def row_of(shape):
    return lax.broadcasted_iota(jnp.int32, shape, len(shape) - 2)


def kernel(
    cnt_ref, off_ref, vis_ref, affine_ref, proj_ref, qkv_ref, raw_ref, attn_ref, cos_ref, sin_ref,
    out_ref,
    wp, wq, vis_all, vis_own, stats, image_stats, text_ref, pick_ref, sel_ref, acts, vs, im, ia,
    v_fo, v_fi, v_no, v_ni, v_own, i_fo, i_fi, i_no, i_ni, i_own, t_fo, t_fi, t_no, t_ni, t_own,
    a2s, a2r, vis_col, text_mid, im_col, relay_y, relay_x,
    l_sem, z_s, z_r, st_s, st_r, ys_s, ys_r, xs_s, xs_r, tx_s, tx_r, d_s, d_r, f_s, f_r, g_s, g_r, n_s, n_r,
    a_s, a_r,
):
    dp = lax.axis_index("dp")
    tn = lax.axis_index("tensor")
    x, z = dp // NZ, dp % NZ
    y, c = tn // 2, tn % 2
    pending = []

    def remote(src, dst, ssem, rsem, to):
        return pltpu.make_async_remote_copy(
            src_ref=src, dst_ref=dst, send_sem=ssem, recv_sem=rsem, device_id=to,
            device_id_type=MESH,
        )

    def send(src, dst, ssem, rsem, to):
        copy = remote(src, dst, ssem, rsem, to)
        copy.start()
        pending.append(copy)

    here = (dp, tn)

    def arrived(ref, ssem, rsem):
        remote(ref, ref, ssem, rsem, here).wait_recv()

    def own(u):
        return proj_ref.at[u] if u < 2 else qkv_ref.at[u - 2]

    def slot_ref(u, source):
        if u < 2:
            return wp.at[u, source, pl.ds(0, ROWS)]
        return wq.at[u - 2, source]

    def goes(u, e, k):
        return k < 4 or (u % 2 == e)

    def ring(slot):
        for u, start in enumerate(STARTS):
            k = slot - start
            if k < 0 or k > 4:
                continue
            for e in range(2):
                sign = 1 if e == 0 else -1
                source = (z - sign * k + 2 * NZ) % NZ
                if k >= 1 and goes(u, e, k):
                    arrived(slot_ref(u, source), z_s.at[u, e, k - 1], z_r.at[u, e, k - 1])
                if k <= 3 and goes(u, e, k + 1):
                    to = (x * NZ + (z + sign + NZ) % NZ, tn)
                    src = own(u) if k == 0 else slot_ref(u, source)
                    send(src, slot_ref(u, source), z_s.at[u, e, k], z_r.at[u, e, k], to)

    class Spread:
        def __init__(self, kind, own, column, place):
            self.kind, self.own, self.column, self.place = kind, own, column, place

        def on_y(self, src, slot, h, step):
            k = self.kind
            send(src, self.column(slot, h), ys_s.at[k, slot, h], ys_r.at[k, slot, h],
                 (dp, ((y + step + NY) % NY) * 2 + c))

        def on_x(self, src, j, h, kappa):
            k = self.kind
            copy = remote(src, self.place(c, x, h), xs_s.at[k, j, h], xs_r.at[k, x, h],
                          (kappa * NZ + z, tn))
            local = pltpu.make_async_copy(src, self.place(c, x, h), xs_r.at[k, x, h])

            @pl.when(kappa != x)
            def _():
                copy.start()

            @pl.when(kappa == x)
            def _():
                local.start()

            later.append((copy, kappa != x))

        def begin_y(self):
            for h in range(2):
                self.on_y(self.own(h), 0, h, 1)
                self.on_y(self.own(h), 1, h, -1)

        def begin_x(self):
            for h in range(2):
                self.on_x(self.own(h), 3, h, y)

        def near(self, h):
            k = self.kind
            for slot, step in ((0, 1), (1, -1)):
                arrived(self.column(slot, h), ys_s.at[k, slot, h], ys_r.at[k, slot, h])
                if slot == h:
                    src = self.column(slot, h)
                    send(src, self.column(2, h), ys_s.at[k, 2, h], ys_r.at[k, 2, h],
                         (dp, ((y + step + NY) % NY) * 2 + c))
            for slot, step in ((0, 1), (1, -1)):
                self.on_x(self.column(slot, h), slot, h, (y - step + NY) % NY)

        def far(self, h):
            k = self.kind
            arrived(self.column(2, h), ys_s.at[k, 2, h], ys_r.at[k, 2, h])
            self.on_x(self.column(2, h), 2, h, (y + 2) % NY)

        def to_sibling(self, offsets=(0, 1, 3, 2)):
            k = self.kind
            for o in offsets:
                s = (x + o) % NX
                for h in range(2):
                    ref = self.place(c, s, h)
                    arrived(ref, xs_s.at[k, 0, h], xs_r.at[k, s, h])
                    send(ref, ref, d_s.at[k, s, h], d_r.at[k, s, h], (dp, tn + 1 - 2 * c))

        def from_sibling(self):
            k = self.kind
            for s in range(NX):
                for h in range(2):
                    arrived(self.place(1 - c, s, h), d_s.at[k, s, h], d_r.at[k, s, h])

    later = []
    vis_spread = Spread(
        0,
        lambda h: vis_own.at[pl.ds(2 * h, 2)],
        lambda j, h: vis_col.at[j, pl.ds(2 * h, 2)],
        lambda core, s, h: vis_all.at[pl.ds(4 * core + 2 * h, 2), s],
    )
    def crossed(a, b):
        return ((a // 2 + b // 2) % 2) * 2 + (a + b) % 2

    class TextSpread:
        def part(self, q):
            return pl.ds(q * (SEQ // CHUNKS), SEQ // CHUNKS)

        def block(self, core, step, q):
            return acts.at[core, crossed(x, (y + step + NY) % NY), self.part(q)]

        def hop(self, q, at, src, dst, relay, kind, along):
            other = x if along == "y" else y

            def device(place):
                return (dp, place * 2 + c) if along == "y" else (place * NZ + z, tn)

            ssem, rsem = tx_s.at[kind, q], tx_r.at[kind, q]
            straight = remote(src, dst, ssem, rsem, device(crossed(at, other)))
            local = pltpu.make_async_copy(src, dst, rsem)
            beside = device((at + (1 if q % 2 == 0 else 3)) % 4)
            via = remote(src, relay.at[q], ssem, tx_r.at[kind + 1, q], beside)

            @pl.when(other == 0)
            def _():
                local.start()

            @pl.when((other == 1) | (other == 3))
            def _():
                straight.start()

            @pl.when(other == 2)
            def _():
                via.start()

            later.append((straight, other != 0))

        def relay(self, q, at, dst, relay, kind, along):
            other = x if along == "y" else y
            nxt = (at + (1 if q % 2 == 0 else 3)) % 4
            to = (dp, nxt * 2 + c) if along == "y" else (nxt * NZ + z, tn)
            on = remote(relay.at[q], dst, tx_s.at[kind + 1, q], tx_r.at[kind, q], to)

            @pl.when(other == 2)
            def _():
                remote(relay.at[q], relay.at[q], tx_s.at[kind + 1, q], tx_r.at[kind + 1, q],
                       here).wait_recv()
                on.start()

            later.append((on, other == 2))

        def begin(self):
            for q in range(CHUNKS):
                self.hop(q, y, text_ref.at[self.part(q)], text_mid.at[self.part(q)], relay_y, 0, "y")

        def pass_y(self, q):
            self.relay(q, y, text_mid.at[self.part(q)], relay_y, 0, "y")

        def turn(self, q):
            mid = text_mid.at[self.part(q)]
            arrived(mid, tx_s.at[0, q], tx_r.at[0, q])
            self.hop(q, x, mid, acts.at[c, x, self.part(q)], relay_x, 2, "x")

        def pass_x(self, q):
            source = (x + (3 if q % 2 == 0 else 1)) % NX
            self.relay(q, x, acts.at[c, source, self.part(q)], relay_x, 2, "x")

        def on_y(self, q, block_step, step, kind):
            ref = self.block(c, block_step, q)
            send(ref, ref, tx_s.at[kind, q], tx_r.at[kind, q], (dp, ((y + step + NY) % NY) * 2 + c))

        def to_other(self, q, j, step):
            ref = self.block(c, step, q)
            send(ref, ref, d_s.at[1, j, q], d_r.at[1, j, q], (dp, tn + 1 - 2 * c))

        def mine(self, q):
            arrived(self.block(c, 0, q), tx_s.at[2, q], tx_r.at[2, q])
            self.on_y(q, 0, 1, 4)
            self.on_y(q, 0, -1, 5)
            self.to_other(q, 0, 0)

        def near(self, q):
            arrived(self.block(c, -1, q), tx_s.at[4, q], tx_r.at[4, q])
            arrived(self.block(c, 1, q), tx_s.at[5, q], tx_r.at[5, q])
            if q % 2 == 0:
                self.on_y(q, -1, 1, 6)
            else:
                self.on_y(q, 1, -1, 6)
            self.to_other(q, 1, -1)
            self.to_other(q, 2, 1)

        def far(self, q):
            arrived(self.block(c, 2, q), tx_s.at[6, q], tx_r.at[6, q])
            self.to_other(q, 3, 2)

        def from_sibling(self):
            for q in range(CHUNKS):
                for j, step in enumerate((0, -1, 1, 2)):
                    arrived(self.block(1 - c, step, q), d_s.at[1, j, q], d_r.at[1, j, q])

    text_spread = TextSpread()
    image_spread = Spread(
        2,
        lambda h: im.at[pl.ds(32 * h, 32)],
        lambda j, h: im_col.at[j, pl.ds(32 * h, 32)],
        lambda core, s, h: ia.at[core, s, pl.ds(32 * h, 32)],
    )

    def along_x(o):
        return (((x + o) % NX) * NZ + z, tn)

    barrier = pltpu.get_barrier_semaphore()

    def greet_dp(o, carry):
        pl.semaphore_signal(barrier, inc=1, device_id=((dp + o) % 32, tn), device_id_type=MESH)
        return carry

    def greet_tensor(o, carry):
        pl.semaphore_signal(barrier, inc=1, device_id=(dp, (tn + o) % 8), device_id_type=MESH)
        return carry

    lax.fori_loop(1, 32, greet_dp, 0)
    lax.fori_loop(1, 8, greet_tensor, 0)

    for u in range(2):
        for s in range(NZ):
            wp[u, s, ROWS:LANES, :] = jnp.zeros((LANES - ROWS, 512), BF)
    locals_ = []
    for u in range(5):
        local = pltpu.make_async_copy(own(u), slot_ref(u, z), l_sem.at[u])
        local.start()
        locals_.append(local)

    def lines_of(column):
        rows = column.shape[0]
        wide = jnp.broadcast_to(column, (rows, 128))
        if rows % 128:
            wide = jnp.concatenate([wide, jnp.zeros((128 - rows % 128, 128), F32)], axis=0)
        return [wide[128 * b : 128 * b + 128].T[0:1] for b in range(wide.shape[0] // 128)]

    def column_of(lines, rows):
        wide = [jnp.broadcast_to(line, (128, 128)).T for line in lines]
        wide = wide[0] if len(wide) == 1 else jnp.concatenate(wide, axis=0)
        return wide[0:rows, 0:1]

    xv = vis_ref[...].astype(F32)
    mean = jnp.sum(jnp.sum(xv, axis=0), axis=-1, keepdims=True) / (4 * PART)
    centred = jnp.where(lane_of(xv.shape) < PART, xv - mean[None], 0.0)
    m2 = jnp.sum(jnp.sum(centred * centred, axis=0), axis=-1, keepdims=True)
    raw = raw_ref[...].astype(F32)
    lines = lines_of(jnp.sum(raw * raw, axis=-1, keepdims=True)) + lines_of(mean) + lines_of(m2)
    stats[tn] = jnp.concatenate(lines + [jnp.zeros((3, 128), F32)], axis=0)

    first = jnp.int32(0)
    my_first = jnp.int32(0)
    my_count = jnp.int32(0)
    owners = [jnp.int32(0)] * 8
    for s in range(NX * NZ):
        count = cnt_ref[s]
        my_first = my_first + jnp.where(s < dp, count, 0)
        my_count = my_count + jnp.where(s == dp, count, 0)
        first = first + count
        owners = [a + jnp.where(first <= r * 32 + dp, 1, 0) for r, a in enumerate(owners)]
    shape = (512, 128)
    row, col = row_of(shape), lane_of(shape)
    owner = jnp.zeros(shape, jnp.int32)
    for r in range(8):
        owner = jnp.where(((col >> 3) & 7) == r, owners[r], owner)
    same = ((row >> 4) == owner) & (((row >> 3) & 1) == (col >> 6)) & ((row & 7) == (col & 7))
    pick_ref[...] = jnp.where(same, 1.0, 0.0).astype(BF)
    shape = (SEQ, 512)
    row, col = row_of(shape), lane_of(shape)
    place = row - off_ref[0]
    inside = (place >= 0) & (place < 8 * my_count)
    source = (my_first + (place >> 3)) & 31
    match = inside & ((col >> 4) == source) & ((col & 7) == (place & 7))
    for h in range(2):
        chosen = match & (((col >> 3) & 1) == h)
        sel_ref[h] = jnp.where(chosen, 1.0, 0.0).astype(BF)
    place = row_of((SEQ, 128)) - off_ref[0]
    is_image = (place >= 0) & (place < 8 * my_count)

    pl.semaphore_wait(barrier, 38)
    for o in range(1, 8):
        send(stats.at[tn], stats.at[tn], st_s.at[o - 1], st_r.at[o - 1], (dp, (tn + o) % 8))
    ring(0)
    for o in range(1, 8):
        arrived(stats.at[(tn - o + 8) % 8], st_s.at[o - 1], st_r.at[o - 1])
    means = [stats[t][3:4] for t in range(8)]
    mean = sum(means[1:], means[0]) / 8.0
    total = jnp.zeros((1, 128), F32)
    for t in range(8):
        apart = means[t] - mean
        total = total + stats[t][4:5] + (4.0 * PART) * apart * apart
    scale = column_of([lax.rsqrt(total / (32.0 * PART) + vision_epsilon)], TOK)
    mean = column_of([mean], TOK)
    for i in range(4):
        piece = vis_ref[i].astype(F32)
        vis_own[i] = ((piece - mean) * scale * affine_ref[0, i] + affine_ref[1, i]).astype(BF)
    vis_spread.begin_y()
    vis_spread.begin_x()
    total = stats[0]
    for t in range(1, 8):
        total = total + stats[t]
    scale = lax.rsqrt(total / 8192.0 + decoder_epsilon)
    scale = column_of([scale[b : b + 1] for b in range(3)], SEQ)
    gain = attn_ref[:, pl.ds(pl.multiple_of(tn * 1024, 1024), 1024)]
    text_ref[...] = (raw_ref[...].astype(F32) * scale * gain).astype(BF)
    text_spread.begin()

    class Reduce:
        def __init__(self, index, far_out, far_in, near_out, near_in, own, value):
            self.i, self.value, self.own = index, value, own
            self.far_out, self.far_in = far_out, far_in
            self.near_out, self.near_in = near_out, near_in
            self.half = far_out.shape[0] // 2

        def opposite(self):
            i, half = self.i, self.half
            self.far_out[...] = self.value(2).astype(BF)
            for h in range(2):
                part = pl.ds(half * h, half)
                send(self.far_out.at[part], self.far_in.at[part], f_s.at[i, h], f_r.at[i, h],
                     along_x(1 if h == 0 else 3))
            self.own[...] = self.value(0)

        def neighbours(self):
            i, half = self.i, self.half
            for h in range(2):
                part = pl.ds(half * h, half)
                rest = pl.ds(half * (1 - h), half)
                o = 1 if h == 0 else 3
                value = self.value(o)
                arrived(self.far_in.at[part], f_s.at[i, h], f_r.at[i, h])
                mine = value[half * h : half * h + half] + self.far_in[part, :].astype(F32)
                self.near_out[h, part, :] = mine.astype(BF)
                self.near_out[h, rest, :] = value[half * (1 - h) : half * (1 - h) + half].astype(BF)
                send(self.near_out.at[h], self.near_in.at[h], g_s.at[i, h], g_r.at[i, h], along_x(o))

        def total(self):
            i = self.i
            acc = self.own[...]
            for h in range(2):
                arrived(self.near_in.at[h], g_s.at[i, h], g_r.at[i, h])
                acc = acc + self.near_in[h].astype(F32)
            return acc

    def project(source, u, o):
        s = (x + o) % NX
        first = dot(source[0, s], wq[u, 0:4].reshape(1024, 256))
        return first + dot(source[1, s], wq[u, 4:8].reshape(1024, 256))

    vis_reduce = Reduce(0, v_fo, v_fi, v_no, v_ni, v_own, lambda o: vs[(x + o) % NX])
    image_reduce = Reduce(
        1, i_fo, i_fi, i_no, i_ni, i_own,
        lambda o: jnp.concatenate([project(ia, u, o) for u in range(3)], axis=1),
    )
    text_reduce = [
        Reduce(2 + u, t_fo.at[u], t_fi.at[u], t_no.at[u], t_ni.at[u], t_own.at[u],
               lambda o, u=u: project(acts, u, o))
        for u in range(3)
    ]

    def vision():
        vis_spread.from_sibling()
        for h in range(2):
            acc = None
            for s in range(NZ):
                term = dot(vis_all[s].reshape(NX * TOK, LANES), wp[h, s])
                acc = term if acc is None else acc + term
            vs[:, :, 512 * h : 512 * h + 512] = acc.reshape(NX, TOK, 512)

    def image():
        tokens = vis_reduce.total().astype(BF).astype(F32)
        lines = lines_of(jnp.sum(tokens * tokens, axis=-1, keepdims=True))
        image_stats[tn] = jnp.concatenate(lines + [jnp.zeros((7, 128), F32)], axis=0)
        im[...] = (tokens * gain).astype(BF)
        image_spread.begin_y()
        image_spread.begin_x()
        for o in range(1, 8):
            send(image_stats.at[tn], image_stats.at[tn], n_s.at[o - 1], n_r.at[o - 1],
                 (dp, (tn + o) % 8))

    def locals_done(us):
        for u in us:
            locals_[u].wait()

    vis_spread.near(0)
    vis_spread.near(1)
    ring(1)
    text_spread.pass_y(0)
    text_spread.pass_y(1)
    text_spread.turn(0)
    text_spread.turn(1)
    ring(2)
    text_spread.pass_y(2)
    text_spread.pass_y(3)
    text_spread.turn(2)
    text_spread.turn(3)
    vis_spread.far(0)
    vis_spread.far(1)
    text_spread.pass_x(0)
    text_spread.pass_x(1)
    text_spread.mine(0)
    text_spread.mine(1)
    ring(3)
    text_spread.pass_x(2)
    text_spread.pass_x(3)
    text_spread.mine(2)
    text_spread.mine(3)
    vis_spread.to_sibling()
    text_spread.near(0)
    ring(4)
    locals_done((0, 1))
    vision()
    vis_reduce.opposite()
    text_spread.near(1)
    text_spread.near(2)
    vis_reduce.neighbours()
    text_spread.near(3)
    ring(5)
    text_spread.far(0)
    text_spread.far(1)
    image()
    ring(6)
    text_spread.far(2)
    text_spread.far(3)
    image_spread.near(0)
    image_spread.near(1)
    text_spread.from_sibling()
    locals_done((2, 3, 4))
    text_reduce[0].opposite()
    ring(7)
    image_spread.far(0)
    image_spread.far(1)
    text_reduce[1].opposite()
    text_reduce[0].neighbours()
    ring(8)
    image_spread.to_sibling()
    text_reduce[2].opposite()
    image_spread.from_sibling()
    image_reduce.opposite()
    text_reduce[1].neighbours()
    image_reduce.neighbours()
    text_reduce[2].neighbours()

    total = image_stats[tn]
    for o in range(1, 8):
        source = (tn - o + 8) % 8
        arrived(image_stats.at[source], n_s.at[o - 1], n_r.at[o - 1])
        total = total + image_stats[source]
    image_scale = column_of([lax.rsqrt(total[0:1] / 8192.0 + decoder_epsilon)], TOK)
    image_rows = (image_reduce.total() * image_scale).astype(BF)
    low, high = image_rows[:, 0:384], image_rows[:, 384:768]
    both = jnp.concatenate([low, high], axis=0)
    a2s[...] = dot(pick_ref[...], both).astype(BF).reshape(32, 16, 384)
    a2r[dp] = a2s[dp]

    def route(o, carry):
        to = (dp + o) % 32
        remote(a2s.at[to], a2r.at[dp], a_s.at[o - 1], a_r.at[o - 1], (to, tn)).start()
        return carry

    lax.fori_loop(1, 32, route, 0)

    causal = row_of((SEQ, SEQ)) >= lane_of((SEQ, SEQ))

    def route_done(o, carry):
        source = (dp - o + 32) % 32
        remote(a2s.at[source], a2r.at[source], a_s.at[o - 1], a_r.at[o - 1], here).wait_recv()
        return carry

    lax.fori_loop(1, 32, route_done, 0)
    routed = a2r[...].reshape(512, 384)
    image_low = dot(sel_ref[0], routed)
    image_high = dot(sel_ref[1], routed)

    texts = [text_reduce[u].total() for u in range(3)]
    cos, sin = cos_ref[...], sin_ref[...]

    def column(i):
        text = texts[i // 2][:, 128 * (i % 2) : 128 * (i % 2) + 128]
        picture = image_low if i < 3 else image_high
        picture = picture[:, 128 * (i % 3) : 128 * (i % 3) + 128]
        return jnp.where(is_image, picture, text)

    def turned(value):
        return (value * cos + pltpu.roll(value, 64, 1) * sin).astype(BF)

    key = turned(column(4))
    value = column(5).astype(BF)
    for h in range(4):
        query = turned(column(h))
        scores = lax.dot_general(query, key, (((1,), (1,)), ((), ())), preferred_element_type=F32)
        scores = jnp.where(causal, scores * HEAD_WIDTH ** (-0.5), -1e30)
        powers = jnp.exp(scores - jnp.max(scores, axis=-1, keepdims=True))
        weights = (powers / jnp.sum(powers, axis=-1, keepdims=True)).astype(BF)
        out_ref[:, 128 * h : 128 * h + 128] = dot(weights, value).astype(BF)

    for copy in pending:
        copy.wait_send()
    for copy, went in later:

        @pl.when(went)
        def _(copy=copy):
            copy.wait_send()


    def sent(o, carry):
        to = (dp + o) % 32
        remote(a2s.at[to], a2r.at[dp], a_s.at[o - 1], a_r.at[o - 1], here).wait_send()
        return carry

    lax.fori_loop(1, 32, sent, 0)


def rotation_tables():
    exponents = np.arange(64, dtype=np.float32) * np.float32(2.0 / 128)
    frequency = np.float32(rope_base) ** (-exponents)
    angles = np.arange(SEQ, dtype=np.float32)[:, None] * frequency[None, :]
    cos, sin = np.cos(angles), np.sin(angles)
    return (
        np.concatenate([cos, cos], axis=1).astype(np.float32),
        np.concatenate([-sin, sin], axis=1).astype(np.float32),
    )


def per_device(vis_rows, ln_gain, ln_bias, proj_weight, text_rows, attn_gain, w_query,
               key_value_weight, tile_counts, image_offsets):
    tn = lax.axis_index("tensor")

    def lanes(a):
        return jnp.pad(a, [(0, 0)] * (a.ndim - 1) + [(0, LANES - PART)])

    vis = vis_rows.reshape(TOK, 2, 4, 100).transpose(2, 0, 3, 1).reshape(4, TOK, PART)
    vis = lanes(vis)

    affine = jnp.stack([ln_gain, ln_bias])
    affine = lax.dynamic_slice_in_dim(affine, tn * 400, 400, 2)
    affine = lanes(affine.reshape(2, 2, 4, 100).transpose(0, 2, 3, 1).reshape(2, 4, 1, PART))

    proj = jnp.pad(proj_weight.reshape(PART, 1024), ((0, ROWS - PART), (0, 0)))
    proj = proj.reshape(ROWS, 2, 512).transpose(1, 0, 2)
    qkv = jnp.concatenate([w_query, key_value_weight.reshape(256, 256)], axis=1)
    qkv = qkv.reshape(256, 3, 256).transpose(1, 0, 2)
    cos, sin = rotation_tables()
    vmem = pl.BlockSpec(memory_space=pltpu.VMEM)
    smem = pl.BlockSpec(memory_space=pltpu.SMEM)
    dma = pltpu.SemaphoreType.DMA
    out = pl.pallas_call(
        kernel,
        out_shape=jax.ShapeDtypeStruct((SEQ, 512), BF),
        in_specs=[smem, smem] + [vmem] * 8,
        out_specs=vmem,
        scratch_shapes=[
            pltpu.VMEM((2, NZ, LANES, 512), BF),
            pltpu.VMEM((3, NZ, 256, 256), BF),
            pltpu.VMEM((NZ, NX, TOK, LANES), BF),
            pltpu.VMEM((4, TOK, LANES), BF),
            pltpu.VMEM((8, 8, 128), F32),
            pltpu.VMEM((8, 8, 128), F32),
            pltpu.VMEM((SEQ, 1024), BF),
            pltpu.VMEM((512, 128), BF),
            pltpu.VMEM((2, SEQ, 512), BF),
            pltpu.VMEM((2, NX, SEQ, 1024), BF),
            pltpu.VMEM((NX, TOK, 1024), F32),
            pltpu.VMEM((TOK, 1024), BF),
            pltpu.VMEM((2, NX, TOK, 1024), BF),
            pltpu.VMEM((TOK, 1024), BF),
            pltpu.VMEM((TOK, 1024), BF),
            pltpu.VMEM((2, TOK, 1024), BF),
            pltpu.VMEM((2, TOK, 1024), BF),
            pltpu.VMEM((TOK, 1024), F32),
            pltpu.VMEM((TOK, 768), BF),
            pltpu.VMEM((TOK, 768), BF),
            pltpu.VMEM((2, TOK, 768), BF),
            pltpu.VMEM((2, TOK, 768), BF),
            pltpu.VMEM((TOK, 768), F32),
            pltpu.VMEM((3, SEQ, 256), BF),
            pltpu.VMEM((3, SEQ, 256), BF),
            pltpu.VMEM((3, 2, SEQ, 256), BF),
            pltpu.VMEM((3, 2, SEQ, 256), BF),
            pltpu.VMEM((3, SEQ, 256), F32),
            pltpu.VMEM((32, 16, 384), BF),
            pltpu.VMEM((32, 16, 384), BF),
            pltpu.VMEM((3, 4, TOK, LANES), BF),
            pltpu.VMEM((SEQ, 1024), BF),
            pltpu.VMEM((3, TOK, 1024), BF),
            pltpu.VMEM((CHUNKS, SEQ // CHUNKS, 1024), BF),
            pltpu.VMEM((CHUNKS, SEQ // CHUNKS, 1024), BF),
            dma((5,)),
            dma((5, 2, 4)),
            dma((5, 2, 4)),
            dma((7,)),
            dma((7,)),
            dma((3, 3, 2)),
            dma((3, 3, 2)),
            dma((3, 4, 2)),
            dma((3, NX, 2)),
            dma((7, CHUNKS)),
            dma((7, CHUNKS)),
            dma((3, NX, 4)),
            dma((3, NX, 4)),
            dma((5, 2)),
            dma((5, 2)),
            dma((5, 2)),
            dma((5, 2)),
            dma((7,)),
            dma((7,)),
            dma((31,)),
            dma((31,)),
        ],
        compiler_params=pltpu.CompilerParams(collective_id=0, has_side_effects=True, vmem_limit_bytes=40 << 20),
        name="step",
    )(tile_counts, image_offsets, vis, affine, proj, qkv, text_rows[0],
      attn_gain[None], jnp.asarray(cos), jnp.asarray(sin))
    return out[None]


def solution(mesh):
    in_specs = (
        P(None, "dp", None, "tensor"),
        P(),
        P(),
        P("dp", None, "tensor"),
        P("dp", None, "tensor"),
        P(),
        P("dp", "tensor"),
        P("dp", None, "tensor"),
        P(),
        P("dp"),
    )
    return jax.shard_map(per_device, mesh=mesh, in_specs=in_specs,
                         out_specs=P("dp", None, "tensor"), check_vma=False)
```

```python
import functools

import jax
import jax.numpy as jnp
import numpy as np
from jax import lax
from jax.experimental import pallas as pl
from jax.experimental.pallas import tpu as pltpu
from jax.sharding import PartitionSpec as P

MESH = pl.DeviceIdType.MESH
BF = jnp.bfloat16
F32 = jnp.float32

HEAD_WIDTH = 128
SEQ = 384
TOK = 64
CHUNKS = 4
ROW_FOR = ((0, 2, 3, 1), (1, 3, 2, 0), (3, 0, 1, 2), (2, 1, 0, 3))
COLUMN_FOR = tuple(tuple(row.index(r) for r in range(4)) for row in ROW_FOR)
SAMPLE_AT = tuple(tuple([row[k] for row in ROW_FOR].index(r) for r in range(4)) for k in range(4))
NX, NY, NZ = 4, 4, 8
LANES = 256
ROWS = 208
PART = 200
vision_epsilon = 1e-06
decoder_epsilon = 1e-05
rope_base = 500000.0

STARTS = (0, 0, 2, 3, 4)
SLOTS = max(STARTS) + 5


def dot(a, b):
    return jnp.dot(a, b, preferred_element_type=F32)


def lane_of(shape):
    return lax.broadcasted_iota(jnp.int32, shape, len(shape) - 1)


def row_of(shape):
    return lax.broadcasted_iota(jnp.int32, shape, len(shape) - 2)


def kernel(
    cnt_ref, off_ref, vis_ref, affine_ref, proj_ref, qkv_ref, raw_ref, attn_ref, cos_ref, sin_ref,
    out_ref,
    wp, wq, vis_all, vis_own, stats, image_stats, text_ref, pick_ref, sel_ref, acts, vs, im, ia,
    v_fo, v_fi, v_no, v_ni, v_own, i_fo, i_fi, i_no, i_ni, i_own, t_fo, t_fi, t_no, t_ni, t_own,
    a2s, a2r, vis_col, text_mid, im_col,
    l_sem, z_s, z_r, st_s, st_r, ys_s, ys_r, xs_s, xs_r, tx_s, tx_r, d_s, d_r, f_s, f_r, g_s, g_r, n_s, n_r,
    a_s, a_r,
):
    dp = lax.axis_index("dp")
    tn = lax.axis_index("tensor")
    x, z = dp // NZ, dp % NZ
    y, c = tn // 2, tn % 2
    pending = []

    def remote(src, dst, ssem, rsem, to):
        return pltpu.make_async_remote_copy(
            src_ref=src, dst_ref=dst, send_sem=ssem, recv_sem=rsem, device_id=to,
            device_id_type=MESH,
        )

    def send(src, dst, ssem, rsem, to):
        copy = remote(src, dst, ssem, rsem, to)
        copy.start()
        pending.append(copy)

    here = (dp, tn)

    def arrived(ref, ssem, rsem):
        remote(ref, ref, ssem, rsem, here).wait_recv()

    def own(u):
        return proj_ref.at[u] if u < 2 else qkv_ref.at[u - 2]

    def slot_ref(u, source):
        if u < 2:
            return wp.at[u, source, pl.ds(0, ROWS)]
        return wq.at[u - 2, source]

    def goes(u, e, k):
        return k < 4 or (u % 2 == e)

    def ring(slot):
        for u, start in enumerate(STARTS):
            k = slot - start
            if k < 0 or k > 4:
                continue
            for e in range(2):
                sign = 1 if e == 0 else -1
                source = (z - sign * k + 2 * NZ) % NZ
                if k >= 1 and goes(u, e, k):
                    arrived(slot_ref(u, source), z_s.at[u, e, k - 1], z_r.at[u, e, k - 1])
                if k <= 3 and goes(u, e, k + 1):
                    to = (x * NZ + (z + sign + NZ) % NZ, tn)
                    src = own(u) if k == 0 else slot_ref(u, source)
                    send(src, slot_ref(u, source), z_s.at[u, e, k], z_r.at[u, e, k], to)

    class Spread:
        def __init__(self, kind, own, column, place):
            self.kind, self.own, self.column, self.place = kind, own, column, place

        def on_y(self, src, slot, h, step):
            k = self.kind
            send(src, self.column(slot, h), ys_s.at[k, slot, h], ys_r.at[k, slot, h],
                 (dp, ((y + step + NY) % NY) * 2 + c))

        def on_x(self, src, j, h, kappa):
            k = self.kind
            copy = remote(src, self.place(c, x, h), xs_s.at[k, j, h], xs_r.at[k, x, h],
                          (kappa * NZ + z, tn))
            local = pltpu.make_async_copy(src, self.place(c, x, h), xs_r.at[k, x, h])

            @pl.when(kappa != x)
            def _():
                copy.start()

            @pl.when(kappa == x)
            def _():
                local.start()

            later.append((copy, kappa != x))

        def begin_y(self):
            for h in range(2):
                self.on_y(self.own(h), 0, h, 1)
                self.on_y(self.own(h), 1, h, -1)

        def begin_x(self):
            for h in range(2):
                self.on_x(self.own(h), 3, h, y)

        def near(self, h):
            k = self.kind
            for slot, step in ((0, 1), (1, -1)):
                arrived(self.column(slot, h), ys_s.at[k, slot, h], ys_r.at[k, slot, h])
                if slot == h:
                    src = self.column(slot, h)
                    send(src, self.column(2, h), ys_s.at[k, 2, h], ys_r.at[k, 2, h],
                         (dp, ((y + step + NY) % NY) * 2 + c))
            for slot, step in ((0, 1), (1, -1)):
                self.on_x(self.column(slot, h), slot, h, (y - step + NY) % NY)

        def far(self, h):
            k = self.kind
            arrived(self.column(2, h), ys_s.at[k, 2, h], ys_r.at[k, 2, h])
            self.on_x(self.column(2, h), 2, h, (y + 2) % NY)

        def to_sibling(self, offsets=(0, 1, 3, 2)):
            k = self.kind
            for o in offsets:
                s = (x + o) % NX
                for h in range(2):
                    ref = self.place(c, s, h)
                    arrived(ref, xs_s.at[k, 0, h], xs_r.at[k, s, h])
                    send(ref, ref, d_s.at[k, s, h], d_r.at[k, s, h], (dp, tn + 1 - 2 * c))

        def from_sibling(self):
            k = self.kind
            for s in range(NX):
                for h in range(2):
                    arrived(self.place(1 - c, s, h), d_s.at[k, s, h], d_r.at[k, s, h])

    later = []
    vis_spread = Spread(
        0,
        lambda h: vis_own.at[pl.ds(2 * h, 2)],
        lambda j, h: vis_col.at[j, pl.ds(2 * h, 2)],
        lambda core, s, h: vis_all.at[pl.ds(4 * core + 2 * h, 2), s],
    )
    def entry(rows, a, b):
        value = jnp.int32(0)
        for i, row in enumerate(rows):
            for j, v in enumerate(row):
                value = value + jnp.where((a == i) & (b == j), v, 0)
        return value

    class TextSpread:
        def __init__(self):
            self.row = entry(ROW_FOR, x, y)
            self.column = entry(COLUMN_FOR, x, y)
            self.sample = {step: entry(SAMPLE_AT, x, (y + step + NY) % NY) for step in (0, -1, 1, 2)}

        def part(self, q):
            return pl.ds(q * (SEQ // CHUNKS), SEQ // CHUNKS)

        def block(self, core, step, q):
            return acts.at[core, self.sample[step], self.part(q)]

        def hop(self, q, stays, src, dst, kind, to):
            ssem, rsem = tx_s.at[kind, q], tx_r.at[kind, q]
            copy = remote(src, dst, ssem, rsem, to)
            local = pltpu.make_async_copy(src, dst, rsem)

            @pl.when(stays)
            def _():
                local.start()

            @pl.when(jnp.logical_not(stays))
            def _():
                copy.start()

            later.append((copy, jnp.logical_not(stays)))

        def begin(self):
            for q in range(CHUNKS):
                part = self.part(q)
                self.hop(q, self.row == y, text_ref.at[part], text_mid.at[part], 0,
                         (dp, self.row * 2 + c))

        def turn(self, q):
            mid = text_mid.at[self.part(q)]
            arrived(mid, tx_s.at[0, q], tx_r.at[0, q])
            self.hop(q, self.column == x, mid, acts.at[c, x, self.part(q)], 2,
                     (self.column * NZ + z, tn))

        def on_y(self, q, block_step, step, kind):
            ref = self.block(c, block_step, q)
            send(ref, ref, tx_s.at[kind, q], tx_r.at[kind, q], (dp, ((y + step + NY) % NY) * 2 + c))

        def to_other(self, q, j, step):
            ref = self.block(c, step, q)
            send(ref, ref, d_s.at[1, j, q], d_r.at[1, j, q], (dp, tn + 1 - 2 * c))

        def mine(self, q):
            arrived(self.block(c, 0, q), tx_s.at[2, q], tx_r.at[2, q])
            self.on_y(q, 0, 1, 4)
            self.on_y(q, 0, -1, 5)
            self.to_other(q, 0, 0)

        def near(self, q):
            arrived(self.block(c, -1, q), tx_s.at[4, q], tx_r.at[4, q])
            arrived(self.block(c, 1, q), tx_s.at[5, q], tx_r.at[5, q])
            if q % 2 == 0:
                self.on_y(q, -1, 1, 6)
            else:
                self.on_y(q, 1, -1, 6)
            self.to_other(q, 1, -1)
            self.to_other(q, 2, 1)

        def far(self, q):
            arrived(self.block(c, 2, q), tx_s.at[6, q], tx_r.at[6, q])
            self.to_other(q, 3, 2)

        def from_sibling(self):
            for q in range(CHUNKS):
                for j, step in enumerate((0, -1, 1, 2)):
                    arrived(self.block(1 - c, step, q), d_s.at[1, j, q], d_r.at[1, j, q])

    text_spread = TextSpread()
    image_spread = Spread(
        2,
        lambda h: im.at[pl.ds(32 * h, 32)],
        lambda j, h: im_col.at[j, pl.ds(32 * h, 32)],
        lambda core, s, h: ia.at[core, s, pl.ds(32 * h, 32)],
    )

    def along_x(o):
        return (((x + o) % NX) * NZ + z, tn)

    barrier = pltpu.get_barrier_semaphore()

    def greet_dp(o, carry):
        pl.semaphore_signal(barrier, inc=1, device_id=((dp + o) % 32, tn), device_id_type=MESH)
        return carry

    def greet_tensor(o, carry):
        pl.semaphore_signal(barrier, inc=1, device_id=(dp, (tn + o) % 8), device_id_type=MESH)
        return carry

    lax.fori_loop(1, 32, greet_dp, 0)
    lax.fori_loop(1, 8, greet_tensor, 0)

    for u in range(2):
        for s in range(NZ):
            wp[u, s, ROWS:LANES, :] = jnp.zeros((LANES - ROWS, 512), BF)
    locals_ = []
    for u in range(5):
        local = pltpu.make_async_copy(own(u), slot_ref(u, z), l_sem.at[u])
        local.start()
        locals_.append(local)

    def lines_of(column):
        rows = column.shape[0]
        wide = jnp.broadcast_to(column, (rows, 128))
        if rows % 128:
            wide = jnp.concatenate([wide, jnp.zeros((128 - rows % 128, 128), F32)], axis=0)
        return [wide[128 * b : 128 * b + 128].T[0:1] for b in range(wide.shape[0] // 128)]

    def column_of(lines, rows):
        wide = [jnp.broadcast_to(line, (128, 128)).T for line in lines]
        wide = wide[0] if len(wide) == 1 else jnp.concatenate(wide, axis=0)
        return wide[0:rows, 0:1]

    xv = vis_ref[...].astype(F32)
    mean = jnp.sum(jnp.sum(xv, axis=0), axis=-1, keepdims=True) / (4 * PART)
    centred = jnp.where(lane_of(xv.shape) < PART, xv - mean[None], 0.0)
    m2 = jnp.sum(jnp.sum(centred * centred, axis=0), axis=-1, keepdims=True)
    raw = raw_ref[...].astype(F32)
    lines = lines_of(jnp.sum(raw * raw, axis=-1, keepdims=True)) + lines_of(mean) + lines_of(m2)
    stats[tn] = jnp.concatenate(lines + [jnp.zeros((3, 128), F32)], axis=0)

    first = jnp.int32(0)
    my_first = jnp.int32(0)
    my_count = jnp.int32(0)
    owners = [jnp.int32(0)] * 8
    for s in range(NX * NZ):
        count = cnt_ref[s]
        my_first = my_first + jnp.where(s < dp, count, 0)
        my_count = my_count + jnp.where(s == dp, count, 0)
        first = first + count
        owners = [a + jnp.where(first <= r * 32 + dp, 1, 0) for r, a in enumerate(owners)]
    shape = (512, 128)
    row, col = row_of(shape), lane_of(shape)
    owner = jnp.zeros(shape, jnp.int32)
    for r in range(8):
        owner = jnp.where(((col >> 3) & 7) == r, owners[r], owner)
    same = ((row >> 4) == owner) & (((row >> 3) & 1) == (col >> 6)) & ((row & 7) == (col & 7))
    pick_ref[...] = jnp.where(same, 1.0, 0.0).astype(BF)
    shape = (SEQ, 512)
    row, col = row_of(shape), lane_of(shape)
    place = row - off_ref[0]
    inside = (place >= 0) & (place < 8 * my_count)
    source = (my_first + (place >> 3)) & 31
    match = inside & ((col >> 4) == source) & ((col & 7) == (place & 7))
    for h in range(2):
        chosen = match & (((col >> 3) & 1) == h)
        sel_ref[h] = jnp.where(chosen, 1.0, 0.0).astype(BF)
    place = row_of((SEQ, 128)) - off_ref[0]
    is_image = (place >= 0) & (place < 8 * my_count)

    pl.semaphore_wait(barrier, 38)
    for o in range(1, 8):
        send(stats.at[tn], stats.at[tn], st_s.at[o - 1], st_r.at[o - 1], (dp, (tn + o) % 8))
    ring(0)
    for o in range(1, 8):
        arrived(stats.at[(tn - o + 8) % 8], st_s.at[o - 1], st_r.at[o - 1])
    means = [stats[t][3:4] for t in range(8)]
    mean = sum(means[1:], means[0]) / 8.0
    total = jnp.zeros((1, 128), F32)
    for t in range(8):
        apart = means[t] - mean
        total = total + stats[t][4:5] + (4.0 * PART) * apart * apart
    scale = column_of([lax.rsqrt(total / (32.0 * PART) + vision_epsilon)], TOK)
    mean = column_of([mean], TOK)
    for i in range(4):
        piece = vis_ref[i].astype(F32)
        vis_own[i] = ((piece - mean) * scale * affine_ref[0, i] + affine_ref[1, i]).astype(BF)
    vis_spread.begin_y()
    vis_spread.begin_x()
    total = stats[0]
    for t in range(1, 8):
        total = total + stats[t]
    scale = lax.rsqrt(total / 8192.0 + decoder_epsilon)
    scale = column_of([scale[b : b + 1] for b in range(3)], SEQ)
    gain = attn_ref[:, pl.ds(pl.multiple_of(tn * 1024, 1024), 1024)]
    text_ref[...] = (raw_ref[...].astype(F32) * scale * gain).astype(BF)
    text_spread.begin()

    class Reduce:
        def __init__(self, index, far_out, far_in, near_out, near_in, own, value):
            self.i, self.value, self.own = index, value, own
            self.far_out, self.far_in = far_out, far_in
            self.near_out, self.near_in = near_out, near_in
            self.half = far_out.shape[0] // 2

        def opposite(self):
            i, half = self.i, self.half
            self.far_out[...] = self.value(2).astype(BF)
            for h in range(2):
                part = pl.ds(half * h, half)
                send(self.far_out.at[part], self.far_in.at[part], f_s.at[i, h], f_r.at[i, h],
                     along_x(1 if h == 0 else 3))
            self.own[...] = self.value(0)

        def neighbours(self):
            i, half = self.i, self.half
            for h in range(2):
                part = pl.ds(half * h, half)
                rest = pl.ds(half * (1 - h), half)
                o = 1 if h == 0 else 3
                value = self.value(o)
                arrived(self.far_in.at[part], f_s.at[i, h], f_r.at[i, h])
                mine = value[half * h : half * h + half] + self.far_in[part, :].astype(F32)
                self.near_out[h, part, :] = mine.astype(BF)
                self.near_out[h, rest, :] = value[half * (1 - h) : half * (1 - h) + half].astype(BF)
                send(self.near_out.at[h], self.near_in.at[h], g_s.at[i, h], g_r.at[i, h], along_x(o))

        def total(self):
            i = self.i
            acc = self.own[...]
            for h in range(2):
                arrived(self.near_in.at[h], g_s.at[i, h], g_r.at[i, h])
                acc = acc + self.near_in[h].astype(F32)
            return acc

    def project(source, u, o):
        s = (x + o) % NX
        first = dot(source[0, s], wq[u, 0:4].reshape(1024, 256))
        return first + dot(source[1, s], wq[u, 4:8].reshape(1024, 256))

    vis_reduce = Reduce(0, v_fo, v_fi, v_no, v_ni, v_own, lambda o: vs[(x + o) % NX])
    image_reduce = Reduce(
        1, i_fo, i_fi, i_no, i_ni, i_own,
        lambda o: jnp.concatenate([project(ia, u, o) for u in range(3)], axis=1),
    )
    text_reduce = [
        Reduce(2 + u, t_fo.at[u], t_fi.at[u], t_no.at[u], t_ni.at[u], t_own.at[u],
               lambda o, u=u: project(acts, u, o))
        for u in range(3)
    ]

    def vision():
        vis_spread.from_sibling()
        for h in range(2):
            acc = None
            for s in range(NZ):
                term = dot(vis_all[s].reshape(NX * TOK, LANES), wp[h, s])
                acc = term if acc is None else acc + term
            vs[:, :, 512 * h : 512 * h + 512] = acc.reshape(NX, TOK, 512)

    def image():
        tokens = vis_reduce.total().astype(BF).astype(F32)
        lines = lines_of(jnp.sum(tokens * tokens, axis=-1, keepdims=True))
        image_stats[tn] = jnp.concatenate(lines + [jnp.zeros((7, 128), F32)], axis=0)
        im[...] = (tokens * gain).astype(BF)
        image_spread.begin_y()
        image_spread.begin_x()
        for o in range(1, 8):
            send(image_stats.at[tn], image_stats.at[tn], n_s.at[o - 1], n_r.at[o - 1],
                 (dp, (tn + o) % 8))

    def locals_done(us):
        for u in us:
            locals_[u].wait()

    vis_spread.near(0)
    vis_spread.near(1)
    ring(1)
    text_spread.turn(0)
    text_spread.turn(1)
    ring(2)
    text_spread.turn(2)
    text_spread.turn(3)
    vis_spread.far(0)
    vis_spread.far(1)
    text_spread.mine(0)
    text_spread.mine(1)
    ring(3)
    text_spread.mine(2)
    text_spread.mine(3)
    vis_spread.to_sibling()
    text_spread.near(0)
    text_spread.near(1)
    ring(4)
    locals_done((0, 1))
    vision()
    vis_reduce.opposite()
    text_spread.near(2)
    text_spread.near(3)
    vis_reduce.neighbours()
    text_spread.far(0)
    text_spread.far(1)
    ring(5)
    image()
    text_spread.far(2)
    text_spread.far(3)
    image_spread.near(0)
    image_spread.near(1)
    ring(6)
    image_spread.far(0)
    image_spread.far(1)
    text_spread.from_sibling()
    locals_done((2, 3, 4))
    text_reduce[0].opposite()
    ring(7)
    image_spread.to_sibling()
    text_reduce[1].opposite()
    text_reduce[0].neighbours()
    image_spread.from_sibling()
    ring(8)
    image_reduce.opposite()
    image_reduce.neighbours()
    text_reduce[2].opposite()
    text_reduce[1].neighbours()
    text_reduce[2].neighbours()

    total = image_stats[tn]
    for o in range(1, 8):
        source = (tn - o + 8) % 8
        arrived(image_stats.at[source], n_s.at[o - 1], n_r.at[o - 1])
        total = total + image_stats[source]
    image_scale = column_of([lax.rsqrt(total[0:1] / 8192.0 + decoder_epsilon)], TOK)
    image_rows = (image_reduce.total() * image_scale).astype(BF)
    low, high = image_rows[:, 0:384], image_rows[:, 384:768]
    both = jnp.concatenate([low, high], axis=0)
    a2s[...] = dot(pick_ref[...], both).astype(BF).reshape(32, 16, 384)
    a2r[dp] = a2s[dp]

    def route(o, carry):
        to = (dp + o) % 32
        remote(a2s.at[to], a2r.at[dp], a_s.at[o - 1], a_r.at[o - 1], (to, tn)).start()
        return carry

    lax.fori_loop(1, 32, route, 0)

    causal = row_of((SEQ, SEQ)) >= lane_of((SEQ, SEQ))

    def route_done(o, carry):
        source = (dp - o + 32) % 32
        remote(a2s.at[source], a2r.at[source], a_s.at[o - 1], a_r.at[o - 1], here).wait_recv()
        return carry

    lax.fori_loop(1, 32, route_done, 0)
    routed = a2r[...].reshape(512, 384)
    image_low = dot(sel_ref[0], routed)
    image_high = dot(sel_ref[1], routed)

    texts = [text_reduce[u].total() for u in range(3)]
    cos, sin = cos_ref[...], sin_ref[...]

    def column(i):
        text = texts[i // 2][:, 128 * (i % 2) : 128 * (i % 2) + 128]
        picture = image_low if i < 3 else image_high
        picture = picture[:, 128 * (i % 3) : 128 * (i % 3) + 128]
        return jnp.where(is_image, picture, text)

    def turned(value):
        return (value * cos + pltpu.roll(value, 64, 1) * sin).astype(BF)

    key = turned(column(4))
    value = column(5).astype(BF)
    for h in range(4):
        query = turned(column(h))
        scores = lax.dot_general(query, key, (((1,), (1,)), ((), ())), preferred_element_type=F32)
        scores = jnp.where(causal, scores * HEAD_WIDTH ** (-0.5), -1e30)
        powers = jnp.exp(scores - jnp.max(scores, axis=-1, keepdims=True))
        weights = (powers / jnp.sum(powers, axis=-1, keepdims=True)).astype(BF)
        out_ref[:, 128 * h : 128 * h + 128] = dot(weights, value).astype(BF)

    for copy in pending:
        copy.wait_send()
    for copy, went in later:

        @pl.when(went)
        def _(copy=copy):
            copy.wait_send()


    def sent(o, carry):
        to = (dp + o) % 32
        remote(a2s.at[to], a2r.at[dp], a_s.at[o - 1], a_r.at[o - 1], here).wait_send()
        return carry

    lax.fori_loop(1, 32, sent, 0)


def rotation_tables():
    exponents = np.arange(64, dtype=np.float32) * np.float32(2.0 / 128)
    frequency = np.float32(rope_base) ** (-exponents)
    angles = np.arange(SEQ, dtype=np.float32)[:, None] * frequency[None, :]
    cos, sin = np.cos(angles), np.sin(angles)
    return (
        np.concatenate([cos, cos], axis=1).astype(np.float32),
        np.concatenate([-sin, sin], axis=1).astype(np.float32),
    )


def per_device(vis_rows, ln_gain, ln_bias, proj_weight, text_rows, attn_gain, w_query,
               key_value_weight, tile_counts, image_offsets):
    tn = lax.axis_index("tensor")

    def lanes(a):
        return jnp.pad(a, [(0, 0)] * (a.ndim - 1) + [(0, LANES - PART)])

    vis = vis_rows.reshape(TOK, 2, 4, 100).transpose(2, 0, 3, 1).reshape(4, TOK, PART)
    vis = lanes(vis)

    affine = jnp.stack([ln_gain, ln_bias])
    affine = lax.dynamic_slice_in_dim(affine, tn * 400, 400, 2)
    affine = lanes(affine.reshape(2, 2, 4, 100).transpose(0, 2, 3, 1).reshape(2, 4, 1, PART))

    proj = jnp.pad(proj_weight.reshape(PART, 1024), ((0, ROWS - PART), (0, 0)))
    proj = proj.reshape(ROWS, 2, 512).transpose(1, 0, 2)
    qkv = jnp.concatenate([w_query, key_value_weight.reshape(256, 256)], axis=1)
    qkv = qkv.reshape(256, 3, 256).transpose(1, 0, 2)
    cos, sin = rotation_tables()
    vmem = pl.BlockSpec(memory_space=pltpu.VMEM)
    smem = pl.BlockSpec(memory_space=pltpu.SMEM)
    dma = pltpu.SemaphoreType.DMA
    out = pl.pallas_call(
        kernel,
        out_shape=jax.ShapeDtypeStruct((SEQ, 512), BF),
        in_specs=[smem, smem] + [vmem] * 8,
        out_specs=vmem,
        scratch_shapes=[
            pltpu.VMEM((2, NZ, LANES, 512), BF),
            pltpu.VMEM((3, NZ, 256, 256), BF),
            pltpu.VMEM((NZ, NX, TOK, LANES), BF),
            pltpu.VMEM((4, TOK, LANES), BF),
            pltpu.VMEM((8, 8, 128), F32),
            pltpu.VMEM((8, 8, 128), F32),
            pltpu.VMEM((SEQ, 1024), BF),
            pltpu.VMEM((512, 128), BF),
            pltpu.VMEM((2, SEQ, 512), BF),
            pltpu.VMEM((2, NX, SEQ, 1024), BF),
            pltpu.VMEM((NX, TOK, 1024), F32),
            pltpu.VMEM((TOK, 1024), BF),
            pltpu.VMEM((2, NX, TOK, 1024), BF),
            pltpu.VMEM((TOK, 1024), BF),
            pltpu.VMEM((TOK, 1024), BF),
            pltpu.VMEM((2, TOK, 1024), BF),
            pltpu.VMEM((2, TOK, 1024), BF),
            pltpu.VMEM((TOK, 1024), F32),
            pltpu.VMEM((TOK, 768), BF),
            pltpu.VMEM((TOK, 768), BF),
            pltpu.VMEM((2, TOK, 768), BF),
            pltpu.VMEM((2, TOK, 768), BF),
            pltpu.VMEM((TOK, 768), F32),
            pltpu.VMEM((3, SEQ, 256), BF),
            pltpu.VMEM((3, SEQ, 256), BF),
            pltpu.VMEM((3, 2, SEQ, 256), BF),
            pltpu.VMEM((3, 2, SEQ, 256), BF),
            pltpu.VMEM((3, SEQ, 256), F32),
            pltpu.VMEM((32, 16, 384), BF),
            pltpu.VMEM((32, 16, 384), BF),
            pltpu.VMEM((3, 4, TOK, LANES), BF),
            pltpu.VMEM((SEQ, 1024), BF),
            pltpu.VMEM((3, TOK, 1024), BF),
            dma((5,)),
            dma((5, 2, 4)),
            dma((5, 2, 4)),
            dma((7,)),
            dma((7,)),
            dma((3, 3, 2)),
            dma((3, 3, 2)),
            dma((3, 4, 2)),
            dma((3, NX, 2)),
            dma((7, CHUNKS)),
            dma((7, CHUNKS)),
            dma((3, NX, 4)),
            dma((3, NX, 4)),
            dma((5, 2)),
            dma((5, 2)),
            dma((5, 2)),
            dma((5, 2)),
            dma((7,)),
            dma((7,)),
            dma((31,)),
            dma((31,)),
        ],
        compiler_params=pltpu.CompilerParams(collective_id=0, has_side_effects=True, vmem_limit_bytes=40 << 20),
        name="step",
    )(tile_counts, image_offsets, vis, affine, proj, qkv, text_rows[0],
      attn_gain[None], jnp.asarray(cos), jnp.asarray(sin))
    return out[None]


def solution(mesh):
    in_specs = (
        P(None, "dp", None, "tensor"),
        P(),
        P(),
        P("dp", None, "tensor"),
        P("dp", None, "tensor"),
        P(),
        P("dp", "tensor"),
        P("dp", None, "tensor"),
        P(),
        P("dp"),
    )
    return jax.shard_map(per_device, mesh=mesh, in_specs=in_specs,
                         out_specs=P("dp", None, "tensor"), check_vma=False)
```

```python
import functools

import jax
import jax.numpy as jnp
import numpy as np
from jax import lax
from jax.experimental import pallas as pl
from jax.experimental.pallas import tpu as pltpu
from jax.sharding import PartitionSpec as P

MESH = pl.DeviceIdType.MESH
BF = jnp.bfloat16
F32 = jnp.float32

HEAD_WIDTH = 128
SEQ = 384
TOK = 64
CHUNKS = 4
ROW_FOR = ((0, 2, 3, 1), (1, 3, 2, 0), (3, 0, 1, 2), (2, 1, 0, 3))
COLUMN_FOR = tuple(tuple(row.index(r) for r in range(4)) for row in ROW_FOR)
SAMPLE_AT = tuple(tuple([row[k] for row in ROW_FOR].index(r) for r in range(4)) for k in range(4))
NX, NY, NZ = 4, 4, 8
LANES = 256
ROWS = 208
PART = 200
vision_epsilon = 1e-06
decoder_epsilon = 1e-05
rope_base = 500000.0

STARTS = (0, 0, 2, 3, 4)
SLOTS = max(STARTS) + 5


def dot(a, b):
    return jnp.dot(a, b, preferred_element_type=F32)


def lane_of(shape):
    return lax.broadcasted_iota(jnp.int32, shape, len(shape) - 1)


def row_of(shape):
    return lax.broadcasted_iota(jnp.int32, shape, len(shape) - 2)


def kernel(
    cnt_ref, off_ref, vis_ref, affine_ref, proj_ref, query_ref, keyval_ref, raw_ref, attn_ref, cos_ref, sin_ref,
    out_ref,
    wp, wq, vis_all, vis_own, stats, image_stats, text_ref, pick_ref, sel_ref, acts, vs, im, ia,
    v_fo, v_fi, v_no, v_ni, v_own, i_fo, i_fi, i_no, i_ni, i_own, j_fo, j_fi, j_no, j_ni, j_own, t_fo, t_fi, t_no, t_ni, t_own,
    qs, qr, ks, kr, vis_col, text_mid, im_col,
    l_sem, z_s, z_r, st_s, st_r, ys_s, ys_r, xs_s, xs_r, tx_s, tx_r, d_s, d_r, f_s, f_r, g_s, g_r, n_s, n_r,
    a_s, a_r,
):
    dp = lax.axis_index("dp")
    tn = lax.axis_index("tensor")
    x, z = dp // NZ, dp % NZ
    y, c = tn // 2, tn % 2
    pending = []

    def remote(src, dst, ssem, rsem, to):
        return pltpu.make_async_remote_copy(
            src_ref=src, dst_ref=dst, send_sem=ssem, recv_sem=rsem, device_id=to,
            device_id_type=MESH,
        )

    def send(src, dst, ssem, rsem, to):
        copy = remote(src, dst, ssem, rsem, to)
        copy.start()
        pending.append(copy)

    here = (dp, tn)

    def arrived(ref, ssem, rsem):
        remote(ref, ref, ssem, rsem, here).wait_recv()

    def own(u):
        if u < 2:
            return proj_ref.at[u]
        return keyval_ref if u == 4 else query_ref.at[:, pl.ds(256 * (u - 2), 256)]

    def slot_ref(u, source):
        if u < 2:
            return wp.at[u, source, pl.ds(0, ROWS)]
        return wq.at[u - 2, source]

    def goes(u, e, k):
        return k < 4 or (u % 2 == e)

    def ring(slot):
        for u, start in enumerate(STARTS):
            k = slot - start
            if k < 0 or k > 4:
                continue
            for e in range(2):
                sign = 1 if e == 0 else -1
                source = (z - sign * k + 2 * NZ) % NZ
                if k >= 1 and goes(u, e, k):
                    arrived(slot_ref(u, source), z_s.at[u, e, k - 1], z_r.at[u, e, k - 1])
                if k <= 3 and goes(u, e, k + 1):
                    to = (x * NZ + (z + sign + NZ) % NZ, tn)
                    src = own(u) if k == 0 else slot_ref(u, source)
                    send(src, slot_ref(u, source), z_s.at[u, e, k], z_r.at[u, e, k], to)

    class Spread:
        def __init__(self, kind, own, column, place):
            self.kind, self.own, self.column, self.place = kind, own, column, place

        def on_y(self, src, slot, h, step):
            k = self.kind
            send(src, self.column(slot, h), ys_s.at[k, slot, h], ys_r.at[k, slot, h],
                 (dp, ((y + step + NY) % NY) * 2 + c))

        def on_x(self, src, j, h, kappa):
            k = self.kind
            copy = remote(src, self.place(c, x, h), xs_s.at[k, j, h], xs_r.at[k, x, h],
                          (kappa * NZ + z, tn))
            local = pltpu.make_async_copy(src, self.place(c, x, h), xs_r.at[k, x, h])

            @pl.when(kappa != x)
            def _():
                copy.start()

            @pl.when(kappa == x)
            def _():
                local.start()

            later.append((copy, kappa != x))

        def begin_y(self):
            for h in range(2):
                self.on_y(self.own(h), 0, h, 1)
                self.on_y(self.own(h), 1, h, -1)

        def begin_x(self):
            for h in range(2):
                self.on_x(self.own(h), 3, h, y)

        def near(self, h):
            k = self.kind
            for slot, step in ((0, 1), (1, -1)):
                arrived(self.column(slot, h), ys_s.at[k, slot, h], ys_r.at[k, slot, h])
                if slot == h:
                    src = self.column(slot, h)
                    send(src, self.column(2, h), ys_s.at[k, 2, h], ys_r.at[k, 2, h],
                         (dp, ((y + step + NY) % NY) * 2 + c))
            for slot, step in ((0, 1), (1, -1)):
                self.on_x(self.column(slot, h), slot, h, (y - step + NY) % NY)

        def far(self, h):
            k = self.kind
            arrived(self.column(2, h), ys_s.at[k, 2, h], ys_r.at[k, 2, h])
            self.on_x(self.column(2, h), 2, h, (y + 2) % NY)

        def to_sibling(self, offsets=(0, 1, 3, 2)):
            k = self.kind
            for o in offsets:
                s = (x + o) % NX
                for h in range(2):
                    ref = self.place(c, s, h)
                    arrived(ref, xs_s.at[k, 0, h], xs_r.at[k, s, h])
                    send(ref, ref, d_s.at[k, s, h], d_r.at[k, s, h], (dp, tn + 1 - 2 * c))

        def from_sibling(self):
            k = self.kind
            for s in range(NX):
                for h in range(2):
                    arrived(self.place(1 - c, s, h), d_s.at[k, s, h], d_r.at[k, s, h])

    later = []
    vis_spread = Spread(
        0,
        lambda h: vis_own.at[pl.ds(2 * h, 2)],
        lambda j, h: vis_col.at[j, pl.ds(2 * h, 2)],
        lambda core, s, h: vis_all.at[pl.ds(4 * core + 2 * h, 2), s],
    )
    def entry(rows, a, b):
        value = jnp.int32(0)
        for i, row in enumerate(rows):
            for j, v in enumerate(row):
                value = value + jnp.where((a == i) & (b == j), v, 0)
        return value

    class TextSpread:
        def __init__(self):
            self.row = entry(ROW_FOR, x, y)
            self.column = entry(COLUMN_FOR, x, y)
            self.sample = {step: entry(SAMPLE_AT, x, (y + step + NY) % NY) for step in (0, -1, 1, 2)}

        def part(self, q):
            return pl.ds(q * (SEQ // CHUNKS), SEQ // CHUNKS)

        def block(self, core, step, q):
            return acts.at[core, self.sample[step], self.part(q)]

        def hop(self, q, stays, src, dst, kind, to):
            ssem, rsem = tx_s.at[kind, q], tx_r.at[kind, q]
            copy = remote(src, dst, ssem, rsem, to)
            local = pltpu.make_async_copy(src, dst, rsem)

            @pl.when(stays)
            def _():
                local.start()

            @pl.when(jnp.logical_not(stays))
            def _():
                copy.start()

            later.append((copy, jnp.logical_not(stays)))

        def begin(self):
            for q in range(CHUNKS):
                part = self.part(q)
                self.hop(q, self.row == y, text_ref.at[part], text_mid.at[part], 0,
                         (dp, self.row * 2 + c))

        def turn(self, q):
            mid = text_mid.at[self.part(q)]
            arrived(mid, tx_s.at[0, q], tx_r.at[0, q])
            self.hop(q, self.column == x, mid, acts.at[c, x, self.part(q)], 2,
                     (self.column * NZ + z, tn))

        def on_y(self, q, block_step, step, kind):
            ref = self.block(c, block_step, q)
            send(ref, ref, tx_s.at[kind, q], tx_r.at[kind, q], (dp, ((y + step + NY) % NY) * 2 + c))

        def to_other(self, q, j, step):
            ref = self.block(c, step, q)
            send(ref, ref, d_s.at[1, j, q], d_r.at[1, j, q], (dp, tn + 1 - 2 * c))

        def mine(self, q):
            arrived(self.block(c, 0, q), tx_s.at[2, q], tx_r.at[2, q])
            self.on_y(q, 0, 1, 4)
            self.on_y(q, 0, -1, 5)
            self.to_other(q, 0, 0)

        def near(self, q):
            arrived(self.block(c, -1, q), tx_s.at[4, q], tx_r.at[4, q])
            arrived(self.block(c, 1, q), tx_s.at[5, q], tx_r.at[5, q])
            if q % 2 == 0:
                self.on_y(q, -1, 1, 6)
            else:
                self.on_y(q, 1, -1, 6)
            self.to_other(q, 1, -1)
            self.to_other(q, 2, 1)

        def far(self, q):
            arrived(self.block(c, 2, q), tx_s.at[6, q], tx_r.at[6, q])
            self.to_other(q, 3, 2)

        def from_sibling(self):
            for q in range(CHUNKS):
                for j, step in enumerate((0, -1, 1, 2)):
                    arrived(self.block(1 - c, step, q), d_s.at[1, j, q], d_r.at[1, j, q])

    text_spread = TextSpread()
    image_spread = Spread(
        2,
        lambda h: im.at[pl.ds(32 * h, 32)],
        lambda j, h: im_col.at[j, pl.ds(32 * h, 32)],
        lambda core, s, h: ia.at[core, s, pl.ds(32 * h, 32)],
    )

    def along_x(o):
        return (((x + o) % NX) * NZ + z, tn)

    barrier = pltpu.get_barrier_semaphore()

    def greet_dp(o, carry):
        pl.semaphore_signal(barrier, inc=1, device_id=((dp + o) % 32, tn), device_id_type=MESH)
        return carry

    def greet_tensor(o, carry):
        pl.semaphore_signal(barrier, inc=1, device_id=(dp, (tn + o) % 8), device_id_type=MESH)
        return carry

    lax.fori_loop(1, 32, greet_dp, 0)
    lax.fori_loop(1, 8, greet_tensor, 0)

    for u in range(2):
        for s in range(NZ):
            wp[u, s, ROWS:LANES, :] = jnp.zeros((LANES - ROWS, 512), BF)
    locals_ = []
    for u in range(5):
        local = pltpu.make_async_copy(own(u), slot_ref(u, z), l_sem.at[u])
        local.start()
        locals_.append(local)

    def lines_of(column):
        rows = column.shape[0]
        wide = jnp.broadcast_to(column, (rows, 128))
        if rows % 128:
            wide = jnp.concatenate([wide, jnp.zeros((128 - rows % 128, 128), F32)], axis=0)
        return [wide[128 * b : 128 * b + 128].T[0:1] for b in range(wide.shape[0] // 128)]

    def column_of(lines, rows):
        wide = [jnp.broadcast_to(line, (128, 128)).T for line in lines]
        wide = wide[0] if len(wide) == 1 else jnp.concatenate(wide, axis=0)
        return wide[0:rows, 0:1]

    xv = vis_ref[...].astype(F32)
    mean = jnp.sum(jnp.sum(xv, axis=0), axis=-1, keepdims=True) / (4 * PART)
    centred = jnp.where(lane_of(xv.shape) < PART, xv - mean[None], 0.0)
    m2 = jnp.sum(jnp.sum(centred * centred, axis=0), axis=-1, keepdims=True)
    raw = raw_ref[...].astype(F32)
    lines = lines_of(jnp.sum(raw * raw, axis=-1, keepdims=True)) + lines_of(mean) + lines_of(m2)
    stats[tn] = jnp.concatenate(lines + [jnp.zeros((3, 128), F32)], axis=0)

    first = jnp.int32(0)
    my_first = jnp.int32(0)
    my_count = jnp.int32(0)
    owners = [jnp.int32(0)] * 8
    for s in range(NX * NZ):
        count = cnt_ref[s]
        my_first = my_first + jnp.where(s < dp, count, 0)
        my_count = my_count + jnp.where(s == dp, count, 0)
        first = first + count
        owners = [a + jnp.where(first <= r * 32 + dp, 1, 0) for r, a in enumerate(owners)]
    shape = (512, 128)
    row, col = row_of(shape), lane_of(shape)
    owner = jnp.zeros(shape, jnp.int32)
    for r in range(8):
        owner = jnp.where(((col >> 3) & 7) == r, owners[r], owner)
    same = ((row >> 4) == owner) & (((row >> 3) & 1) == (col >> 6)) & ((row & 7) == (col & 7))
    pick_ref[...] = jnp.where(same, 1.0, 0.0).astype(BF)
    shape = (SEQ, 512)
    row, col = row_of(shape), lane_of(shape)
    place = row - off_ref[0]
    inside = (place >= 0) & (place < 8 * my_count)
    source = (my_first + (place >> 3)) & 31
    match = inside & ((col >> 4) == source) & ((col & 7) == (place & 7))
    for h in range(2):
        chosen = match & (((col >> 3) & 1) == h)
        sel_ref[h] = jnp.where(chosen, 1.0, 0.0).astype(BF)
    place = row_of((SEQ, 128)) - off_ref[0]
    is_image = (place >= 0) & (place < 8 * my_count)

    pl.semaphore_wait(barrier, 38)
    for o in range(1, 8):
        send(stats.at[tn], stats.at[tn], st_s.at[o - 1], st_r.at[o - 1], (dp, (tn + o) % 8))
    ring(0)
    for o in range(1, 8):
        arrived(stats.at[(tn - o + 8) % 8], st_s.at[o - 1], st_r.at[o - 1])
    means = [stats[t][3:4] for t in range(8)]
    mean = sum(means[1:], means[0]) / 8.0
    total = jnp.zeros((1, 128), F32)
    for t in range(8):
        apart = means[t] - mean
        total = total + stats[t][4:5] + (4.0 * PART) * apart * apart
    scale = column_of([lax.rsqrt(total / (32.0 * PART) + vision_epsilon)], TOK)
    mean = column_of([mean], TOK)
    for i in range(4):
        piece = vis_ref[i].astype(F32)
        vis_own[i] = ((piece - mean) * scale * affine_ref[0, i] + affine_ref[1, i]).astype(BF)
    vis_spread.begin_y()
    vis_spread.begin_x()
    total = stats[0]
    for t in range(1, 8):
        total = total + stats[t]
    scale = lax.rsqrt(total / 8192.0 + decoder_epsilon)
    scale = column_of([scale[b : b + 1] for b in range(3)], SEQ)
    gain = attn_ref[:, pl.ds(pl.multiple_of(tn * 1024, 1024), 1024)]
    text_ref[...] = (raw_ref[...].astype(F32) * scale * gain).astype(BF)
    text_spread.begin()

    class Reduce:
        def __init__(self, index, far_out, far_in, near_out, near_in, own, value):
            self.i, self.value, self.own = index, value, own
            self.far_out, self.far_in = far_out, far_in
            self.near_out, self.near_in = near_out, near_in
            self.half = far_out.shape[0] // 2

        def opposite(self):
            i, half = self.i, self.half
            self.far_out[...] = self.value(2).astype(BF)
            for h in range(2):
                part = pl.ds(half * h, half)
                send(self.far_out.at[part], self.far_in.at[part], f_s.at[i, h], f_r.at[i, h],
                     along_x(1 if h == 0 else 3))
            self.own[...] = self.value(0)

        def neighbours(self):
            i, half = self.i, self.half
            for h in range(2):
                part = pl.ds(half * h, half)
                rest = pl.ds(half * (1 - h), half)
                o = 1 if h == 0 else 3
                value = self.value(o)
                arrived(self.far_in.at[part], f_s.at[i, h], f_r.at[i, h])
                mine = value[half * h : half * h + half] + self.far_in[part, :].astype(F32)
                self.near_out[h, part, :] = mine.astype(BF)
                self.near_out[h, rest, :] = value[half * (1 - h) : half * (1 - h) + half].astype(BF)
                send(self.near_out.at[h], self.near_in.at[h], g_s.at[i, h], g_r.at[i, h], along_x(o))

        def total(self):
            i = self.i
            acc = self.own[...]
            for h in range(2):
                arrived(self.near_in.at[h], g_s.at[i, h], g_r.at[i, h])
                acc = acc + self.near_in[h].astype(F32)
            return acc

    def project(source, u, o):
        s = (x + o) % NX
        first = dot(source[0, s], wq[u, 0:4].reshape(1024, 256))
        return first + dot(source[1, s], wq[u, 4:8].reshape(1024, 256))

    vis_reduce = Reduce(0, v_fo, v_fi, v_no, v_ni, v_own, lambda o: vs[(x + o) % NX])
    image_queries = Reduce(
        1, i_fo, i_fi, i_no, i_ni, i_own,
        lambda o: jnp.concatenate([project(ia, u, o) for u in range(2)], axis=1),
    )
    image_keyvals = Reduce(5, j_fo, j_fi, j_no, j_ni, j_own, lambda o: project(ia, 2, o))
    text_reduce = [
        Reduce(2 + u, t_fo.at[u], t_fi.at[u], t_no.at[u], t_ni.at[u], t_own.at[u],
               lambda o, u=u: project(acts, u, o))
        for u in range(3)
    ]

    def vision():
        vis_spread.from_sibling()
        for h in range(2):
            acc = None
            for s in range(NZ):
                term = dot(vis_all[s].reshape(NX * TOK, LANES), wp[h, s])
                acc = term if acc is None else acc + term
            vs[:, :, 512 * h : 512 * h + 512] = acc.reshape(NX, TOK, 512)

    def image():
        tokens = vis_reduce.total().astype(BF).astype(F32)
        lines = lines_of(jnp.sum(tokens * tokens, axis=-1, keepdims=True))
        image_stats[tn] = jnp.concatenate(lines + [jnp.zeros((7, 128), F32)], axis=0)
        im[...] = (tokens * gain).astype(BF)
        image_spread.begin_y()
        image_spread.begin_x()
        for o in range(1, 8):
            send(image_stats.at[tn], image_stats.at[tn], n_s.at[o - 1], n_r.at[o - 1],
                 (dp, (tn + o) % 8))

    def locals_done(us):
        for u in us:
            locals_[u].wait()

    def image_scale():
        total = image_stats[tn]
        for o in range(1, 8):
            source = (tn - o + 8) % 8
            arrived(image_stats.at[source], n_s.at[o - 1], n_r.at[o - 1])
            total = total + image_stats[source]
        return column_of([lax.rsqrt(total[0:1] / 8192.0 + decoder_epsilon)], TOK)

    def route(i, reduced, scale, out, into):
        half = out.shape[2]
        rows = (reduced.total() * scale).astype(BF)
        both = jnp.concatenate([rows[:, 0:half], rows[:, half : 2 * half]], axis=0)
        out[...] = dot(pick_ref[...], both).astype(BF).reshape(32, 16, half)
        into[dp] = out[dp]

        def one(o, carry):
            to = (dp + o) % 32
            remote(out.at[to], into.at[dp], a_s.at[i, o - 1], a_r.at[i, o - 1], (to, tn)).start()
            return carry

        lax.fori_loop(1, 32, one, 0)

    def routed(i, out, into):
        def one(o, carry):
            source = (dp - o + 32) % 32
            remote(out.at[source], into.at[source], a_s.at[i, o - 1], a_r.at[i, o - 1],
                   here).wait_recv()
            return carry

        lax.fori_loop(1, 32, one, 0)
        return into[...].reshape(512, into.shape[2])

    def routes_sent(i, out, into):
        def one(o, carry):
            to = (dp + o) % 32
            remote(out.at[to], into.at[dp], a_s.at[i, o - 1], a_r.at[i, o - 1], here).wait_send()
            return carry

        lax.fori_loop(1, 32, one, 0)

    vis_spread.near(0)
    vis_spread.near(1)
    ring(1)
    text_spread.turn(0)
    text_spread.turn(1)
    ring(2)
    text_spread.turn(2)
    text_spread.turn(3)
    vis_spread.far(0)
    vis_spread.far(1)
    text_spread.mine(0)
    text_spread.mine(1)
    ring(3)
    text_spread.mine(2)
    text_spread.mine(3)
    vis_spread.to_sibling()
    text_spread.near(0)
    text_spread.near(1)
    ring(4)
    locals_done((0, 1))
    vision()
    vis_reduce.opposite()
    text_spread.near(2)
    text_spread.near(3)
    vis_reduce.neighbours()
    text_spread.far(0)
    text_spread.far(1)
    ring(5)
    image()
    text_spread.far(2)
    text_spread.far(3)
    image_spread.near(0)
    image_spread.near(1)
    ring(6)
    image_spread.far(0)
    image_spread.far(1)
    text_spread.from_sibling()
    locals_done((2, 3, 4))
    text_reduce[0].opposite()
    ring(7)
    image_spread.to_sibling()
    text_reduce[1].opposite()
    image_spread.from_sibling()
    image_queries.opposite()
    text_reduce[0].neighbours()
    ring(8)
    image_keyvals.opposite()
    scale = image_scale()
    image_queries.neighbours()
    text_reduce[2].opposite()
    image_keyvals.neighbours()
    route(0, image_queries, scale, qs, qr)
    text_reduce[1].neighbours()
    route(1, image_keyvals, scale, ks, kr)
    text_reduce[2].neighbours()

    causal = row_of((SEQ, SEQ)) >= lane_of((SEQ, SEQ))

    images_q = routed(0, qs, qr)
    images_k = routed(1, ks, kr)
    placed = [dot(sel_ref[h], images) for images in (images_q, images_k) for h in range(2)]

    texts = [text_reduce[u].total() for u in range(3)]
    cos, sin = cos_ref[...], sin_ref[...]

    def column(i):
        text = texts[i // 2][:, 128 * (i % 2) : 128 * (i % 2) + 128]
        picture = placed[i // 2] if i < 4 else placed[i - 2]
        if i < 4:
            picture = picture[:, 128 * (i % 2) : 128 * (i % 2) + 128]
        return jnp.where(is_image, picture, text)

    def turned(value):
        return (value * cos + pltpu.roll(value, 64, 1) * sin).astype(BF)

    key = turned(column(4))
    value = column(5).astype(BF)
    for h in range(4):
        query = turned(column(h))
        scores = lax.dot_general(query, key, (((1,), (1,)), ((), ())), preferred_element_type=F32)
        scores = jnp.where(causal, scores * HEAD_WIDTH ** (-0.5), -1e30)
        powers = jnp.exp(scores - jnp.max(scores, axis=-1, keepdims=True))
        weights = (powers / jnp.sum(powers, axis=-1, keepdims=True)).astype(BF)
        out_ref[:, 128 * h : 128 * h + 128] = dot(weights, value).astype(BF)

    for copy in pending:
        copy.wait_send()
    for copy, went in later:

        @pl.when(went)
        def _(copy=copy):
            copy.wait_send()


    routes_sent(0, qs, qr)
    routes_sent(1, ks, kr)


def rotation_tables():
    exponents = np.arange(64, dtype=np.float32) * np.float32(2.0 / 128)
    frequency = np.float32(rope_base) ** (-exponents)
    angles = np.arange(SEQ, dtype=np.float32)[:, None] * frequency[None, :]
    cos, sin = np.cos(angles), np.sin(angles)
    return (
        np.concatenate([cos, cos], axis=1).astype(np.float32),
        np.concatenate([-sin, sin], axis=1).astype(np.float32),
    )


def per_device(vis_rows, ln_gain, ln_bias, proj_weight, text_rows, attn_gain, w_query,
               key_value_weight, tile_counts, image_offsets):
    tn = lax.axis_index("tensor")

    def lanes(a):
        return jnp.pad(a, [(0, 0)] * (a.ndim - 1) + [(0, LANES - PART)])

    vis = vis_rows.reshape(TOK, 2, 4, 100).transpose(2, 0, 3, 1).reshape(4, TOK, PART)
    vis = lanes(vis)

    affine = jnp.stack([ln_gain, ln_bias])
    affine = lax.dynamic_slice_in_dim(affine, tn * 400, 400, 2)
    affine = lanes(affine.reshape(2, 2, 4, 100).transpose(0, 2, 3, 1).reshape(2, 4, 1, PART))

    proj = jnp.pad(proj_weight.reshape(PART, 1024), ((0, ROWS - PART), (0, 0)))
    proj = proj.reshape(ROWS, 2, 512).transpose(1, 0, 2)
    cos, sin = rotation_tables()
    vmem = pl.BlockSpec(memory_space=pltpu.VMEM)
    smem = pl.BlockSpec(memory_space=pltpu.SMEM)
    dma = pltpu.SemaphoreType.DMA
    out = pl.pallas_call(
        kernel,
        out_shape=jax.ShapeDtypeStruct((SEQ, 512), BF),
        in_specs=[smem, smem] + [vmem] * 9,
        out_specs=vmem,
        scratch_shapes=[
            pltpu.VMEM((2, NZ, LANES, 512), BF),
            pltpu.VMEM((3, NZ, 256, 256), BF),
            pltpu.VMEM((NZ, NX, TOK, LANES), BF),
            pltpu.VMEM((4, TOK, LANES), BF),
            pltpu.VMEM((8, 8, 128), F32),
            pltpu.VMEM((8, 8, 128), F32),
            pltpu.VMEM((SEQ, 1024), BF),
            pltpu.VMEM((512, 128), BF),
            pltpu.VMEM((2, SEQ, 512), BF),
            pltpu.VMEM((2, NX, SEQ, 1024), BF),
            pltpu.VMEM((NX, TOK, 1024), F32),
            pltpu.VMEM((TOK, 1024), BF),
            pltpu.VMEM((2, NX, TOK, 1024), BF),
            pltpu.VMEM((TOK, 1024), BF),
            pltpu.VMEM((TOK, 1024), BF),
            pltpu.VMEM((2, TOK, 1024), BF),
            pltpu.VMEM((2, TOK, 1024), BF),
            pltpu.VMEM((TOK, 1024), F32),
            pltpu.VMEM((TOK, 512), BF),
            pltpu.VMEM((TOK, 512), BF),
            pltpu.VMEM((2, TOK, 512), BF),
            pltpu.VMEM((2, TOK, 512), BF),
            pltpu.VMEM((TOK, 512), F32),
            pltpu.VMEM((TOK, 256), BF),
            pltpu.VMEM((TOK, 256), BF),
            pltpu.VMEM((2, TOK, 256), BF),
            pltpu.VMEM((2, TOK, 256), BF),
            pltpu.VMEM((TOK, 256), F32),
            pltpu.VMEM((3, SEQ, 256), BF),
            pltpu.VMEM((3, SEQ, 256), BF),
            pltpu.VMEM((3, 2, SEQ, 256), BF),
            pltpu.VMEM((3, 2, SEQ, 256), BF),
            pltpu.VMEM((3, SEQ, 256), F32),
            pltpu.VMEM((32, 16, 256), BF),
            pltpu.VMEM((32, 16, 256), BF),
            pltpu.VMEM((32, 16, 128), BF),
            pltpu.VMEM((32, 16, 128), BF),
            pltpu.VMEM((3, 4, TOK, LANES), BF),
            pltpu.VMEM((SEQ, 1024), BF),
            pltpu.VMEM((3, TOK, 1024), BF),
            dma((5,)),
            dma((5, 2, 4)),
            dma((5, 2, 4)),
            dma((7,)),
            dma((7,)),
            dma((3, 3, 2)),
            dma((3, 3, 2)),
            dma((3, 4, 2)),
            dma((3, NX, 2)),
            dma((7, CHUNKS)),
            dma((7, CHUNKS)),
            dma((3, NX, 4)),
            dma((3, NX, 4)),
            dma((6, 2)),
            dma((6, 2)),
            dma((6, 2)),
            dma((6, 2)),
            dma((7,)),
            dma((7,)),
            dma((2, 31)),
            dma((2, 31)),
        ],
        compiler_params=pltpu.CompilerParams(collective_id=0, has_side_effects=True, vmem_limit_bytes=40 << 20),
        name="step",
    )(tile_counts, image_offsets, vis, affine, proj, w_query,
      key_value_weight.reshape(256, 256), text_rows[0],
      attn_gain[None], jnp.asarray(cos), jnp.asarray(sin))
    return out[None]


def solution(mesh):
    in_specs = (
        P(None, "dp", None, "tensor"),
        P(),
        P(),
        P("dp", None, "tensor"),
        P("dp", None, "tensor"),
        P(),
        P("dp", "tensor"),
        P("dp", None, "tensor"),
        P(),
        P("dp"),
    )
    return jax.shard_map(per_device, mesh=mesh, in_specs=in_specs,
                         out_specs=P("dp", None, "tensor"), check_vma=False)
```

```python
import functools

import jax
import jax.numpy as jnp
import numpy as np
from jax import lax
from jax.experimental import pallas as pl
from jax.experimental.pallas import tpu as pltpu
from jax.sharding import PartitionSpec as P

MESH = pl.DeviceIdType.MESH
BF = jnp.bfloat16
F32 = jnp.float32

HEAD_WIDTH = 128
SEQ = 384
TOK = 64
CHUNKS = 4
ROW_FOR = ((0, 2, 3, 1), (1, 3, 2, 0), (3, 0, 1, 2), (2, 1, 0, 3))
COLUMN_FOR = tuple(tuple(row.index(r) for r in range(4)) for row in ROW_FOR)
SAMPLE_AT = tuple(tuple([row[k] for row in ROW_FOR].index(r) for r in range(4)) for k in range(4))
NX, NY, NZ = 4, 4, 8
LANES = 256
ROWS = 208
PART = 200
vision_epsilon = 1e-06
decoder_epsilon = 1e-05
rope_base = 500000.0

STARTS = (0, 0, 2, 3, 4)
SLOTS = max(STARTS) + 5


def dot(a, b):
    return jnp.dot(a, b, preferred_element_type=F32)


def lane_of(shape):
    return lax.broadcasted_iota(jnp.int32, shape, len(shape) - 1)


def row_of(shape):
    return lax.broadcasted_iota(jnp.int32, shape, len(shape) - 2)


def kernel(
    cnt_ref, off_ref, vis_ref, affine_ref, proj_ref, query_ref, keyval_ref, raw_ref, attn_ref, cos_ref, sin_ref,
    out_ref,
    wp, wq, vis_all, vis_own, stats, image_stats, text_ref, pick_ref, sel_ref, acts, vs, im, ia,
    v_fo, v_fi, v_no, v_ni, v_own, i_fo, i_fi, i_no, i_ni, i_own, j_fo, j_fi, j_no, j_ni, j_own, t_fo, t_fi, t_no, t_ni, t_own,
    pair_ref, qs, qr, ks, kr, vis_col, text_mid, im_col,
    l_sem, z_s, z_r, st_s, st_r, ys_s, ys_r, xs_s, xs_r, tx_s, tx_r, d_s, d_r, f_s, f_r, g_s, g_r, n_s, n_r,
    a_s, a_r,
):
    dp = lax.axis_index("dp")
    tn = lax.axis_index("tensor")
    x, z = dp // NZ, dp % NZ
    y, c = tn // 2, tn % 2
    pending = []

    def remote(src, dst, ssem, rsem, to):
        return pltpu.make_async_remote_copy(
            src_ref=src, dst_ref=dst, send_sem=ssem, recv_sem=rsem, device_id=to,
            device_id_type=MESH,
        )

    def send(src, dst, ssem, rsem, to):
        copy = remote(src, dst, ssem, rsem, to)
        copy.start()
        pending.append(copy)

    here = (dp, tn)

    def arrived(ref, ssem, rsem):
        remote(ref, ref, ssem, rsem, here).wait_recv()

    def own(u):
        if u < 2:
            return proj_ref.at[u]
        return keyval_ref if u == 4 else query_ref.at[:, pl.ds(256 * (u - 2), 256)]

    def slot_ref(u, source):
        if u < 2:
            return wp.at[u, source, pl.ds(0, ROWS)]
        return wq.at[u - 2, source]

    def goes(u, e, k):
        return k < 4 or (u % 2 == e)

    def ring(slot):
        for u, start in enumerate(STARTS):
            k = slot - start
            if k < 0 or k > 4:
                continue
            for e in range(2):
                sign = 1 if e == 0 else -1
                source = (z - sign * k + 2 * NZ) % NZ
                if k >= 1 and goes(u, e, k):
                    arrived(slot_ref(u, source), z_s.at[u, e, k - 1], z_r.at[u, e, k - 1])
                if k <= 3 and goes(u, e, k + 1):
                    to = (x * NZ + (z + sign + NZ) % NZ, tn)
                    src = own(u) if k == 0 else slot_ref(u, source)
                    send(src, slot_ref(u, source), z_s.at[u, e, k], z_r.at[u, e, k], to)

    class Spread:
        def __init__(self, kind, own, column, place):
            self.kind, self.own, self.column, self.place = kind, own, column, place

        def on_y(self, src, slot, h, step):
            k = self.kind
            send(src, self.column(slot, h), ys_s.at[k, slot, h], ys_r.at[k, slot, h],
                 (dp, ((y + step + NY) % NY) * 2 + c))

        def on_x(self, src, j, h, kappa):
            k = self.kind
            copy = remote(src, self.place(c, x, h), xs_s.at[k, j, h], xs_r.at[k, x, h],
                          (kappa * NZ + z, tn))
            local = pltpu.make_async_copy(src, self.place(c, x, h), xs_r.at[k, x, h])

            @pl.when(kappa != x)
            def _():
                copy.start()

            @pl.when(kappa == x)
            def _():
                local.start()

            later.append((copy, kappa != x))

        def begin_y(self):
            for h in range(2):
                self.on_y(self.own(h), 0, h, 1)
                self.on_y(self.own(h), 1, h, -1)

        def begin_x(self):
            for h in range(2):
                self.on_x(self.own(h), 3, h, y)

        def near(self, h):
            k = self.kind
            for slot, step in ((0, 1), (1, -1)):
                arrived(self.column(slot, h), ys_s.at[k, slot, h], ys_r.at[k, slot, h])
                if slot == h:
                    src = self.column(slot, h)
                    send(src, self.column(2, h), ys_s.at[k, 2, h], ys_r.at[k, 2, h],
                         (dp, ((y + step + NY) % NY) * 2 + c))
            for slot, step in ((0, 1), (1, -1)):
                self.on_x(self.column(slot, h), slot, h, (y - step + NY) % NY)

        def far(self, h):
            k = self.kind
            arrived(self.column(2, h), ys_s.at[k, 2, h], ys_r.at[k, 2, h])
            self.on_x(self.column(2, h), 2, h, (y + 2) % NY)

        def to_sibling(self, offsets=(0, 1, 3, 2)):
            k = self.kind
            for o in offsets:
                s = (x + o) % NX
                for h in range(2):
                    ref = self.place(c, s, h)
                    arrived(ref, xs_s.at[k, 0, h], xs_r.at[k, s, h])
                    send(ref, ref, d_s.at[k, s, h], d_r.at[k, s, h], (dp, tn + 1 - 2 * c))

        def from_sibling(self):
            k = self.kind
            for s in range(NX):
                for h in range(2):
                    arrived(self.place(1 - c, s, h), d_s.at[k, s, h], d_r.at[k, s, h])

    later = []
    vis_spread = Spread(
        0,
        lambda h: vis_own.at[pl.ds(2 * h, 2)],
        lambda j, h: vis_col.at[j, pl.ds(2 * h, 2)],
        lambda core, s, h: vis_all.at[pl.ds(4 * core + 2 * h, 2), s],
    )
    def entry(rows, a, b):
        value = jnp.int32(0)
        for i, row in enumerate(rows):
            for j, v in enumerate(row):
                value = value + jnp.where((a == i) & (b == j), v, 0)
        return value

    class TextSpread:
        def __init__(self):
            self.row = entry(ROW_FOR, x, y)
            self.column = entry(COLUMN_FOR, x, y)
            self.sample = {step: entry(SAMPLE_AT, x, (y + step + NY) % NY) for step in (0, -1, 1, 2)}

        def part(self, q):
            return pl.ds(q * (SEQ // CHUNKS), SEQ // CHUNKS)

        def block(self, core, step, q):
            return acts.at[core, self.sample[step], self.part(q)]

        def hop(self, q, stays, src, dst, kind, to):
            ssem, rsem = tx_s.at[kind, q], tx_r.at[kind, q]
            copy = remote(src, dst, ssem, rsem, to)
            local = pltpu.make_async_copy(src, dst, rsem)

            @pl.when(stays)
            def _():
                local.start()

            @pl.when(jnp.logical_not(stays))
            def _():
                copy.start()

            later.append((copy, jnp.logical_not(stays)))

        def begin(self):
            for q in range(CHUNKS):
                part = self.part(q)
                self.hop(q, self.row == y, text_ref.at[part], text_mid.at[part], 0,
                         (dp, self.row * 2 + c))

        def turn(self, q):
            mid = text_mid.at[self.part(q)]
            arrived(mid, tx_s.at[0, q], tx_r.at[0, q])
            self.hop(q, self.column == x, mid, acts.at[c, x, self.part(q)], 2,
                     (self.column * NZ + z, tn))

        def on_y(self, q, block_step, step, kind):
            ref = self.block(c, block_step, q)
            send(ref, ref, tx_s.at[kind, q], tx_r.at[kind, q], (dp, ((y + step + NY) % NY) * 2 + c))

        def to_other(self, q, j, step):
            ref = self.block(c, step, q)
            send(ref, ref, d_s.at[1, j, q], d_r.at[1, j, q], (dp, tn + 1 - 2 * c))

        def mine(self, q):
            arrived(self.block(c, 0, q), tx_s.at[2, q], tx_r.at[2, q])
            self.on_y(q, 0, 1, 4)
            self.on_y(q, 0, -1, 5)
            self.to_other(q, 0, 0)

        def near(self, q):
            arrived(self.block(c, -1, q), tx_s.at[4, q], tx_r.at[4, q])
            arrived(self.block(c, 1, q), tx_s.at[5, q], tx_r.at[5, q])
            if q % 2 == 0:
                self.on_y(q, -1, 1, 6)
            else:
                self.on_y(q, 1, -1, 6)
            self.to_other(q, 1, -1)
            self.to_other(q, 2, 1)

        def far(self, q):
            arrived(self.block(c, 2, q), tx_s.at[6, q], tx_r.at[6, q])
            self.to_other(q, 3, 2)

        def from_sibling(self):
            for q in range(CHUNKS):
                for j, step in enumerate((0, -1, 1, 2)):
                    arrived(self.block(1 - c, step, q), d_s.at[1, j, q], d_r.at[1, j, q])

    text_spread = TextSpread()
    image_spread = Spread(
        2,
        lambda h: im.at[pl.ds(32 * h, 32)],
        lambda j, h: im_col.at[j, pl.ds(32 * h, 32)],
        lambda core, s, h: ia.at[core, s, pl.ds(32 * h, 32)],
    )

    def along_x(o):
        return (((x + o) % NX) * NZ + z, tn)

    barrier = pltpu.get_barrier_semaphore()

    def greet_dp(o, carry):
        pl.semaphore_signal(barrier, inc=1, device_id=((dp + o) % 32, tn), device_id_type=MESH)
        return carry

    def greet_tensor(o, carry):
        pl.semaphore_signal(barrier, inc=1, device_id=(dp, (tn + o) % 8), device_id_type=MESH)
        return carry

    lax.fori_loop(1, 32, greet_dp, 0)
    lax.fori_loop(1, 8, greet_tensor, 0)

    for u in range(2):
        for s in range(NZ):
            wp[u, s, ROWS:LANES, :] = jnp.zeros((LANES - ROWS, 512), BF)
    locals_ = []
    for u in range(5):
        local = pltpu.make_async_copy(own(u), slot_ref(u, z), l_sem.at[u])
        local.start()
        locals_.append(local)

    def lines_of(column):
        rows = column.shape[0]
        wide = jnp.broadcast_to(column, (rows, 128))
        if rows % 128:
            wide = jnp.concatenate([wide, jnp.zeros((128 - rows % 128, 128), F32)], axis=0)
        return [wide[128 * b : 128 * b + 128].T[0:1] for b in range(wide.shape[0] // 128)]

    def column_of(lines, rows):
        wide = [jnp.broadcast_to(line, (128, 128)).T for line in lines]
        wide = wide[0] if len(wide) == 1 else jnp.concatenate(wide, axis=0)
        return wide[0:rows, 0:1]

    xv = vis_ref[...].astype(F32)
    mean = jnp.sum(jnp.sum(xv, axis=0), axis=-1, keepdims=True) / (4 * PART)
    centred = jnp.where(lane_of(xv.shape) < PART, xv - mean[None], 0.0)
    m2 = jnp.sum(jnp.sum(centred * centred, axis=0), axis=-1, keepdims=True)
    raw = raw_ref[...].astype(F32)
    lines = lines_of(jnp.sum(raw * raw, axis=-1, keepdims=True)) + lines_of(mean) + lines_of(m2)
    stats[tn] = jnp.concatenate(lines + [jnp.zeros((3, 128), F32)], axis=0)

    first = jnp.int32(0)
    my_first = jnp.int32(0)
    my_count = jnp.int32(0)
    owners = [jnp.int32(0)] * 8
    for s in range(NX * NZ):
        count = cnt_ref[s]
        my_first = my_first + jnp.where(s < dp, count, 0)
        my_count = my_count + jnp.where(s == dp, count, 0)
        first = first + count
        owners = [a + jnp.where(first <= r * 32 + dp, 1, 0) for r, a in enumerate(owners)]
    shape = (512, 128)
    row, col = row_of(shape), lane_of(shape)
    owner = jnp.zeros(shape, jnp.int32)
    for r in range(8):
        owner = jnp.where(((col >> 3) & 7) == r, owners[r], owner)
    same = ((row >> 4) == owner) & (((row >> 3) & 1) == (col >> 6)) & ((row & 7) == (col & 7))
    pick_ref[...] = jnp.where(same, 1.0, 0.0).astype(BF)
    shape = (SEQ, 512)
    row, col = row_of(shape), lane_of(shape)
    place = row - off_ref[0]
    inside = (place >= 0) & (place < 8 * my_count)
    source = (my_first + (place >> 3)) & 31
    match = inside & ((col >> 4) == source) & ((col & 7) == (place & 7))
    for h in range(2):
        chosen = match & (((col >> 3) & 1) == h)
        sel_ref[h] = jnp.where(chosen, 1.0, 0.0).astype(BF)
    place = row_of((SEQ, 128)) - off_ref[0]
    is_image = (place >= 0) & (place < 8 * my_count)

    pl.semaphore_wait(barrier, 38)
    for o in range(1, 8):
        send(stats.at[tn], stats.at[tn], st_s.at[o - 1], st_r.at[o - 1], (dp, (tn + o) % 8))
    ring(0)
    for o in range(1, 8):
        arrived(stats.at[(tn - o + 8) % 8], st_s.at[o - 1], st_r.at[o - 1])
    means = [stats[t][3:4] for t in range(8)]
    mean = sum(means[1:], means[0]) / 8.0
    total = jnp.zeros((1, 128), F32)
    for t in range(8):
        apart = means[t] - mean
        total = total + stats[t][4:5] + (4.0 * PART) * apart * apart
    scale = column_of([lax.rsqrt(total / (32.0 * PART) + vision_epsilon)], TOK)
    mean = column_of([mean], TOK)
    for i in range(4):
        piece = vis_ref[i].astype(F32)
        vis_own[i] = ((piece - mean) * scale * affine_ref[0, i] + affine_ref[1, i]).astype(BF)
    vis_spread.begin_y()
    vis_spread.begin_x()
    total = stats[0]
    for t in range(1, 8):
        total = total + stats[t]
    scale = lax.rsqrt(total / 8192.0 + decoder_epsilon)
    scale = column_of([scale[b : b + 1] for b in range(3)], SEQ)
    gain = attn_ref[:, pl.ds(pl.multiple_of(tn * 1024, 1024), 1024)]
    text_ref[...] = (raw_ref[...].astype(F32) * scale * gain).astype(BF)
    text_spread.begin()

    class Reduce:
        def __init__(self, index, far_out, far_in, near_out, near_in, own, value, both=None):
            self.i, self.value, self.own, self.both = index, value, own, both
            self.far_out, self.far_in = far_out, far_in
            self.near_out, self.near_in = near_out, near_in
            self.half = far_out.shape[0] // 2

        def opposite(self):
            i, half = self.i, self.half
            if self.both is not None:
                self.both(2, 0)
            opposite = self.value(2) if self.both is None else pair_ref[0]
            self.far_out[...] = opposite.astype(BF)
            for h in range(2):
                part = pl.ds(half * h, half)
                send(self.far_out.at[part], self.far_in.at[part], f_s.at[i, h], f_r.at[i, h],
                     along_x(1 if h == 0 else 3))
            self.own[...] = self.value(0) if self.both is None else pair_ref[1]

        def neighbours(self):
            i, half = self.i, self.half
            if self.both is not None:
                self.both(1, 3)
            for h in range(2):
                part = pl.ds(half * h, half)
                rest = pl.ds(half * (1 - h), half)
                o = 1 if h == 0 else 3
                value = self.value(o) if self.both is None else pair_ref[h]
                arrived(self.far_in.at[part], f_s.at[i, h], f_r.at[i, h])
                mine = value[half * h : half * h + half] + self.far_in[part, :].astype(F32)
                self.near_out[h, part, :] = mine.astype(BF)
                self.near_out[h, rest, :] = value[half * (1 - h) : half * (1 - h) + half].astype(BF)
                send(self.near_out.at[h], self.near_in.at[h], g_s.at[i, h], g_r.at[i, h], along_x(o))

        def total(self):
            i = self.i
            acc = self.own[...]
            for h in range(2):
                arrived(self.near_in.at[h], g_s.at[i, h], g_r.at[i, h])
                acc = acc + self.near_in[h].astype(F32)
            return acc

    def project(source, u, o):
        s = (x + o + NX) % NX
        first = dot(source[0, s], wq[u, 0:4].reshape(1024, 256))
        return first + dot(source[1, s], wq[u, 4:8].reshape(1024, 256))

    def text_pair(u, a, b):
        def one(i, carry):
            pair_ref[i] = project(acts, u, a + i * (b - a))
            return carry

        lax.fori_loop(0, 2, one, 0)

    vis_reduce = Reduce(0, v_fo, v_fi, v_no, v_ni, v_own, lambda o: vs[(x + o) % NX])
    image_queries = Reduce(
        1, i_fo, i_fi, i_no, i_ni, i_own,
        lambda o: jnp.concatenate([project(ia, u, o) for u in range(2)], axis=1),
    )
    image_keyvals = Reduce(5, j_fo, j_fi, j_no, j_ni, j_own, lambda o: project(ia, 2, o))
    text_reduce = [
        Reduce(2 + u, t_fo.at[u], t_fi.at[u], t_no.at[u], t_ni.at[u], t_own.at[u],
               None, functools.partial(text_pair, u))
        for u in range(3)
    ]

    def vision():
        vis_spread.from_sibling()
        for h in range(2):
            acc = None
            for s in range(NZ):
                term = dot(vis_all[s].reshape(NX * TOK, LANES), wp[h, s])
                acc = term if acc is None else acc + term
            vs[:, :, 512 * h : 512 * h + 512] = acc.reshape(NX, TOK, 512)

    def image():
        tokens = vis_reduce.total().astype(BF).astype(F32)
        lines = lines_of(jnp.sum(tokens * tokens, axis=-1, keepdims=True))
        image_stats[tn] = jnp.concatenate(lines + [jnp.zeros((7, 128), F32)], axis=0)
        im[...] = (tokens * gain).astype(BF)
        image_spread.begin_y()
        image_spread.begin_x()
        for o in range(1, 8):
            send(image_stats.at[tn], image_stats.at[tn], n_s.at[o - 1], n_r.at[o - 1],
                 (dp, (tn + o) % 8))

    def locals_done(us):
        for u in us:
            locals_[u].wait()

    def image_scale():
        total = image_stats[tn]
        for o in range(1, 8):
            source = (tn - o + 8) % 8
            arrived(image_stats.at[source], n_s.at[o - 1], n_r.at[o - 1])
            total = total + image_stats[source]
        return column_of([lax.rsqrt(total[0:1] / 8192.0 + decoder_epsilon)], TOK)

    def route(i, reduced, scale, out, into):
        half = out.shape[2]
        rows = (reduced.total() * scale).astype(BF)
        both = jnp.concatenate([rows[:, 0:half], rows[:, half : 2 * half]], axis=0)
        out[...] = dot(pick_ref[...], both).astype(BF).reshape(32, 16, half)
        into[dp] = out[dp]

        def one(o, carry):
            to = (dp + o) % 32
            remote(out.at[to], into.at[dp], a_s.at[i, o - 1], a_r.at[i, o - 1], (to, tn)).start()
            return carry

        lax.fori_loop(1, 32, one, 0)

    def routed(i, out, into):
        def one(o, carry):
            source = (dp - o + 32) % 32
            remote(out.at[source], into.at[source], a_s.at[i, o - 1], a_r.at[i, o - 1],
                   here).wait_recv()
            return carry

        lax.fori_loop(1, 32, one, 0)
        return into[...].reshape(512, into.shape[2])

    def routes_sent(i, out, into):
        def one(o, carry):
            to = (dp + o) % 32
            remote(out.at[to], into.at[dp], a_s.at[i, o - 1], a_r.at[i, o - 1], here).wait_send()
            return carry

        lax.fori_loop(1, 32, one, 0)

    vis_spread.near(0)
    vis_spread.near(1)
    ring(1)
    text_spread.turn(0)
    text_spread.turn(1)
    ring(2)
    text_spread.turn(2)
    text_spread.turn(3)
    vis_spread.far(0)
    vis_spread.far(1)
    text_spread.mine(0)
    text_spread.mine(1)
    ring(3)
    text_spread.mine(2)
    text_spread.mine(3)
    vis_spread.to_sibling()
    text_spread.near(0)
    text_spread.near(1)
    ring(4)
    locals_done((0, 1))
    vision()
    vis_reduce.opposite()
    text_spread.near(2)
    vis_reduce.neighbours()
    text_spread.near(3)
    text_spread.far(0)
    text_spread.far(1)
    ring(5)
    image()
    text_spread.far(2)
    text_spread.far(3)
    image_spread.near(0)
    image_spread.near(1)
    ring(6)
    image_spread.far(0)
    image_spread.far(1)
    text_spread.from_sibling()
    locals_done((2, 3, 4))
    text_reduce[0].opposite()
    image_spread.to_sibling()
    ring(7)
    text_reduce[1].opposite()
    text_reduce[0].neighbours()
    image_spread.from_sibling()
    image_queries.opposite()
    ring(8)
    image_keyvals.opposite()
    text_reduce[2].opposite()
    scale = image_scale()
    image_queries.neighbours()
    image_keyvals.neighbours()
    text_reduce[1].neighbours()
    route(0, image_queries, scale, qs, qr)
    route(1, image_keyvals, scale, ks, kr)
    text_reduce[2].neighbours()

    causal = row_of((SEQ, SEQ)) >= lane_of((SEQ, SEQ))

    images_q = routed(0, qs, qr)
    images_k = routed(1, ks, kr)
    placed = [dot(sel_ref[h], images) for images in (images_q, images_k) for h in range(2)]

    texts = [text_reduce[u].total() for u in range(3)]
    cos, sin = cos_ref[...], sin_ref[...]

    def column(i):
        text = texts[i // 2][:, 128 * (i % 2) : 128 * (i % 2) + 128]
        picture = placed[i // 2] if i < 4 else placed[i - 2]
        if i < 4:
            picture = picture[:, 128 * (i % 2) : 128 * (i % 2) + 128]
        return jnp.where(is_image, picture, text)

    def turned(value):
        return (value * cos + pltpu.roll(value, 64, 1) * sin).astype(BF)

    key = turned(column(4))
    value = column(5).astype(BF)
    for h in range(4):
        query = turned(column(h))
        scores = lax.dot_general(query, key, (((1,), (1,)), ((), ())), preferred_element_type=F32)
        scores = jnp.where(causal, scores * HEAD_WIDTH ** (-0.5), -1e30)
        powers = jnp.exp(scores - jnp.max(scores, axis=-1, keepdims=True))
        weights = (powers / jnp.sum(powers, axis=-1, keepdims=True)).astype(BF)
        out_ref[:, 128 * h : 128 * h + 128] = dot(weights, value).astype(BF)

    for copy in pending:
        copy.wait_send()
    for copy, went in later:

        @pl.when(went)
        def _(copy=copy):
            copy.wait_send()


    routes_sent(0, qs, qr)
    routes_sent(1, ks, kr)


def rotation_tables():
    exponents = np.arange(64, dtype=np.float32) * np.float32(2.0 / 128)
    frequency = np.float32(rope_base) ** (-exponents)
    angles = np.arange(SEQ, dtype=np.float32)[:, None] * frequency[None, :]
    cos, sin = np.cos(angles), np.sin(angles)
    return (
        np.concatenate([cos, cos], axis=1).astype(np.float32),
        np.concatenate([-sin, sin], axis=1).astype(np.float32),
    )


def per_device(vis_rows, ln_gain, ln_bias, proj_weight, text_rows, attn_gain, w_query,
               key_value_weight, tile_counts, image_offsets):
    tn = lax.axis_index("tensor")

    def lanes(a):
        return jnp.pad(a, [(0, 0)] * (a.ndim - 1) + [(0, LANES - PART)])

    vis = vis_rows.reshape(TOK, 2, 4, 100).transpose(2, 0, 3, 1).reshape(4, TOK, PART)
    vis = lanes(vis)

    affine = jnp.stack([ln_gain, ln_bias])
    affine = lax.dynamic_slice_in_dim(affine, tn * 400, 400, 2)
    affine = lanes(affine.reshape(2, 2, 4, 100).transpose(0, 2, 3, 1).reshape(2, 4, 1, PART))

    proj = jnp.pad(proj_weight.reshape(PART, 1024), ((0, ROWS - PART), (0, 0)))
    proj = proj.reshape(ROWS, 2, 512).transpose(1, 0, 2)
    cos, sin = rotation_tables()
    vmem = pl.BlockSpec(memory_space=pltpu.VMEM)
    smem = pl.BlockSpec(memory_space=pltpu.SMEM)
    dma = pltpu.SemaphoreType.DMA
    out = pl.pallas_call(
        kernel,
        out_shape=jax.ShapeDtypeStruct((SEQ, 512), BF),
        in_specs=[smem, smem] + [vmem] * 9,
        out_specs=vmem,
        scratch_shapes=[
            pltpu.VMEM((2, NZ, LANES, 512), BF),
            pltpu.VMEM((3, NZ, 256, 256), BF),
            pltpu.VMEM((NZ, NX, TOK, LANES), BF),
            pltpu.VMEM((4, TOK, LANES), BF),
            pltpu.VMEM((8, 8, 128), F32),
            pltpu.VMEM((8, 8, 128), F32),
            pltpu.VMEM((SEQ, 1024), BF),
            pltpu.VMEM((512, 128), BF),
            pltpu.VMEM((2, SEQ, 512), BF),
            pltpu.VMEM((2, NX, SEQ, 1024), BF),
            pltpu.VMEM((NX, TOK, 1024), F32),
            pltpu.VMEM((TOK, 1024), BF),
            pltpu.VMEM((2, NX, TOK, 1024), BF),
            pltpu.VMEM((TOK, 1024), BF),
            pltpu.VMEM((TOK, 1024), BF),
            pltpu.VMEM((2, TOK, 1024), BF),
            pltpu.VMEM((2, TOK, 1024), BF),
            pltpu.VMEM((TOK, 1024), F32),
            pltpu.VMEM((TOK, 512), BF),
            pltpu.VMEM((TOK, 512), BF),
            pltpu.VMEM((2, TOK, 512), BF),
            pltpu.VMEM((2, TOK, 512), BF),
            pltpu.VMEM((TOK, 512), F32),
            pltpu.VMEM((TOK, 256), BF),
            pltpu.VMEM((TOK, 256), BF),
            pltpu.VMEM((2, TOK, 256), BF),
            pltpu.VMEM((2, TOK, 256), BF),
            pltpu.VMEM((TOK, 256), F32),
            pltpu.VMEM((3, SEQ, 256), BF),
            pltpu.VMEM((3, SEQ, 256), BF),
            pltpu.VMEM((3, 2, SEQ, 256), BF),
            pltpu.VMEM((3, 2, SEQ, 256), BF),
            pltpu.VMEM((3, SEQ, 256), F32),
            pltpu.VMEM((2, SEQ, 256), F32),
            pltpu.VMEM((32, 16, 256), BF),
            pltpu.VMEM((32, 16, 256), BF),
            pltpu.VMEM((32, 16, 128), BF),
            pltpu.VMEM((32, 16, 128), BF),
            pltpu.VMEM((3, 4, TOK, LANES), BF),
            pltpu.VMEM((SEQ, 1024), BF),
            pltpu.VMEM((3, TOK, 1024), BF),
            dma((5,)),
            dma((5, 2, 4)),
            dma((5, 2, 4)),
            dma((7,)),
            dma((7,)),
            dma((3, 3, 2)),
            dma((3, 3, 2)),
            dma((3, 4, 2)),
            dma((3, NX, 2)),
            dma((7, CHUNKS)),
            dma((7, CHUNKS)),
            dma((3, NX, 4)),
            dma((3, NX, 4)),
            dma((6, 2)),
            dma((6, 2)),
            dma((6, 2)),
            dma((6, 2)),
            dma((7,)),
            dma((7,)),
            dma((2, 31)),
            dma((2, 31)),
        ],
        compiler_params=pltpu.CompilerParams(collective_id=0, has_side_effects=True, vmem_limit_bytes=40 << 20),
        name="step",
    )(tile_counts, image_offsets, vis, affine, proj, w_query,
      key_value_weight.reshape(256, 256), text_rows[0],
      attn_gain[None], jnp.asarray(cos), jnp.asarray(sin))
    return out[None]


def solution(mesh):
    in_specs = (
        P(None, "dp", None, "tensor"),
        P(),
        P(),
        P("dp", None, "tensor"),
        P("dp", None, "tensor"),
        P(),
        P("dp", "tensor"),
        P("dp", None, "tensor"),
        P(),
        P("dp"),
    )
    return jax.shard_map(per_device, mesh=mesh, in_specs=in_specs,
                         out_specs=P("dp", None, "tensor"), check_vma=False)
```

```python
import functools

import jax
import jax.numpy as jnp
import numpy as np
from jax import lax
from jax.experimental import pallas as pl
from jax.experimental.pallas import tpu as pltpu
from jax.sharding import PartitionSpec as P

MESH = pl.DeviceIdType.MESH
BF = jnp.bfloat16
F32 = jnp.float32

HEAD_WIDTH = 128
SEQ = 384
TOK = 64
CHUNKS = 4
ROW_FOR = ((0, 2, 3, 1), (1, 3, 2, 0), (3, 0, 1, 2), (2, 1, 0, 3))
COLUMN_FOR = tuple(tuple(row.index(r) for r in range(4)) for row in ROW_FOR)
SAMPLE_AT = tuple(tuple([row[k] for row in ROW_FOR].index(r) for r in range(4)) for k in range(4))
NX, NY, NZ = 4, 4, 8
LANES = 256
ROWS = 208
PART = 200
vision_epsilon = 1e-06
decoder_epsilon = 1e-05
rope_base = 500000.0

STARTS = (0, 0, 2, 3, 4)
SLOTS = max(STARTS) + 5


def dot(a, b):
    return jnp.dot(a, b, preferred_element_type=F32)


def lane_of(shape):
    return lax.broadcasted_iota(jnp.int32, shape, len(shape) - 1)


def row_of(shape):
    return lax.broadcasted_iota(jnp.int32, shape, len(shape) - 2)


def kernel(
    cnt_ref, off_ref, vis_ref, affine_ref, proj_ref, query_ref, keyval_ref, raw_ref, attn_ref, cos_ref, sin_ref,
    out_ref,
    wp, wq, vis_all, vis_own, stats, image_stats, text_ref, pick_ref, sel_ref, acts, vs, im, ia,
    v_fo, v_fi, v_no, v_ni, v_own, i_fo, i_fi, i_no, i_ni, i_own, j_fo, j_fi, j_no, j_ni, j_own, t_fo, t_fi, t_no, t_ni, t_own,
    pair_ref, qpair_ref, kpair_ref, qs, qr, ks, kr, vis_col, text_mid, im_col,
    l_sem, z_s, z_r, st_s, st_r, ys_s, ys_r, xs_s, xs_r, tx_s, tx_r, d_s, d_r, f_s, f_r, g_s, g_r, n_s, n_r,
    a_s, a_r,
):
    dp = lax.axis_index("dp")
    tn = lax.axis_index("tensor")
    x, z = dp // NZ, dp % NZ
    y, c = tn // 2, tn % 2
    pending = []

    def remote(src, dst, ssem, rsem, to):
        return pltpu.make_async_remote_copy(
            src_ref=src, dst_ref=dst, send_sem=ssem, recv_sem=rsem, device_id=to,
            device_id_type=MESH,
        )

    def send(src, dst, ssem, rsem, to):
        copy = remote(src, dst, ssem, rsem, to)
        copy.start()
        pending.append(copy)

    here = (dp, tn)

    def arrived(ref, ssem, rsem):
        remote(ref, ref, ssem, rsem, here).wait_recv()

    def own(u):
        if u < 2:
            return proj_ref.at[u]
        return keyval_ref if u == 4 else query_ref.at[:, pl.ds(256 * (u - 2), 256)]

    def slot_ref(u, source):
        if u < 2:
            return wp.at[u, source, pl.ds(0, ROWS)]
        return wq.at[u - 2, source]

    def goes(u, e, k):
        return k < 4 or (u % 2 == e)

    def ring(slot):
        for u, start in enumerate(STARTS):
            k = slot - start
            if k < 0 or k > 4:
                continue
            for e in range(2):
                sign = 1 if e == 0 else -1
                source = (z - sign * k + 2 * NZ) % NZ
                if k >= 1 and goes(u, e, k):
                    arrived(slot_ref(u, source), z_s.at[u, e, k - 1], z_r.at[u, e, k - 1])
                if k <= 3 and goes(u, e, k + 1):
                    to = (x * NZ + (z + sign + NZ) % NZ, tn)
                    src = own(u) if k == 0 else slot_ref(u, source)
                    send(src, slot_ref(u, source), z_s.at[u, e, k], z_r.at[u, e, k], to)

    class Spread:
        def __init__(self, kind, own, column, place):
            self.kind, self.own, self.column, self.place = kind, own, column, place

        def on_y(self, src, slot, h, step):
            k = self.kind
            send(src, self.column(slot, h), ys_s.at[k, slot, h], ys_r.at[k, slot, h],
                 (dp, ((y + step + NY) % NY) * 2 + c))

        def on_x(self, src, j, h, kappa):
            k = self.kind
            copy = remote(src, self.place(c, x, h), xs_s.at[k, j, h], xs_r.at[k, x, h],
                          (kappa * NZ + z, tn))
            local = pltpu.make_async_copy(src, self.place(c, x, h), xs_r.at[k, x, h])

            @pl.when(kappa != x)
            def _():
                copy.start()

            @pl.when(kappa == x)
            def _():
                local.start()

            later.append((copy, kappa != x))

        def begin_y(self):
            for h in range(2):
                self.on_y(self.own(h), 0, h, 1)
                self.on_y(self.own(h), 1, h, -1)

        def begin_x(self):
            for h in range(2):
                self.on_x(self.own(h), 3, h, y)

        def near(self, h):
            k = self.kind
            for slot, step in ((0, 1), (1, -1)):
                arrived(self.column(slot, h), ys_s.at[k, slot, h], ys_r.at[k, slot, h])
                if slot == h:
                    src = self.column(slot, h)
                    send(src, self.column(2, h), ys_s.at[k, 2, h], ys_r.at[k, 2, h],
                         (dp, ((y + step + NY) % NY) * 2 + c))
            for slot, step in ((0, 1), (1, -1)):
                self.on_x(self.column(slot, h), slot, h, (y - step + NY) % NY)

        def far(self, h):
            k = self.kind
            arrived(self.column(2, h), ys_s.at[k, 2, h], ys_r.at[k, 2, h])
            self.on_x(self.column(2, h), 2, h, (y + 2) % NY)

        def to_sibling(self, offsets=(0, 1, 3, 2)):
            k = self.kind
            for o in offsets:
                s = (x + o) % NX
                for h in range(2):
                    ref = self.place(c, s, h)
                    arrived(ref, xs_s.at[k, 0, h], xs_r.at[k, s, h])
                    send(ref, ref, d_s.at[k, s, h], d_r.at[k, s, h], (dp, tn + 1 - 2 * c))

        def from_sibling(self):
            k = self.kind
            for s in range(NX):
                for h in range(2):
                    arrived(self.place(1 - c, s, h), d_s.at[k, s, h], d_r.at[k, s, h])

    later = []
    vis_spread = Spread(
        0,
        lambda h: vis_own.at[pl.ds(2 * h, 2)],
        lambda j, h: vis_col.at[j, pl.ds(2 * h, 2)],
        lambda core, s, h: vis_all.at[pl.ds(4 * core + 2 * h, 2), s],
    )
    def entry(rows, a, b):
        value = jnp.int32(0)
        for i, row in enumerate(rows):
            for j, v in enumerate(row):
                value = value + jnp.where((a == i) & (b == j), v, 0)
        return value

    class TextSpread:
        def __init__(self):
            self.row = entry(ROW_FOR, x, y)
            self.column = entry(COLUMN_FOR, x, y)
            self.sample = {step: entry(SAMPLE_AT, x, (y + step + NY) % NY) for step in (0, -1, 1, 2)}

        def part(self, q):
            return pl.ds(q * (SEQ // CHUNKS), SEQ // CHUNKS)

        def block(self, core, step, q):
            return acts.at[core, self.sample[step], self.part(q)]

        def hop(self, q, stays, src, dst, kind, to):
            ssem, rsem = tx_s.at[kind, q], tx_r.at[kind, q]
            copy = remote(src, dst, ssem, rsem, to)
            local = pltpu.make_async_copy(src, dst, rsem)

            @pl.when(stays)
            def _():
                local.start()

            @pl.when(jnp.logical_not(stays))
            def _():
                copy.start()

            later.append((copy, jnp.logical_not(stays)))

        def begin(self):
            for q in range(CHUNKS):
                part = self.part(q)
                self.hop(q, self.row == y, text_ref.at[part], text_mid.at[part], 0,
                         (dp, self.row * 2 + c))

        def turn(self, q):
            mid = text_mid.at[self.part(q)]
            arrived(mid, tx_s.at[0, q], tx_r.at[0, q])
            self.hop(q, self.column == x, mid, acts.at[c, x, self.part(q)], 2,
                     (self.column * NZ + z, tn))

        def on_y(self, q, block_step, step, kind):
            ref = self.block(c, block_step, q)
            send(ref, ref, tx_s.at[kind, q], tx_r.at[kind, q], (dp, ((y + step + NY) % NY) * 2 + c))

        def to_other(self, q, j, step):
            ref = self.block(c, step, q)
            send(ref, ref, d_s.at[1, j, q], d_r.at[1, j, q], (dp, tn + 1 - 2 * c))

        def mine(self, q):
            arrived(self.block(c, 0, q), tx_s.at[2, q], tx_r.at[2, q])
            self.on_y(q, 0, 1, 4)
            self.on_y(q, 0, -1, 5)
            self.to_other(q, 0, 0)

        def near(self, q):
            arrived(self.block(c, -1, q), tx_s.at[4, q], tx_r.at[4, q])
            arrived(self.block(c, 1, q), tx_s.at[5, q], tx_r.at[5, q])
            if q % 2 == 0:
                self.on_y(q, -1, 1, 6)
            else:
                self.on_y(q, 1, -1, 6)
            self.to_other(q, 1, -1)
            self.to_other(q, 2, 1)

        def far(self, q):
            arrived(self.block(c, 2, q), tx_s.at[6, q], tx_r.at[6, q])
            self.to_other(q, 3, 2)

        def from_sibling(self):
            for q in range(CHUNKS):
                for j, step in enumerate((0, -1, 1, 2)):
                    arrived(self.block(1 - c, step, q), d_s.at[1, j, q], d_r.at[1, j, q])

    text_spread = TextSpread()
    image_spread = Spread(
        2,
        lambda h: im.at[pl.ds(32 * h, 32)],
        lambda j, h: im_col.at[j, pl.ds(32 * h, 32)],
        lambda core, s, h: ia.at[core, s, pl.ds(32 * h, 32)],
    )

    def along_x(o):
        return (((x + o) % NX) * NZ + z, tn)

    barrier = pltpu.get_barrier_semaphore()

    def greet_dp(o, carry):
        pl.semaphore_signal(barrier, inc=1, device_id=((dp + o) % 32, tn), device_id_type=MESH)
        return carry

    def greet_tensor(o, carry):
        pl.semaphore_signal(barrier, inc=1, device_id=(dp, (tn + o) % 8), device_id_type=MESH)
        return carry

    lax.fori_loop(1, 32, greet_dp, 0)
    lax.fori_loop(1, 8, greet_tensor, 0)

    for u in range(2):
        for s in range(NZ):
            wp[u, s, ROWS:LANES, :] = jnp.zeros((LANES - ROWS, 512), BF)
    locals_ = []
    for u in range(5):
        local = pltpu.make_async_copy(own(u), slot_ref(u, z), l_sem.at[u])
        local.start()
        locals_.append(local)

    def lines_of(column):
        rows = column.shape[0]
        wide = jnp.broadcast_to(column, (rows, 128))
        if rows % 128:
            wide = jnp.concatenate([wide, jnp.zeros((128 - rows % 128, 128), F32)], axis=0)
        return [wide[128 * b : 128 * b + 128].T[0:1] for b in range(wide.shape[0] // 128)]

    def column_of(lines, rows):
        wide = [jnp.broadcast_to(line, (128, 128)).T for line in lines]
        wide = wide[0] if len(wide) == 1 else jnp.concatenate(wide, axis=0)
        return wide[0:rows, 0:1]

    xv = vis_ref[...].astype(F32)
    mean = jnp.sum(jnp.sum(xv, axis=0), axis=-1, keepdims=True) / (4 * PART)
    centred = jnp.where(lane_of(xv.shape) < PART, xv - mean[None], 0.0)
    m2 = jnp.sum(jnp.sum(centred * centred, axis=0), axis=-1, keepdims=True)
    raw = raw_ref[...].astype(F32)
    lines = lines_of(jnp.sum(raw * raw, axis=-1, keepdims=True)) + lines_of(mean) + lines_of(m2)
    stats[tn] = jnp.concatenate(lines + [jnp.zeros((3, 128), F32)], axis=0)

    first = jnp.int32(0)
    my_first = jnp.int32(0)
    my_count = jnp.int32(0)
    owners = [jnp.int32(0)] * 8
    for s in range(NX * NZ):
        count = cnt_ref[s]
        my_first = my_first + jnp.where(s < dp, count, 0)
        my_count = my_count + jnp.where(s == dp, count, 0)
        first = first + count
        owners = [a + jnp.where(first <= r * 32 + dp, 1, 0) for r, a in enumerate(owners)]
    shape = (512, 128)
    row, col = row_of(shape), lane_of(shape)
    owner = jnp.zeros(shape, jnp.int32)
    for r in range(8):
        owner = jnp.where(((col >> 3) & 7) == r, owners[r], owner)
    same = ((row >> 4) == owner) & (((row >> 3) & 1) == (col >> 6)) & ((row & 7) == (col & 7))
    pick_ref[...] = jnp.where(same, 1.0, 0.0).astype(BF)
    shape = (SEQ, 512)
    row, col = row_of(shape), lane_of(shape)
    place = row - off_ref[0]
    inside = (place >= 0) & (place < 8 * my_count)
    source = (my_first + (place >> 3)) & 31
    match = inside & ((col >> 4) == source) & ((col & 7) == (place & 7))
    for h in range(2):
        chosen = match & (((col >> 3) & 1) == h)
        sel_ref[h] = jnp.where(chosen, 1.0, 0.0).astype(BF)
    place = row_of((SEQ, 128)) - off_ref[0]
    is_image = (place >= 0) & (place < 8 * my_count)

    pl.semaphore_wait(barrier, 38)
    for o in range(1, 8):
        send(stats.at[tn], stats.at[tn], st_s.at[o - 1], st_r.at[o - 1], (dp, (tn + o) % 8))
    ring(0)
    for o in range(1, 8):
        arrived(stats.at[(tn - o + 8) % 8], st_s.at[o - 1], st_r.at[o - 1])
    means = [stats[t][3:4] for t in range(8)]
    mean = sum(means[1:], means[0]) / 8.0
    total = jnp.zeros((1, 128), F32)
    for t in range(8):
        apart = means[t] - mean
        total = total + stats[t][4:5] + (4.0 * PART) * apart * apart
    scale = column_of([lax.rsqrt(total / (32.0 * PART) + vision_epsilon)], TOK)
    mean = column_of([mean], TOK)
    for i in range(4):
        piece = vis_ref[i].astype(F32)
        vis_own[i] = ((piece - mean) * scale * affine_ref[0, i] + affine_ref[1, i]).astype(BF)
    vis_spread.begin_y()
    vis_spread.begin_x()
    total = stats[0]
    for t in range(1, 8):
        total = total + stats[t]
    scale = lax.rsqrt(total / 8192.0 + decoder_epsilon)
    scale = column_of([scale[b : b + 1] for b in range(3)], SEQ)
    gain = attn_ref[:, pl.ds(pl.multiple_of(tn * 1024, 1024), 1024)]
    text_ref[...] = (raw_ref[...].astype(F32) * scale * gain).astype(BF)
    text_spread.begin()

    class Reduce:
        def __init__(self, index, far_out, far_in, near_out, near_in, own, value, both=None, pair=None):
            self.i, self.value, self.own, self.both, self.pair = index, value, own, both, pair
            self.far_out, self.far_in = far_out, far_in
            self.near_out, self.near_in = near_out, near_in
            self.half = far_out.shape[0] // 2

        def opposite(self):
            i, half = self.i, self.half
            if self.both is not None:
                self.both(2, 0)
            opposite = self.value(2) if self.both is None else self.pair[0]
            self.far_out[...] = opposite.astype(BF)
            for h in range(2):
                part = pl.ds(half * h, half)
                send(self.far_out.at[part], self.far_in.at[part], f_s.at[i, h], f_r.at[i, h],
                     along_x(1 if h == 0 else 3))
            self.own[...] = self.value(0) if self.both is None else self.pair[1]

        def neighbours(self):
            i, half = self.i, self.half
            if self.both is not None:
                self.both(1, 3)
            for h in range(2):
                part = pl.ds(half * h, half)
                rest = pl.ds(half * (1 - h), half)
                o = 1 if h == 0 else 3
                value = self.value(o) if self.both is None else self.pair[h]
                arrived(self.far_in.at[part], f_s.at[i, h], f_r.at[i, h])
                mine = value[half * h : half * h + half] + self.far_in[part, :].astype(F32)
                self.near_out[h, part, :] = mine.astype(BF)
                self.near_out[h, rest, :] = value[half * (1 - h) : half * (1 - h) + half].astype(BF)
                send(self.near_out.at[h], self.near_in.at[h], g_s.at[i, h], g_r.at[i, h], along_x(o))

        def total(self):
            i = self.i
            acc = self.own[...]
            for h in range(2):
                arrived(self.near_in.at[h], g_s.at[i, h], g_r.at[i, h])
                acc = acc + self.near_in[h].astype(F32)
            return acc

    def project(source, u, o):
        s = (x + o + NX) % NX
        first = dot(source[0, s], wq[u, 0:4].reshape(1024, 256))
        return first + dot(source[1, s], wq[u, 4:8].reshape(1024, 256))

    def text_pair(u, a, b):
        def one(i, carry):
            pair_ref[i] = project(acts, u, a + i * (b - a))
            return carry

        lax.fori_loop(0, 2, one, 0)

    def image_pair(units, pair, a, b):
        def one(i, carry):
            for n, u in enumerate(units):
                pair[i, :, 256 * n : 256 * n + 256] = project(ia, u, a + i * (b - a))
            return carry

        lax.fori_loop(0, 2, one, 0)

    vis_reduce = Reduce(0, v_fo, v_fi, v_no, v_ni, v_own, lambda o: vs[(x + o) % NX])
    image_queries = Reduce(1, i_fo, i_fi, i_no, i_ni, i_own, None,
                           functools.partial(image_pair, (0, 1), qpair_ref), qpair_ref)
    image_keyvals = Reduce(5, j_fo, j_fi, j_no, j_ni, j_own, None,
                           functools.partial(image_pair, (2,), kpair_ref), kpair_ref)
    text_reduce = [
        Reduce(2 + u, t_fo.at[u], t_fi.at[u], t_no.at[u], t_ni.at[u], t_own.at[u],
               None, functools.partial(text_pair, u), pair_ref)
        for u in range(3)
    ]

    def vision():
        vis_spread.from_sibling()
        for h in range(2):
            acc = None
            for s in range(NZ):
                term = dot(vis_all[s].reshape(NX * TOK, LANES), wp[h, s])
                acc = term if acc is None else acc + term
            vs[:, :, 512 * h : 512 * h + 512] = acc.reshape(NX, TOK, 512)

    def image():
        tokens = vis_reduce.total().astype(BF).astype(F32)
        lines = lines_of(jnp.sum(tokens * tokens, axis=-1, keepdims=True))
        image_stats[tn] = jnp.concatenate(lines + [jnp.zeros((7, 128), F32)], axis=0)
        im[...] = (tokens * gain).astype(BF)
        image_spread.begin_y()
        image_spread.begin_x()
        for o in range(1, 8):
            send(image_stats.at[tn], image_stats.at[tn], n_s.at[o - 1], n_r.at[o - 1],
                 (dp, (tn + o) % 8))

    def locals_done(us):
        for u in us:
            locals_[u].wait()

    def image_scale():
        total = image_stats[tn]
        for o in range(1, 8):
            source = (tn - o + 8) % 8
            arrived(image_stats.at[source], n_s.at[o - 1], n_r.at[o - 1])
            total = total + image_stats[source]
        return column_of([lax.rsqrt(total[0:1] / 8192.0 + decoder_epsilon)], TOK)

    def route(i, reduced, scale, out, into):
        half = out.shape[2]
        rows = (reduced.total() * scale).astype(BF)
        both = jnp.concatenate([rows[:, 0:half], rows[:, half : 2 * half]], axis=0)
        out[...] = dot(pick_ref[...], both).astype(BF).reshape(32, 16, half)
        into[dp] = out[dp]

        def one(o, carry):
            to = (dp + o) % 32
            remote(out.at[to], into.at[dp], a_s.at[i, o - 1], a_r.at[i, o - 1], (to, tn)).start()
            return carry

        lax.fori_loop(1, 32, one, 0)

    def routed(i, out, into):
        def one(o, carry):
            source = (dp - o + 32) % 32
            remote(out.at[source], into.at[source], a_s.at[i, o - 1], a_r.at[i, o - 1],
                   here).wait_recv()
            return carry

        lax.fori_loop(1, 32, one, 0)
        return into[...].reshape(512, into.shape[2])

    def routes_sent(i, out, into):
        def one(o, carry):
            to = (dp + o) % 32
            remote(out.at[to], into.at[dp], a_s.at[i, o - 1], a_r.at[i, o - 1], here).wait_send()
            return carry

        lax.fori_loop(1, 32, one, 0)

    vis_spread.near(0)
    vis_spread.near(1)
    ring(1)
    text_spread.turn(0)
    text_spread.turn(1)
    ring(2)
    text_spread.turn(2)
    text_spread.turn(3)
    vis_spread.far(0)
    vis_spread.far(1)
    text_spread.mine(0)
    text_spread.mine(1)
    ring(3)
    text_spread.mine(2)
    text_spread.mine(3)
    vis_spread.to_sibling()
    text_spread.near(0)
    text_spread.near(1)
    ring(4)
    locals_done((0, 1))
    vision()
    vis_reduce.opposite()
    text_spread.near(2)
    vis_reduce.neighbours()
    text_spread.near(3)
    text_spread.far(0)
    text_spread.far(1)
    ring(5)
    image()
    text_spread.far(2)
    text_spread.far(3)
    image_spread.near(0)
    image_spread.near(1)
    ring(6)
    image_spread.far(0)
    image_spread.far(1)
    text_spread.from_sibling()
    locals_done((2, 3, 4))
    text_reduce[0].opposite()
    image_spread.to_sibling()
    ring(7)
    text_reduce[1].opposite()
    text_reduce[0].neighbours()
    image_spread.from_sibling()
    image_queries.opposite()
    ring(8)
    image_keyvals.opposite()
    text_reduce[2].opposite()
    scale = image_scale()
    image_queries.neighbours()
    image_keyvals.neighbours()
    text_reduce[1].neighbours()
    route(0, image_queries, scale, qs, qr)
    route(1, image_keyvals, scale, ks, kr)
    text_reduce[2].neighbours()

    causal = row_of((SEQ, SEQ)) >= lane_of((SEQ, SEQ))

    images_q = routed(0, qs, qr)
    images_k = routed(1, ks, kr)
    placed = [dot(sel_ref[h], images) for images in (images_q, images_k) for h in range(2)]

    texts = [text_reduce[u].total() for u in range(3)]
    cos, sin = cos_ref[...], sin_ref[...]

    def column(i):
        text = texts[i // 2][:, 128 * (i % 2) : 128 * (i % 2) + 128]
        picture = placed[i // 2] if i < 4 else placed[i - 2]
        if i < 4:
            picture = picture[:, 128 * (i % 2) : 128 * (i % 2) + 128]
        return jnp.where(is_image, picture, text)

    def turned(value):
        return (value * cos + pltpu.roll(value, 64, 1) * sin).astype(BF)

    key = turned(column(4))
    value = column(5).astype(BF)
    for h in range(4):
        query = turned(column(h))
        scores = lax.dot_general(query, key, (((1,), (1,)), ((), ())), preferred_element_type=F32)
        scores = jnp.where(causal, scores * HEAD_WIDTH ** (-0.5), -1e30)
        powers = jnp.exp(scores - jnp.max(scores, axis=-1, keepdims=True))
        weights = (powers / jnp.sum(powers, axis=-1, keepdims=True)).astype(BF)
        out_ref[:, 128 * h : 128 * h + 128] = dot(weights, value).astype(BF)

    for copy in pending:
        copy.wait_send()
    for copy, went in later:

        @pl.when(went)
        def _(copy=copy):
            copy.wait_send()


    routes_sent(0, qs, qr)
    routes_sent(1, ks, kr)


def rotation_tables():
    exponents = np.arange(64, dtype=np.float32) * np.float32(2.0 / 128)
    frequency = np.float32(rope_base) ** (-exponents)
    angles = np.arange(SEQ, dtype=np.float32)[:, None] * frequency[None, :]
    cos, sin = np.cos(angles), np.sin(angles)
    return (
        np.concatenate([cos, cos], axis=1).astype(np.float32),
        np.concatenate([-sin, sin], axis=1).astype(np.float32),
    )


def per_device(vis_rows, ln_gain, ln_bias, proj_weight, text_rows, attn_gain, w_query,
               key_value_weight, tile_counts, image_offsets):
    tn = lax.axis_index("tensor")

    def lanes(a):
        return jnp.pad(a, [(0, 0)] * (a.ndim - 1) + [(0, LANES - PART)])

    vis = vis_rows.reshape(TOK, 2, 4, 100).transpose(2, 0, 3, 1).reshape(4, TOK, PART)
    vis = lanes(vis)

    affine = jnp.stack([ln_gain, ln_bias])
    affine = lax.dynamic_slice_in_dim(affine, tn * 400, 400, 2)
    affine = lanes(affine.reshape(2, 2, 4, 100).transpose(0, 2, 3, 1).reshape(2, 4, 1, PART))

    proj = jnp.pad(proj_weight.reshape(PART, 1024), ((0, ROWS - PART), (0, 0)))
    proj = proj.reshape(ROWS, 2, 512).transpose(1, 0, 2)
    cos, sin = rotation_tables()
    vmem = pl.BlockSpec(memory_space=pltpu.VMEM)
    smem = pl.BlockSpec(memory_space=pltpu.SMEM)
    dma = pltpu.SemaphoreType.DMA
    out = pl.pallas_call(
        kernel,
        out_shape=jax.ShapeDtypeStruct((SEQ, 512), BF),
        in_specs=[smem, smem] + [vmem] * 9,
        out_specs=vmem,
        scratch_shapes=[
            pltpu.VMEM((2, NZ, LANES, 512), BF),
            pltpu.VMEM((3, NZ, 256, 256), BF),
            pltpu.VMEM((NZ, NX, TOK, LANES), BF),
            pltpu.VMEM((4, TOK, LANES), BF),
            pltpu.VMEM((8, 8, 128), F32),
            pltpu.VMEM((8, 8, 128), F32),
            pltpu.VMEM((SEQ, 1024), BF),
            pltpu.VMEM((512, 128), BF),
            pltpu.VMEM((2, SEQ, 512), BF),
            pltpu.VMEM((2, NX, SEQ, 1024), BF),
            pltpu.VMEM((NX, TOK, 1024), F32),
            pltpu.VMEM((TOK, 1024), BF),
            pltpu.VMEM((2, NX, TOK, 1024), BF),
            pltpu.VMEM((TOK, 1024), BF),
            pltpu.VMEM((TOK, 1024), BF),
            pltpu.VMEM((2, TOK, 1024), BF),
            pltpu.VMEM((2, TOK, 1024), BF),
            pltpu.VMEM((TOK, 1024), F32),
            pltpu.VMEM((TOK, 512), BF),
            pltpu.VMEM((TOK, 512), BF),
            pltpu.VMEM((2, TOK, 512), BF),
            pltpu.VMEM((2, TOK, 512), BF),
            pltpu.VMEM((TOK, 512), F32),
            pltpu.VMEM((TOK, 256), BF),
            pltpu.VMEM((TOK, 256), BF),
            pltpu.VMEM((2, TOK, 256), BF),
            pltpu.VMEM((2, TOK, 256), BF),
            pltpu.VMEM((TOK, 256), F32),
            pltpu.VMEM((3, SEQ, 256), BF),
            pltpu.VMEM((3, SEQ, 256), BF),
            pltpu.VMEM((3, 2, SEQ, 256), BF),
            pltpu.VMEM((3, 2, SEQ, 256), BF),
            pltpu.VMEM((3, SEQ, 256), F32),
            pltpu.VMEM((2, SEQ, 256), F32),
            pltpu.VMEM((2, TOK, 512), F32),
            pltpu.VMEM((2, TOK, 256), F32),
            pltpu.VMEM((32, 16, 256), BF),
            pltpu.VMEM((32, 16, 256), BF),
            pltpu.VMEM((32, 16, 128), BF),
            pltpu.VMEM((32, 16, 128), BF),
            pltpu.VMEM((3, 4, TOK, LANES), BF),
            pltpu.VMEM((SEQ, 1024), BF),
            pltpu.VMEM((3, TOK, 1024), BF),
            dma((5,)),
            dma((5, 2, 4)),
            dma((5, 2, 4)),
            dma((7,)),
            dma((7,)),
            dma((3, 3, 2)),
            dma((3, 3, 2)),
            dma((3, 4, 2)),
            dma((3, NX, 2)),
            dma((7, CHUNKS)),
            dma((7, CHUNKS)),
            dma((3, NX, 4)),
            dma((3, NX, 4)),
            dma((6, 2)),
            dma((6, 2)),
            dma((6, 2)),
            dma((6, 2)),
            dma((7,)),
            dma((7,)),
            dma((2, 31)),
            dma((2, 31)),
        ],
        compiler_params=pltpu.CompilerParams(collective_id=0, has_side_effects=True, vmem_limit_bytes=40 << 20),
        name="step",
    )(tile_counts, image_offsets, vis, affine, proj, w_query,
      key_value_weight.reshape(256, 256), text_rows[0],
      attn_gain[None], jnp.asarray(cos), jnp.asarray(sin))
    return out[None]


def solution(mesh):
    in_specs = (
        P(None, "dp", None, "tensor"),
        P(),
        P(),
        P("dp", None, "tensor"),
        P("dp", None, "tensor"),
        P(),
        P("dp", "tensor"),
        P("dp", None, "tensor"),
        P(),
        P("dp"),
    )
    return jax.shard_map(per_device, mesh=mesh, in_specs=in_specs,
                         out_specs=P("dp", None, "tensor"), check_vma=False)
```
